8 devices in a mesh: pod: 1 (over z), data: 2 (over y), model: 4 (over x, core).
Axes of the slice: x: 2, y: 2, z: 1, core: 2. Of those that a mesh axis runs over, the one named last changes fastest.
Arguments:
- x_in: bfloat16 [2, 1024, 2048], P(('pod', 'data'), 'model')
- dy_in: bfloat16 [2, 1024, 2048], P(('pod', 'data'), 'model')
- w_q: bfloat16 [2048, 8, 256], P(None, 'model')
- w_k: bfloat16 [1, 2048, 256], replicated
- w_v: bfloat16 [1, 2048, 256], replicated
- w_o: bfloat16 [8, 256, 2048], P('model')
Outputs:
- output 1: bfloat16 [2, 1024, 2048], P(('pod', 'data'), 'model')
- output 2: float32 [2048, 8, 256], P(('pod', 'data'), 'model')
- output 3: float32 [2048, 256], P(('pod', 'model', 'data'))
- output 4: float32 [2048, 256], P(('pod', 'model', 'data'))
- output 5: float32 [8, 256, 2048], P(('pod', 'model'), None, 'data')
All inputs are finite; a program needn't handle non-finite values.
Results may differ from the reference program's by a relative error of at most 0.00941715.
Values are sent between devices in bfloat16 or wider.
A program may use at most 1 GiB of HBM per device.

```python
import jax
import jax.numpy as jnp
from jax import lax

NUM_SEQS = 2
SEQ_LEN = 1024
MODEL_DIM = 2048
Q_HEADS = 8
KV_HEADS = 1
HEAD_DIM = 256

GROUP_HEADS = Q_HEADS // KV_HEADS


def setup_inputs(seed: int = 0, part: int = 0) -> dict:
    shared_key = jax.random.key(seed)
    part_key = jax.random.fold_in(jax.random.key(seed + 1), part)
    key_x, key_dy = jax.random.split(part_key, 2)
    key_wq, key_wk, key_wv, key_wo = jax.random.split(shared_key, 4)
    act_shape = (NUM_SEQS, SEQ_LEN, MODEL_DIM)
    in_scale = MODEL_DIM ** -0.5
    out_scale = (Q_HEADS * HEAD_DIM) ** -0.5
    x_in = jax.random.normal(key_x, act_shape, jnp.float32)
    dy_in = jax.random.normal(key_dy, act_shape, jnp.float32)
    w_q = jax.random.normal(key_wq, (MODEL_DIM, Q_HEADS, HEAD_DIM), jnp.float32) * in_scale
    w_k = jax.random.normal(key_wk, (KV_HEADS, MODEL_DIM, HEAD_DIM), jnp.float32) * in_scale
    w_v = jax.random.normal(key_wv, (KV_HEADS, MODEL_DIM, HEAD_DIM), jnp.float32) * in_scale
    w_o = jax.random.normal(key_wo, (Q_HEADS, HEAD_DIM, MODEL_DIM), jnp.float32) * out_scale
    return {'x_in': x_in.astype(jnp.bfloat16), 'dy_in': dy_in.astype(jnp.bfloat16),
            'w_q': w_q.astype(jnp.bfloat16), 'w_k': w_k.astype(jnp.bfloat16),
            'w_v': w_v.astype(jnp.bfloat16), 'w_o': w_o.astype(jnp.bfloat16)}


def group_attention(operands):
    q_grp, k_one, v_one, dout_grp = operands
    score_scale = HEAD_DIM ** -0.5
    q_f32 = q_grp.astype(jnp.float32)
    k_f32 = k_one.astype(jnp.float32)
    v_f32 = v_one.astype(jnp.float32)
    dout_f32 = dout_grp.astype(jnp.float32)
    positions = jnp.arange(SEQ_LEN)
    causal = positions[:, None] >= positions[None, :]
    scores = jnp.einsum('qhe,ke->hqk', q_f32, k_f32) * score_scale
    attn_prob = jax.nn.softmax(jnp.where(causal, scores, -jnp.inf), axis=-1)
    prob_bf = attn_prob.astype(jnp.bfloat16).astype(jnp.float32)
    attn_out = jnp.einsum('hqk,ke->qhe', prob_bf, v_f32).astype(jnp.bfloat16)
    grad_prob = jnp.einsum('qhe,ke->hqk', dout_f32, v_f32)
    row_delta = jnp.einsum('qhe,qhe->hq', dout_f32, attn_out.astype(jnp.float32))
    grad_score = (attn_prob * (grad_prob - row_delta[:, :, None])).astype(jnp.bfloat16).astype(jnp.float32)
    grad_q = (jnp.einsum('hqk,ke->qhe', grad_score, k_f32) * score_scale).astype(jnp.bfloat16)
    grad_k = (jnp.einsum('hqk,qhe->ke', grad_score, q_f32) * score_scale).astype(jnp.bfloat16)
    grad_v = jnp.einsum('hqk,qhe->ke', prob_bf, dout_f32).astype(jnp.bfloat16)
    return attn_out, grad_q, grad_k, grad_v


def heads_to_items(per_head):
    return per_head.reshape(NUM_SEQS, SEQ_LEN, KV_HEADS, GROUP_HEADS, HEAD_DIM).transpose(0, 2, 1, 3, 4).reshape(NUM_SEQS * KV_HEADS, SEQ_LEN, GROUP_HEADS, HEAD_DIM)


def items_to_heads(per_item):
    return per_item.reshape(NUM_SEQS, KV_HEADS, SEQ_LEN, GROUP_HEADS, HEAD_DIM).transpose(0, 2, 1, 3, 4).reshape(NUM_SEQS, SEQ_LEN, Q_HEADS, HEAD_DIM)


def reference(x_in, dy_in, w_q, w_k, w_v, w_o):
    x_f32 = x_in.astype(jnp.float32)
    dy_f32 = dy_in.astype(jnp.float32)
    wq_f32 = w_q.astype(jnp.float32)
    wk_f32 = w_k.astype(jnp.float32)
    wv_f32 = w_v.astype(jnp.float32)
    wo_f32 = w_o.astype(jnp.float32)
    q_proj = jnp.einsum('std,dhe->sthe', x_f32, wq_f32).astype(jnp.bfloat16)
    k_proj = jnp.einsum('std,jde->sjte', x_f32, wk_f32).astype(jnp.bfloat16)
    v_proj = jnp.einsum('std,jde->sjte', x_f32, wv_f32).astype(jnp.bfloat16)
    dout_proj = jnp.einsum('std,hed->sthe', dy_f32, wo_f32).astype(jnp.bfloat16)
    item_count = NUM_SEQS * KV_HEADS
    attn_out, grad_q, grad_k, grad_v = lax.map(group_attention, (
        heads_to_items(q_proj), k_proj.reshape(item_count, SEQ_LEN, HEAD_DIM),
        v_proj.reshape(item_count, SEQ_LEN, HEAD_DIM), heads_to_items(dout_proj)))
    out_f32 = items_to_heads(attn_out).astype(jnp.float32)
    gq_f32 = items_to_heads(grad_q).astype(jnp.float32)
    gk_f32 = grad_k.reshape(NUM_SEQS, KV_HEADS, SEQ_LEN, HEAD_DIM).astype(jnp.float32)
    gv_f32 = grad_v.reshape(NUM_SEQS, KV_HEADS, SEQ_LEN, HEAD_DIM).astype(jnp.float32)
    dw_q = jnp.einsum('std,sthe->dhe', x_f32, gq_f32)
    dw_k = jnp.einsum('std,sjte->jde', x_f32, gk_f32).reshape(KV_HEADS * MODEL_DIM, HEAD_DIM)
    dw_v = jnp.einsum('std,sjte->jde', x_f32, gv_f32).reshape(KV_HEADS * MODEL_DIM, HEAD_DIM)
    dw_o = jnp.einsum('sthe,std->hed', out_f32, dy_f32)
    dx_f32 = (jnp.einsum('sthe,dhe->std', gq_f32, wq_f32)
              + jnp.einsum('sjte,jde->std', gk_f32, wk_f32)
              + jnp.einsum('sjte,jde->std', gv_f32, wv_f32))
    return dx_f32.astype(jnp.bfloat16), dw_q, dw_k, dw_v, dw_o
```

```python
import functools

import jax
import jax.numpy as jnp
from jax import lax
from jax.experimental import pallas as pl
from jax.experimental.pallas import tpu as pltpu
from jax.sharding import PartitionSpec as P

F32 = jnp.float32
BF16 = jnp.bfloat16
SEQ = 1024
BLK = 256
DIM = 2048
HD = 256
HEADS = 2
CH = 512
NCH = DIM // CH
HALF = DIM // 2
SCALE = HD ** -0.5
MESH = pl.DeviceIdType.MESH


def dot_nn(a, b):
    return lax.dot_general(a, b, (((1,), (0,)), ((), ())), preferred_element_type=F32)


def dot_nt(a, b):
    return lax.dot_general(a, b, (((1,), (1,)), ((), ())), preferred_element_type=F32)


def at(start, size, align=256):
    return pl.ds(pl.multiple_of(start, align), size)


def body(x_ref, dy_ref, wq_ref, wk_ref, wv_ref, wo_ref,
         dx_ref, dwq_ref, dwkv_ref, dwo_ref,
         xb, x_t, dyb, wq4, wkv, wo, q, k, v, k_t, v_t, p_t, o_t, do_acc, do_t,
         dkv, dkv_mate, dkv_send, dkv_part, dkv_full, dq, dq_mate,
         dwo_own, dwo_send, dwo_recv, dwq_own, dwq_send, dwq_recv,
         dx_own, dx_send, dx_recv, dx_out, dwkv_own, dwkv_send, dwkv_recv,
         sems, recvs, locs):
    model = lax.axis_index('model')
    data = lax.axis_index('data')
    chip = model // 2
    core = model % 2
    mate = {'model': chip * 2 + 1 - core}
    partner = {'model': (1 - chip) * 2 + core}
    peer = {'data': 1 - data}
    mate_row = (chip * 2 + 1 - core) * BLK
    own_row = model * BLK
    partner_row = ((1 - chip) * 2 + core) * BLK
    diag_row = ((1 - chip) * 2 + 1 - core) * BLK

    started = []
    slots = {}

    def slot(name):
        return slots.setdefault(name, len(slots))

    def send(name, src, dst, device):
        n = slot(name)
        copy = pltpu.make_async_remote_copy(src_ref=src, dst_ref=dst, send_sem=sems.at[n], recv_sem=recvs.at[n],
                                            device_id=device, device_id_type=MESH)
        copy.start()
        started.append(copy)

    def arrived(name, dst, device):
        n = slot(name)
        pltpu.make_async_remote_copy(src_ref=dst, dst_ref=dst, send_sem=sems.at[n], recv_sem=recvs.at[n],
                                     device_id=device, device_id_type=MESH).wait_recv()

    local_count = [0]

    def local(src, dst):
        copy = pltpu.make_async_copy(src, dst, locs.at[local_count[0]])
        local_count[0] += 1
        copy.start()
        return copy

    def chunk_at(j):
        return lax.rem((1 - data) * (NCH // 2) + j, NCH)

    barrier = pltpu.get_barrier_semaphore()
    for device in (mate, partner, peer):
        pl.semaphore_signal(barrier, inc=1, device_id=device, device_id_type=MESH)
    pl.semaphore_wait(barrier, 3)

    send('x_far', x_ref, xb.at[at(own_row, BLK)], partner)
    for j in range(NCH):
        c = chunk_at(j)
        send(f'dy_far{j}', dy_ref.at[:, at(c * CH, CH)], dyb.at[c, at(own_row, BLK)], partner)
    send('x_mate', x_ref, xb.at[at(own_row, BLK)], mate)
    loads = [local(x_ref, xb.at[at(own_row, BLK)]),
             local(wq_ref, wq4.at[pl.ds(core * HEADS, HEADS)]),
             local(wk_ref, wkv.at[0]), local(wv_ref, wkv.at[1])]
    late_loads = [local(wo_ref, wo)]
    for j in range(NCH):
        c = chunk_at(j)
        late_loads.append(local(dy_ref.at[:, at(c * CH, CH)], dyb.at[c, at(own_row, BLK)]))
        send(f'dy_mate{j}', dy_ref.at[:, at(c * CH, CH)], dyb.at[c, at(own_row, BLK)], mate)
    send('wq_mate', wq_ref, wq4.at[pl.ds(core * HEADS, HEADS)], mate)

    def project(first_row):
        def rows_step(r, carry):
            rows = at(first_row + r * BLK, BLK)
            xr = xb[rows, :]
            for h in range(HEADS):
                q[rows, h * HD:(h + 1) * HD] = dot_nn(xr, wq4[core * HEADS + h]).astype(BF16)
            kr = dot_nn(xr, wkv[0]).astype(BF16)
            vr = dot_nn(xr, wkv[1]).astype(BF16)
            k[rows, :] = kr
            v[rows, :] = vr
            k_t[:, rows] = kr.T
            v_t[:, rows] = vr.T

            def flip(t, inner):
                cols = at(t * 256, 256)
                x_t[cols, rows] = xb[rows, cols].T
                return inner
            lax.fori_loop(0, DIM // 256, flip, 0)
            return carry
        lax.fori_loop(0, 2, rows_step, 0)

    for copy in loads:
        copy.wait()
    arrived('x_mate', xb.at[at(mate_row, BLK)], mate)
    project(chip * 2 * BLK)

    arrived('x_far', xb.at[at(partner_row, BLK)], partner)
    send('x_fwd', xb.at[at(partner_row, BLK)], xb.at[at(partner_row, BLK)], mate)
    for copy in late_loads:
        copy.wait()
    for j in range(NCH):
        arrived(f'dy_mate{j}', dyb.at[chunk_at(j), at(mate_row, BLK)], mate)
    arrived('wq_mate', wq4.at[pl.ds((1 - core) * HEADS, HEADS)], mate)
    arrived('x_fwd', xb.at[at(diag_row, BLK)], mate)
    project((1 - chip) * 2 * BLK)

    def forward_chunk(j):
        c = chunk_at(j)
        block = dyb.at[c, at(partner_row, BLK)]
        arrived(f'dy_far{j}', block, partner)
        send(f'dy_fwd{j}', block, block, mate)

    mask = lax.broadcasted_iota(jnp.int32, (BLK, BLK), 0) <= lax.broadcasted_iota(jnp.int32, (BLK, BLK), 1)

    def forward_head(h, carry):
        heads = at(h * HD, HD)
        for i in range(SEQ // BLK):
            cols = slice(i * BLK, (i + 1) * BLK)
            qi = q[cols, heads]
            parts = []
            for j in range(i + 1):
                s = dot_nt(k[j * BLK:(j + 1) * BLK, :], qi) * SCALE
                parts.append(jnp.where(mask, s, -jnp.inf) if j == i else s)
            top = functools.reduce(jnp.maximum, [jnp.max(s, axis=0, keepdims=True) for s in parts])
            parts = [jnp.exp(s - top) for s in parts]
            total = functools.reduce(jnp.add, [jnp.sum(s, axis=0, keepdims=True) for s in parts])
            inv = 1.0 / total
            out = jnp.zeros((HD, BLK), F32)
            for j in range(i + 1):
                prob = parts[j] * inv
                p_t[h, j * BLK:(j + 1) * BLK, cols] = prob
                out += dot_nn(v_t[:, j * BLK:(j + 1) * BLK], prob.astype(BF16))
            o_t[heads, cols] = out.astype(BF16)
        return carry
    lax.fori_loop(0, HEADS, forward_head, 0)

    for j in range(NCH):
        c = chunk_at(j)
        forward_chunk(j)
        arrived(f'dy_fwd{j}', dyb.at[c, at(diag_row, BLK)], mate)
        part = dot_nt(wo[:, at(c * CH, CH)], dyb[c])
        if j == 0:
            do_acc[...] = part
        elif j < NCH - 1:
            do_acc[...] += part
        else:
            do_t[...] = (do_acc[...] + part).astype(BF16)
        if j < NCH // 2:
            dwo_send[j] = dot_nn(o_t[...], dyb[c]).astype(BF16)
            send(f'dwo{j}', dwo_send.at[j], dwo_recv.at[j], peer)

    dkv[...] = jnp.zeros(dkv.shape, F32)

    def backward_head(h, carry):
        heads = at(h * HD, HD)
        for i in range(SEQ // BLK):
            cols = slice(i * BLK, (i + 1) * BLK)
            qi = q[cols, heads]
            doi = do_t[heads, cols]
            delta = jnp.sum(doi.astype(F32) * o_t[heads, cols].astype(F32), axis=0, keepdims=True)
            dqi = jnp.zeros((HD, BLK), F32)
            for j in range(i + 1):
                rows = slice(j * BLK, (j + 1) * BLK)
                prob = p_t[h, rows, cols]
                ds = (prob * (dot_nn(v[rows, :], doi) - delta)).astype(BF16)
                dqi += dot_nn(k_t[:, rows], ds)
                dkv[0, rows, :] += dot_nn(ds, qi)
                dkv[1, rows, :] += dot_nt(prob.astype(BF16), doi)
            dq[h, cols, :] = (dqi * SCALE).astype(BF16).T
        return carry
    lax.fori_loop(0, HEADS, backward_head, 0)

    send('dkv_mate', dkv.at[1 - core], dkv_mate, mate)
    for b in range(2):
        rows = at((b * 2 + 1 - core) * BLK, BLK)
        send(f'dq_mate{b}', dq.at[:, rows], dq_mate.at[b], mate)
    arrived('dkv_mate', dkv_mate, mate)
    factor = jnp.where(core == 0, SCALE, 1.0).astype(F32)
    summed = (dkv[core] + dkv_mate[...]) * factor
    dkv_mate[...] = summed
    dkv_send[...] = summed.astype(BF16)
    send('dkv_far', dkv_send, dkv_part, partner)
    for b in range(2):
        arrived(f'dq_mate{b}', dq_mate.at[b], mate)

    def dx_cols(block, cols):
        rows = at((block * 2 + core) * BLK, BLK)
        acc = jnp.zeros((BLK, CH), F32)
        for h in range(HEADS):
            acc += dot_nt(dq[h, rows, :], wq4[core * HEADS + h, cols, :])
            acc += dot_nt(dq_mate[block, h], wq4[(1 - core) * HEADS + h, cols, :])
        return acc

    for j in range(NCH):
        dx_send[j] = dx_cols(1 - chip, slice(j * CH, (j + 1) * CH)).astype(BF16)
        send(f'dx{j}', dx_send.at[j], dx_recv.at[j], partner)

    def dwq_step(r, carry):
        rows = at((1 - data) * HALF + r * 256, 256)
        for h in range(HEADS):
            dwq_send[h, at(r * 256, 256), :] = dot_nn(x_t[rows, :], dq[h]).astype(BF16)
        return carry
    lax.fori_loop(0, HALF // 256, dwq_step, 0)
    send('dwq', dwq_send, dwq_recv, peer)

    def dwq_own_step(r, carry):
        rows = at(data * HALF + r * 256, 256)
        for h in range(HEADS):
            dwq_own[h, at(r * 256, 256), :] = dot_nn(x_t[rows, :], dq[h])
        return carry
    lax.fori_loop(0, HALF // 256, dwq_own_step, 0)

    for j in range(NCH):
        dx_own[:, j * CH:(j + 1) * CH] = dx_cols(chip, slice(j * CH, (j + 1) * CH))
    for j in range(NCH // 2, NCH):
        dwo_own[:, (j - NCH // 2) * CH:(j - NCH // 2 + 1) * CH] = dot_nn(o_t[...], dyb[chunk_at(j)])

    arrived('dkv_far', dkv_part, partner)
    dkv_full[core] = (dkv_mate[...] + dkv_part[...].astype(F32)).astype(BF16)
    send('dkv_full', dkv_full.at[core], dkv_full.at[core], mate)
    for j in range(NCH // 2):
        arrived(f'dwo{j}', dwo_recv.at[j], peer)
        dwo_own[:, j * CH:(j + 1) * CH] += dwo_recv[j].astype(F32)
    outs = []
    outs.append(local(dwo_own, dwo_ref))
    arrived('dkv_full', dkv_full.at[1 - core], mate)
    for n in range(2):
        peer_rows = at((model * 2 + 1 - data) * 256, 256)
        dwkv_send[n] = dot_nn(x_t[peer_rows, :], dkv_full[n]).astype(BF16)
    send('dwkv', dwkv_send, dwkv_recv, peer)
    for n in range(2):
        dwkv_own[n] = dot_nn(x_t[at((model * 2 + data) * 256, 256), :], dkv_full[n])
    for j in range(NCH):
        cols = slice(j * CH, (j + 1) * CH)
        dx_own[:, cols] += (dot_nt(dkv_full[0, at(own_row, BLK), :], wkv[0, cols, :])
                            + dot_nt(dkv_full[1, at(own_row, BLK), :], wkv[1, cols, :]))

    arrived('dwq', dwq_recv, peer)

    def dwq_sum(r, carry):
        rows = at(r * 256, 256)
        for h in range(HEADS):
            dwq_own[h, rows, :] += dwq_recv[h, rows, :].astype(F32)
        return carry
    lax.fori_loop(0, HALF // 256, dwq_sum, 0)
    outs.append(local(dwq_own, dwq_ref))
    arrived('dwkv', dwkv_recv, peer)
    for n in range(2):
        dwkv_own[n] += dwkv_recv[n].astype(F32)
    outs.append(local(dwkv_own, dwkv_ref))
    for j in range(NCH):
        arrived(f'dx{j}', dx_recv.at[j], partner)
        cols = slice(j * CH, (j + 1) * CH)
        dx_out[:, cols] = (dx_own[:, cols] + dx_recv[j].astype(F32)).astype(BF16)
    outs.append(local(dx_out, dx_ref))
    for copy in started:
        copy.wait_send()
    for copy in outs:
        copy.wait()
    assert len(slots) <= sems.shape[0] and local_count[0] <= locs.shape[0]


def fused_step(x, dy, wq, wk, wv, wo):
    any_spec = pl.BlockSpec(memory_space=pl.ANY)
    scratch = [
        pltpu.VMEM((SEQ, DIM), BF16),
        pltpu.VMEM((DIM, SEQ), BF16),
        pltpu.VMEM((NCH, SEQ, CH), BF16),
        pltpu.VMEM((2 * HEADS, DIM, HD), BF16),
        pltpu.VMEM((2, DIM, HD), BF16),
        pltpu.VMEM((HEADS * HD, DIM), BF16),
        pltpu.VMEM((SEQ, HEADS * HD), BF16),
        pltpu.VMEM((SEQ, HD), BF16),
        pltpu.VMEM((SEQ, HD), BF16),
        pltpu.VMEM((HD, SEQ), BF16),
        pltpu.VMEM((HD, SEQ), BF16),
        pltpu.VMEM((HEADS, SEQ, SEQ), F32),
        pltpu.VMEM((HEADS * HD, SEQ), BF16),
        pltpu.VMEM((HEADS * HD, SEQ), F32),
        pltpu.VMEM((HEADS * HD, SEQ), BF16),
        pltpu.VMEM((2, SEQ, HD), F32),
        pltpu.VMEM((SEQ, HD), F32),
        pltpu.VMEM((SEQ, HD), BF16),
        pltpu.VMEM((SEQ, HD), BF16),
        pltpu.VMEM((2, SEQ, HD), BF16),
        pltpu.VMEM((HEADS, SEQ, HD), BF16),
        pltpu.VMEM((2, HEADS, BLK, HD), BF16),
        pltpu.VMEM((HEADS * HD, HALF), F32),
        pltpu.VMEM((NCH // 2, HEADS * HD, CH), BF16),
        pltpu.VMEM((NCH // 2, HEADS * HD, CH), BF16),
        pltpu.VMEM((HEADS, HALF, HD), F32),
        pltpu.VMEM((HEADS, HALF, HD), BF16),
        pltpu.VMEM((HEADS, HALF, HD), BF16),
        pltpu.VMEM((BLK, DIM), F32),
        pltpu.VMEM((NCH, BLK, CH), BF16),
        pltpu.VMEM((NCH, BLK, CH), BF16),
        pltpu.VMEM((BLK, DIM), BF16),
        pltpu.VMEM((2, 256, HD), F32),
        pltpu.VMEM((2, 256, HD), BF16),
        pltpu.VMEM((2, 256, HD), BF16),
        pltpu.SemaphoreType.DMA((32,)),
        pltpu.SemaphoreType.DMA((32,)),
        pltpu.SemaphoreType.DMA((16,)),
    ]
    return pl.pallas_call(
        body,
        out_shape=(jax.ShapeDtypeStruct((BLK, DIM), BF16),
                   jax.ShapeDtypeStruct((HEADS, HALF, HD), F32),
                   jax.ShapeDtypeStruct((2, 256, HD), F32),
                   jax.ShapeDtypeStruct((HEADS * HD, HALF), F32)),
        in_specs=[any_spec] * 6,
        out_specs=(any_spec,) * 4,
        scratch_shapes=scratch,
        compiler_params=pltpu.CompilerParams(collective_id=0, has_side_effects=True,
                                             vmem_limit_bytes=67_043_328),
        name='attention_backward',
    )(x, dy, wq, wk, wv, wo)


def solution(mesh):
    tok_spec = P(('pod', 'data'), 'model', None)

    def device_step(x_loc, dy_loc, w_q, w_k, w_v, w_o):
        dx, dwq, dwkv, dwo = fused_step(x_loc[0], dy_loc[0], jnp.transpose(w_q, (1, 0, 2)), w_k[0], w_v[0],
                                        w_o.reshape(HEADS * HD, DIM))
        return (dx[None], jnp.transpose(dwq, (1, 0, 2)), dwkv[0], dwkv[1], dwo.reshape(HEADS, HD, HALF))

    kv_rows = P(('pod', 'model', 'data'), None)
    return jax.shard_map(device_step, mesh=mesh,
                         in_specs=(tok_spec, tok_spec, P(None, 'model', None), P(), P(), P('model', None, None)),
                         out_specs=(tok_spec, P(('pod', 'data'), 'model', None), kv_rows, kv_rows,
                                    P(('pod', 'model'), None, 'data')),
                         check_vma=False)
```

```python
import functools

import jax
import jax.numpy as jnp
from jax import lax
from jax.experimental import pallas as pl
from jax.experimental.pallas import tpu as pltpu
from jax.sharding import PartitionSpec as P

F32 = jnp.float32
BF16 = jnp.bfloat16
SEQ = 1024
BLK = 256
DIM = 2048
HD = 256
HEADS = 2
CH = 512
NCH = DIM // CH
PIECE = 64
NP = BLK // PIECE
HALF = DIM // 2
SCALE = HD ** -0.5
MESH = pl.DeviceIdType.MESH


def dot_nn(a, b):
    return lax.dot_general(a, b, (((1,), (0,)), ((), ())), preferred_element_type=F32)


def dot_nt(a, b):
    return lax.dot_general(a, b, (((1,), (1,)), ((), ())), preferred_element_type=F32)


def at(start, size, align=256):
    return pl.ds(pl.multiple_of(start, align), size)


def body(x_ref, dy_ref, wq_ref, wk_ref, wv_ref, wo_ref,
         dx_out, dwq_out, dwk_out, dwv_out, dwo_out,
         xb, x_t, dyb, wq_raw, wq4, wkv, wo, q, k, v, k_t, v_t, p_t, ds_t, o_t, do_acc, do_t,
         dkv, dkv_mate, dkv_send, dkv_part, dkv_full, dq, dq_mate,
         dwo_send, dwo_recv, dwq_send, dwq_recv,
         dx_own, dx_send, dx_recv, dwkv_send, dwkv_recv,
         sems, recvs, locs):
    model = lax.axis_index('model')
    data = lax.axis_index('data')
    chip = model // 2
    core = model % 2
    mate = {'model': chip * 2 + 1 - core}
    partner = {'model': (1 - chip) * 2 + core}
    peer = {'data': 1 - data}
    own_row = model * BLK
    mate_row = (chip * 2 + 1 - core) * BLK
    partner_row = ((1 - chip) * 2 + core) * BLK
    diag_row = ((1 - chip) * 2 + 1 - core) * BLK
    near = chip * 2 * BLK
    far = (1 - chip) * 2 * BLK

    started = []
    slots = {}

    def slot(name):
        return slots.setdefault(name, len(slots))

    def send(name, src, dst, device):
        n = slot(name)
        copy = pltpu.make_async_remote_copy(src_ref=src, dst_ref=dst, send_sem=sems.at[n], recv_sem=recvs.at[n],
                                            device_id=device, device_id_type=MESH)
        copy.start()
        started.append(copy)

    def arrived(name, dst, device):
        n = slot(name)
        with jax.named_scope('w_' + name):
            pltpu.make_async_remote_copy(src_ref=dst, dst_ref=dst, send_sem=sems.at[n], recv_sem=recvs.at[n],
                                         device_id=device, device_id_type=MESH).wait_recv()

    local_count = [0]

    def local(src, dst):
        copy = pltpu.make_async_copy(src, dst, locs.at[local_count[0]])
        local_count[0] += 1
        copy.start()
        return copy

    def chunk_at(j):
        return lax.rem((1 - data) * (NCH // 2) + j, NCH)

    def x_piece(row, p):
        return at(row + p * PIECE, PIECE, PIECE)

    def send_dy(j):
        c = chunk_at(j)
        send(f'dy_far{j}', dy_ref.at[:, at(c * CH, CH)], dyb.at[c, at(own_row, BLK)], partner)

    barrier = pltpu.get_barrier_semaphore()
    for device in (mate, partner, peer):
        pl.semaphore_signal(barrier, inc=1, device_id=device, device_id_type=MESH)
    loads = [local(x_ref, xb.at[at(own_row, BLK)]), local(wq_ref, wq_raw),
             local(wk_ref, wkv.at[0]), local(wv_ref, wkv.at[1])]
    with jax.named_scope('barrier'):
        pl.semaphore_wait(barrier, 3)

    for p in range(NP):
        send(f'x_far{p}', x_ref.at[pl.ds(p * PIECE, PIECE)], xb.at[x_piece(own_row, p)], partner)
    send('x_mate', x_ref, xb.at[at(own_row, BLK)], mate)
    late_loads = [local(wo_ref, wo)]
    for j in range(NCH):
        c = chunk_at(j)
        late_loads.append(local(dy_ref.at[:, at(c * CH, CH)], dyb.at[c, at(own_row, BLK)]))
        send(f'dy_mate{j}', dy_ref.at[:, at(c * CH, CH)], dyb.at[c, at(own_row, BLK)], mate)

    def project(xr, pieces):
        def put(dst, lo, value):
            for row, size, off in pieces:
                dst[row, lo:lo + HD] = value[off:off + size]
        for h in range(HEADS):
            put(q, h * HD, dot_nn(xr, wq4[core * HEADS + h]).astype(BF16))
        for n, (dst, dst_t) in enumerate(((k, k_t), (v, v_t))):
            value = dot_nn(xr, wkv[n]).astype(BF16)
            put(dst, 0, value)

    def flip_x(first_row):
        def step(t, carry):
            cols = at(t * 256, 256)
            for r in range(2):
                rows = at(first_row + r * BLK, BLK)
                x_t[cols, rows] = xb[rows, cols].T
            return carry
        lax.fori_loop(0, DIM // 256, step, 0)

    def flip_kv(first_row):
        for r in range(2):
            rows = at(first_row + r * BLK, BLK)
            k_t[:, rows] = k[rows, :].T
            v_t[:, rows] = v[rows, :].T

    with jax.named_scope('loads'):
        for copy in loads:
            copy.wait()

    with jax.named_scope('relay'):
        def relay(r, carry):
            rows = at(r * 128, 128, 128)
            for h in range(HEADS):
                wq4[core * HEADS + h, rows, :] = wq_raw[rows, h, :]
            return carry
        lax.fori_loop(0, DIM // 128, relay, 0)
    send('wq_mate', wq4.at[pl.ds(core * HEADS, HEADS)], wq4.at[pl.ds(core * HEADS, HEADS)], mate)

    arrived('x_mate', xb.at[at(mate_row, BLK)], mate)
    with jax.named_scope('proj1'):
        def project_near(r, carry):
            rows = at(near + r * BLK, BLK)
            project(xb[rows, :], [(rows, BLK, 0)])
            return carry
        lax.fori_loop(0, 2, project_near, 0)
        flip_kv(near)

    def forward_x(p):
        block = xb.at[x_piece(partner_row, p)]
        arrived(f'x_far{p}', block, partner)
        send(f'x_fwd{p}', block, block, mate)

    def project_far(p):
        for n in (p - 1, p):
            arrived(f'x_fwd{n}', xb.at[x_piece(diag_row, n)], mate)
        first = (p - 1) * PIECE
        rows = [at(row + first, 2 * PIECE, PIECE) for row in (partner_row, diag_row)]
        xr = jnp.concatenate([xb[r, :] for r in rows], axis=0)
        with jax.named_scope('proj2'):
            project(xr, [(rows[0], 2 * PIECE, 0), (rows[1], 2 * PIECE, 2 * PIECE)])

    forward_x(0)
    with jax.named_scope('flip1'):
        flip_x(near)
    forward_x(1)
    send_dy(0)
    project_far(1)
    for copy in late_loads:
        copy.wait()
    for j in range(NCH):
        arrived(f'dy_mate{j}', dyb.at[chunk_at(j), at(mate_row, BLK)], mate)
    with jax.named_scope('do_near'):
        for half in range(HEADS):
            heads = slice(half * HD, (half + 1) * HD)
            acc = jnp.zeros((HD, 2 * BLK), F32)
            for c in range(NCH):
                acc += dot_nt(wo[heads, c * CH:(c + 1) * CH], dyb[c, at(near, 2 * BLK), :])
            do_t[heads, at(near, 2 * BLK)] = acc.astype(BF16)
        dkv[...] = jnp.zeros(dkv.shape, F32)
    forward_x(2)
    send_dy(1)
    forward_x(3)
    send_dy(2)
    send_dy(3)
    project_far(3)
    flip_kv(far)

    mask = lax.broadcasted_iota(jnp.int32, (BLK, BLK), 0) <= lax.broadcasted_iota(jnp.int32, (BLK, BLK), 1)

    def forward_head(h, carry):
        heads = at(h * HD, HD)
        for i in range(SEQ // BLK):
            cols = slice(i * BLK, (i + 1) * BLK)
            qi = q[cols, heads]
            parts = []
            for j in range(i + 1):
                s = dot_nt(k[j * BLK:(j + 1) * BLK, :], qi) * SCALE
                parts.append(jnp.where(mask, s, -jnp.inf) if j == i else s)
            top = functools.reduce(jnp.maximum, [jnp.max(s, axis=0, keepdims=True) for s in parts])
            parts = [jnp.exp(s - top) for s in parts]
            total = functools.reduce(jnp.add, [jnp.sum(s, axis=0, keepdims=True) for s in parts])
            inv = 1.0 / total
            out = jnp.zeros((HD, BLK), F32)
            for j in range(i + 1):
                prob = parts[j] * inv
                p_t[h, j * BLK:(j + 1) * BLK, cols] = prob
                out += dot_nn(v_t[:, j * BLK:(j + 1) * BLK], prob.astype(BF16))
            o_t[heads, cols] = out.astype(BF16)
        return carry
    with jax.named_scope('fwd'):
        lax.fori_loop(0, HEADS, forward_head, 0)

    def add_dkv(h, i, j, prob, ds):
        rows = slice(j * BLK, (j + 1) * BLK)
        cols = slice(i * BLK, (i + 1) * BLK)
        heads = at(h * HD, HD)
        dkv[0, rows, :] += dot_nn(ds, q[cols, heads])
        dkv[1, rows, :] += dot_nt(prob.astype(BF16), do_t[heads, cols])

    def backward_block(h, i, keep):
        heads = at(h * HD, HD)
        cols = slice(i * BLK, (i + 1) * BLK)
        doi = do_t[heads, cols]
        delta = jnp.sum(doi.astype(F32) * o_t[heads, cols].astype(F32), axis=0, keepdims=True)
        dqi = jnp.zeros((HD, BLK), F32)
        for j in range(i + 1):
            rows = slice(j * BLK, (j + 1) * BLK)
            prob = p_t[h, rows, cols]
            ds = (prob * (dot_nn(v[rows, :], doi) - delta)).astype(BF16)
            dqi += dot_nn(k_t[:, rows], ds)
            if keep:
                ds_t[h, rows, (i % 2) * BLK:(i % 2 + 1) * BLK] = ds
            else:
                add_dkv(h, i, j, prob, ds)
        dq[h, cols, :] = (dqi * SCALE).astype(BF16).T

    def over_heads(step):
        def one(h, carry):
            step(h)
            return carry
        lax.fori_loop(0, HEADS, one, 0)

    def take_chunk(j):
        c = chunk_at(j)
        block = dyb.at[c, at(partner_row, BLK)]
        arrived(f'dy_far{j}', block, partner)
        send(f'dy_fwd{j}', block, block, mate)
        arrived(f'dy_fwd{j}', dyb.at[c, at(diag_row, BLK)], mate)
        part = dot_nt(wo[:, at(c * CH, CH)], dyb[c, at(far, 2 * BLK), :])
        if j == 0:
            do_acc[...] = part
        elif j < NCH - 1:
            do_acc[...] += part
        else:
            do_t[:, at(far, 2 * BLK)] = (do_acc[...] + part).astype(BF16)
        if j < NCH // 2:
            dwo_send[j] = dot_nn(o_t[...], dyb[c]).astype(BF16)
            send(f'dwo{j}', dwo_send.at[j], dwo_recv.at[j], peer)

    take_chunk(0)
    take_chunk(1)

    for c in range(2):
        @pl.when(chip == c)
        def _(c=c):
            def step(h):
                for i in (2 * c, 2 * c + 1):
                    backward_block(h, i, False)
            with jax.named_scope('bwd_near'):
                over_heads(step)
    send('dq_near', dq.at[:, at(mate_row, BLK)], dq_mate.at[chip], mate)
    take_chunk(2)
    with jax.named_scope('flip2'):
        flip_x(far)
    take_chunk(3)

    for c in range(2):
        for first in range(2):
            @pl.when((chip == c) & (core == 1 - first))
            def _(c=c, first=first):
                with jax.named_scope('bwd_far0'):
                    over_heads(lambda h: backward_block(h, 2 * (1 - c) + first, True))
    send('dq_far', dq.at[:, at(diag_row, BLK)], dq_mate.at[1 - chip], mate)
    for c in range(2):
        for first in range(2):
            @pl.when((chip == c) & (core == 1 - first))
            def _(c=c, first=first):
                with jax.named_scope('bwd_far1'):
                    over_heads(lambda h: backward_block(h, 2 * (1 - c) + 1 - first, True))
    arrived('wq_mate', wq4.at[pl.ds((1 - core) * HEADS, HEADS)], mate)
    arrived('dq_far', dq_mate.at[1 - chip], mate)

    def dx_cols(block, cols):
        rows = at((block * 2 + core) * BLK, BLK)
        acc = jnp.zeros((BLK, CH), F32)
        for h in range(HEADS):
            acc += dot_nt(dq[h, rows, :], wq4[core * HEADS + h, cols, :])
            acc += dot_nt(dq_mate[block, h], wq4[(1 - core) * HEADS + h, cols, :])
        return acc

    def send_dx(j):
        dx_send[j] = dx_cols(1 - chip, slice(j * CH, (j + 1) * CH)).astype(BF16)
        send(f'dx{j}', dx_send.at[j], dx_recv.at[j], partner)

    send_dx(0)
    send_dx(1)
    for c in range(2):
        @pl.when(chip == c)
        def _(c=c):
            def step(h):
                for i in (2 * (1 - c), 2 * (1 - c) + 1):
                    for j in range(i + 1):
                        rows = slice(j * BLK, (j + 1) * BLK)
                        add_dkv(h, i, j, p_t[h, rows, i * BLK:(i + 1) * BLK],
                                ds_t[h, rows, (i % 2) * BLK:(i % 2 + 1) * BLK])
            with jax.named_scope('dkv'):
                over_heads(step)
    send('dkv_mate', dkv.at[1 - core], dkv_mate, mate)

    def send_dwq(r):
        with jax.named_scope('dwq'):
            rows = at((1 - data) * HALF + r * 256, 256)
            for h in range(HEADS):
                dwq_send[r, h] = dot_nn(x_t[rows, :], dq[h]).astype(BF16)
            send(f'dwq{r}', dwq_send.at[r], dwq_recv.at[r], peer)
    send_dwq(0)
    arrived('dkv_mate', dkv_mate, mate)
    factor = jnp.where(core == 0, SCALE, 1.0).astype(F32)
    summed = (dkv[core] + dkv_mate[...]) * factor
    dkv_mate[...] = summed
    dkv_send[...] = summed.astype(BF16)
    send('dkv_far', dkv_send, dkv_part, partner)
    send_dx(2)
    send_dx(3)
    for r in range(1, 4):
        send_dwq(r)

    arrived('dq_near', dq_mate.at[chip], mate)
    for j in range(NCH):
        dx_own[:, j * CH:(j + 1) * CH] = dx_cols(chip, slice(j * CH, (j + 1) * CH))
    for j in range(NCH // 2):
        arrived(f'dwo{j}', dwo_recv.at[j], peer)
        cols = slice(j * CH, (j + 1) * CH)
        dwo_out[:, cols] = dot_nn(o_t[...], dyb[chunk_at(NCH // 2 + j)]) + dwo_recv[j].astype(F32)

    arrived('dkv_far', dkv_part, partner)
    dkv_full[core] = (dkv_mate[...] + dkv_part[...].astype(F32)).astype(BF16)
    send('dkv_full', dkv_full.at[core], dkv_full.at[core], mate)
    arrived('dkv_full', dkv_full.at[1 - core], mate)
    for n in range(2):
        peer_rows = at((model * 2 + 1 - data) * 256, 256)
        dwkv_send[n] = dot_nn(x_t[peer_rows, :], dkv_full[n]).astype(BF16)
    send('dwkv', dwkv_send, dwkv_recv, peer)
    kept_rows = at((model * 2 + data) * 256, 256)
    dwk_out[...] = dot_nn(x_t[kept_rows, :], dkv_full[0])
    dwv_out[...] = dot_nn(x_t[kept_rows, :], dkv_full[1])
    for j in range(NCH):
        cols = slice(j * CH, (j + 1) * CH)
        dx_own[:, cols] += (dot_nt(dkv_full[0, at(own_row, BLK), :], wkv[0, cols, :])
                            + dot_nt(dkv_full[1, at(own_row, BLK), :], wkv[1, cols, :]))

    def finish_dx(j):
        arrived(f'dx{j}', dx_recv.at[j], partner)
        cols = slice(j * CH, (j + 1) * CH)
        dx_out[:, cols] = (dx_own[:, cols] + dx_recv[j].astype(F32)).astype(BF16)

    finish_dx(0)
    finish_dx(1)
    for r in range(4):
        arrived(f'dwq{r}', dwq_recv.at[r], peer)
        with jax.named_scope('dwq_sum'):
            rows = at(data * HALF + r * 256, 256)
            for h in range(HEADS):
                value = dot_nn(x_t[rows, :], dq[h]) + dwq_recv[r, h].astype(F32)
                dwq_out[r * 256:(r + 1) * 256, h, :] = value
    finish_dx(2)
    arrived('dwkv', dwkv_recv, peer)
    dwk_out[...] += dwkv_recv[0].astype(F32)
    dwv_out[...] += dwkv_recv[1].astype(F32)
    finish_dx(3)
    with jax.named_scope('sends'):
        for copy in started:
            copy.wait_send()
    assert len(slots) <= sems.shape[0] and local_count[0] <= locs.shape[0]


def fused_step(x, dy, wq, wk, wv, wo):
    any_spec = pl.BlockSpec(memory_space=pl.ANY)
    vmem_spec = pl.BlockSpec(memory_space=pltpu.VMEM)
    scratch = [
        pltpu.VMEM((SEQ, DIM), BF16),
        pltpu.VMEM((DIM, SEQ), BF16),
        pltpu.VMEM((NCH, SEQ, CH), BF16),
        pltpu.VMEM((DIM, HEADS, HD), BF16),
        pltpu.VMEM((2 * HEADS, DIM, HD), BF16),
        pltpu.VMEM((2, DIM, HD), BF16),
        pltpu.VMEM((HEADS * HD, DIM), BF16),
        pltpu.VMEM((SEQ, HEADS * HD), BF16),
        pltpu.VMEM((SEQ, HD), BF16),
        pltpu.VMEM((SEQ, HD), BF16),
        pltpu.VMEM((HD, SEQ), BF16),
        pltpu.VMEM((HD, SEQ), BF16),
        pltpu.VMEM((HEADS, SEQ, SEQ), F32),
        pltpu.VMEM((HEADS, SEQ, 2 * BLK), BF16),
        pltpu.VMEM((HEADS * HD, SEQ), BF16),
        pltpu.VMEM((HEADS * HD, 2 * BLK), F32),
        pltpu.VMEM((HEADS * HD, SEQ), BF16),
        pltpu.VMEM((2, SEQ, HD), F32),
        pltpu.VMEM((SEQ, HD), F32),
        pltpu.VMEM((SEQ, HD), BF16),
        pltpu.VMEM((SEQ, HD), BF16),
        pltpu.VMEM((2, SEQ, HD), BF16),
        pltpu.VMEM((HEADS, SEQ, HD), BF16),
        pltpu.VMEM((2, HEADS, BLK, HD), BF16),
        pltpu.VMEM((NCH // 2, HEADS * HD, CH), BF16),
        pltpu.VMEM((NCH // 2, HEADS * HD, CH), BF16),
        pltpu.VMEM((4, HEADS, HALF // 4, HD), BF16),
        pltpu.VMEM((4, HEADS, HALF // 4, HD), BF16),
        pltpu.VMEM((BLK, DIM), F32),
        pltpu.VMEM((NCH, BLK, CH), BF16),
        pltpu.VMEM((NCH, BLK, CH), BF16),
        pltpu.VMEM((2, 256, HD), BF16),
        pltpu.VMEM((2, 256, HD), BF16),
        pltpu.SemaphoreType.DMA((48,)),
        pltpu.SemaphoreType.DMA((48,)),
        pltpu.SemaphoreType.DMA((16,)),
    ]
    return pl.pallas_call(
        body,
        out_shape=(pltpu.VMEM((BLK, DIM), BF16),
                   pltpu.VMEM((HALF, HEADS, HD), F32),
                   pltpu.VMEM((256, HD), F32),
                   pltpu.VMEM((256, HD), F32),
                   pltpu.VMEM((HEADS * HD, HALF), F32)),
        in_specs=[any_spec] * 6,
        out_specs=(vmem_spec,) * 5,
        scratch_shapes=scratch,
        compiler_params=pltpu.CompilerParams(collective_id=0, has_side_effects=True,
                                             vmem_limit_bytes=58 * 2 ** 20),
        name='attention_backward',
    )(x, dy, wq, wk, wv, wo)


def solution(mesh):
    tok_spec = P(('pod', 'data'), 'model', None)

    def device_step(x_loc, dy_loc, w_q, w_k, w_v, w_o):
        dx, dwq, dwk, dwv, dwo = fused_step(x_loc[0], dy_loc[0], w_q, w_k[0], w_v[0],
                                            w_o.reshape(HEADS * HD, DIM))
        return dx[None], dwq, dwk, dwv, dwo.reshape(HEADS, HD, HALF)

    kv_rows = P(('pod', 'model', 'data'), None)
    return jax.shard_map(device_step, mesh=mesh,
                         in_specs=(tok_spec, tok_spec, P(None, 'model', None), P(), P(), P('model', None, None)),
                         out_specs=(tok_spec, P(('pod', 'data'), 'model', None), kv_rows, kv_rows,
                                    P(('pod', 'model'), None, 'data')),
                         check_vma=False)
```

```python
import functools

import jax
import jax.numpy as jnp
from jax import lax
from jax.experimental import pallas as pl
from jax.experimental.pallas import tpu as pltpu
from jax.sharding import PartitionSpec as P

F32 = jnp.float32
BF16 = jnp.bfloat16
SEQ = 1024
BLK = 256
DIM = 2048
HD = 256
HEADS = 2
CH = 256
NCH = DIM // CH
DXC = 512
NDX = DIM // DXC
PIECE = 64
NP = BLK // PIECE
HALF = DIM // 2
SCALE = HD ** -0.5
MESH = pl.DeviceIdType.MESH


def dot_nn(a, b):
    return lax.dot_general(a, b, (((1,), (0,)), ((), ())), preferred_element_type=F32)


def dot_nt(a, b):
    return lax.dot_general(a, b, (((1,), (1,)), ((), ())), preferred_element_type=F32)


def at(start, size, align=256):
    return pl.ds(pl.multiple_of(start, align), size)


def body(x_ref, dy_ref, wq_ref, wk_ref, wv_ref, wo_ref,
         dx_out, dwq_out, dwk_out, dwv_out, dwo_out,
         xb, x_t, dyb, wq_raw, wq4, wkv, wo, q, k, v, k_t, v_t, p_t, ds_t, o_t, do_acc, do_t,
         dkv, dkv_mate, dkv_send, dkv_part, dkv_full, dq, dq_mate,
         dwo_send, dwo_recv, dwq_send, dwq_recv,
         dx_own, dx_send, dx_recv, dwkv_send, dwkv_recv,
         sems, recvs, locs):
    model = lax.axis_index('model')
    data = lax.axis_index('data')
    chip = model // 2
    core = model % 2
    mate = {'model': chip * 2 + 1 - core}
    partner = {'model': (1 - chip) * 2 + core}
    peer = {'data': 1 - data}
    own_row = model * BLK
    mate_row = (chip * 2 + 1 - core) * BLK
    partner_row = ((1 - chip) * 2 + core) * BLK
    diag_row = ((1 - chip) * 2 + 1 - core) * BLK
    near = chip * 2 * BLK
    far = (1 - chip) * 2 * BLK

    groups = {}
    slots = {}
    devices = {}

    def send(name, src, dst, device, group=None, part=None):
        group = group or name
        devices[group] = device
        copy = pltpu.make_async_remote_copy(
            src_ref=src, dst_ref=dst, send_sem=sems.at[groups.setdefault(group, len(groups))],
            recv_sem=recvs.at[slots.setdefault(part or name, len(slots))],
            device_id=device, device_id_type=MESH)
        copy.start()

    def arrived(name, dst, device):
        with jax.named_scope('w_' + name):
            pltpu.make_async_remote_copy(
                src_ref=dst, dst_ref=dst, send_sem=sems.at[0],
                recv_sem=recvs.at[slots.setdefault(name, len(slots))],
                device_id=device, device_id_type=MESH).wait_recv()

    def sent(group, src):
        pltpu.make_async_remote_copy(src_ref=src, dst_ref=src, send_sem=sems.at[groups[group]], recv_sem=recvs.at[0],
                                     device_id=devices[group], device_id_type=MESH).wait_send()

    def local(src, dst, n):
        copy = pltpu.make_async_copy(src, dst, locs.at[n])
        copy.start()
        return copy

    def chunk_at(j):
        return lax.rem((1 - data) * (NCH // 2) + j, NCH)

    def x_piece(row, p):
        return at(row + p * PIECE, PIECE, PIECE)

    def send_dy(j):
        c = chunk_at(j)
        send(f'dy_far{j}', dy_ref.at[:, at(c * CH, CH)], dyb.at[c, at(own_row, BLK)], partner, 'dy_far')

    barrier = pltpu.get_barrier_semaphore()
    for device in (mate, partner, peer):
        pl.semaphore_signal(barrier, inc=1, device_id=device, device_id_type=MESH)
    loads = [local(x_ref, xb.at[at(own_row, BLK)], 0), local(wq_ref, wq_raw, 1),
             local(wk_ref, wkv.at[0], 2), local(wv_ref, wkv.at[1], 3)]
    with jax.named_scope('barrier'):
        pl.semaphore_wait(barrier, 3)

    for p in range(NP):
        send(f'x_far{p}', x_ref.at[pl.ds(p * PIECE, PIECE)], xb.at[x_piece(own_row, p)], partner, 'x_far')
    send('x_mate', x_ref, xb.at[at(own_row, BLK)], mate)
    late_load = local(wo_ref, wo, 4)
    for c in range(NCH):
        own_chunk = dyb.at[c, at(own_row, BLK)]
        local(dy_ref.at[:, c * CH:(c + 1) * CH], own_chunk, 5)
        send('dy_mate', dy_ref.at[:, c * CH:(c + 1) * CH], own_chunk, mate)

    def project(xr, pieces):
        def put(dst, lo, value):
            for row, size, off in pieces:
                dst[row, lo:lo + HD] = value[off:off + size]
        for h in range(HEADS):
            put(q, h * HD, dot_nn(xr, wq4[core * HEADS + h]).astype(BF16))
        for n, (dst, dst_t) in enumerate(((k, k_t), (v, v_t))):
            value = dot_nn(xr, wkv[n]).astype(BF16)
            put(dst, 0, value)

    def flip_x(first_row):
        def step(t, carry):
            cols = at(t * 256, 256)
            for r in range(2):
                rows = at(first_row + r * BLK, BLK)
                x_t[cols, rows] = xb[rows, cols].T
            return carry
        lax.fori_loop(0, DIM // 256, step, 0)

    def flip_kv(first_row):
        for r in range(2):
            rows = at(first_row + r * BLK, BLK)
            k_t[:, rows] = k[rows, :].T
            v_t[:, rows] = v[rows, :].T

    with jax.named_scope('loads'):
        for copy in loads:
            copy.wait()

    with jax.named_scope('relay'):
        def relay(r, carry):
            rows = at(r * 128, 128, 128)
            for h in range(HEADS):
                wq4[core * HEADS + h, rows, :] = wq_raw[rows, h, :]
            return carry
        lax.fori_loop(0, DIM // 128, relay, 0)
    send('wq_mate', wq4.at[pl.ds(core * HEADS, HEADS)], wq4.at[pl.ds(core * HEADS, HEADS)], mate)

    arrived('x_mate', xb.at[at(mate_row, BLK)], mate)
    with jax.named_scope('proj1'):
        def project_near(r, carry):
            rows = at(near + r * BLK, BLK)
            project(xb[rows, :], [(rows, BLK, 0)])
            return carry
        lax.fori_loop(0, 2, project_near, 0)
        flip_kv(near)

    def forward_x(p):
        block = xb.at[x_piece(partner_row, p)]
        arrived(f'x_far{p}', block, partner)
        send(f'x_fwd{p}', block, block, mate, 'x_fwd', f'x_fwd{p | 1}')

    def project_far(p):
        first = (p - 1) * PIECE
        arrived(f'x_fwd{p}', xb.at[at(diag_row + first, 2 * PIECE, PIECE)], mate)
        rows = [at(row + first, 2 * PIECE, PIECE) for row in (partner_row, diag_row)]
        xr = jnp.concatenate([xb[r, :] for r in rows], axis=0)
        with jax.named_scope('proj2'):
            project(xr, [(rows[0], 2 * PIECE, 0), (rows[1], 2 * PIECE, 2 * PIECE)])

    forward_x(0)
    with jax.named_scope('flip1'):
        flip_x(near)
    forward_x(1)
    project_far(1)
    late_load.wait()
    own_dy = dyb.at[:, at(own_row, BLK)]
    pltpu.make_async_copy(own_dy, own_dy, locs.at[5]).wait()
    arrived('dy_mate', dyb.at[:, at(mate_row, BLK)], mate)
    with jax.named_scope('do_near'):
        for half in range(HEADS):
            heads = slice(half * HD, (half + 1) * HD)
            acc = jnp.zeros((HD, 2 * BLK), F32)
            for c in range(NCH):
                acc += dot_nt(wo[heads, c * CH:(c + 1) * CH], dyb[c, at(near, 2 * BLK), :])
            do_t[heads, at(near, 2 * BLK)] = acc.astype(BF16)
        dkv[...] = jnp.zeros(dkv.shape, F32)
    forward_x(2)
    for j in range(NCH):
        send_dy(j)
    forward_x(3)
    project_far(3)
    flip_kv(far)

    def forward_dy(j):
        block = dyb.at[chunk_at(j), at(partner_row, BLK)]
        arrived(f'dy_far{j}', block, partner)
        send(f'dy_fwd{j}', block, block, mate, 'dy_fwd')

    forward_dy(0)
    mask = lax.broadcasted_iota(jnp.int32, (BLK, BLK), 0) <= lax.broadcasted_iota(jnp.int32, (BLK, BLK), 1)

    def forward_head(h, carry):
        heads = slice(h * HD, (h + 1) * HD) if isinstance(h, int) else at(h * HD, HD)
        for i in range(SEQ // BLK):
            cols = slice(i * BLK, (i + 1) * BLK)
            qi = q[cols, heads]
            parts = []
            for j in range(i + 1):
                s = dot_nt(k[j * BLK:(j + 1) * BLK, :], qi) * SCALE
                parts.append(jnp.where(mask, s, -jnp.inf) if j == i else s)
            top = functools.reduce(jnp.maximum, [jnp.max(s, axis=0, keepdims=True) for s in parts])
            parts = [jnp.exp(s - top) for s in parts]
            total = functools.reduce(jnp.add, [jnp.sum(s, axis=0, keepdims=True) for s in parts])
            inv = 1.0 / total
            out = jnp.zeros((HD, BLK), F32)
            for j in range(i + 1):
                prob = parts[j] * inv
                p_t[h, j * BLK:(j + 1) * BLK, cols] = prob
                out += dot_nn(v_t[:, j * BLK:(j + 1) * BLK], prob.astype(BF16))
            o_t[heads, cols] = out.astype(BF16)
        return carry
    with jax.named_scope('fwd'):
        for h in range(HEADS):
            forward_head(h, 0)

    def add_dkv(h, i, j, prob, ds):
        rows = slice(j * BLK, (j + 1) * BLK)
        cols = slice(i * BLK, (i + 1) * BLK)
        heads = slice(h * HD, (h + 1) * HD) if isinstance(h, int) else at(h * HD, HD)
        dkv[0, rows, :] += dot_nn(ds, q[cols, heads])
        dkv[1, rows, :] += dot_nt(prob.astype(BF16), do_t[heads, cols])

    def backward_block(h, i, keep):
        heads = slice(h * HD, (h + 1) * HD) if isinstance(h, int) else at(h * HD, HD)
        cols = slice(i * BLK, (i + 1) * BLK)
        doi = do_t[heads, cols]
        delta = jnp.sum(doi.astype(F32) * o_t[heads, cols].astype(F32), axis=0, keepdims=True)
        dqi = jnp.zeros((HD, BLK), F32)
        for j in range(i + 1):
            rows = slice(j * BLK, (j + 1) * BLK)
            prob = p_t[h, rows, cols]
            ds = (prob * (dot_nn(v[rows, :], doi) - delta)).astype(BF16)
            dqi += dot_nn(k_t[:, rows], ds)
            if keep:
                ds_t[h, rows, (i % 2) * BLK:(i % 2 + 1) * BLK] = ds
            else:
                add_dkv(h, i, j, prob, ds)
        dq[h, cols, :] = (dqi * SCALE).astype(BF16).T

    def over_heads(step):
        def one(h, carry):
            step(h)
            return carry
        lax.fori_loop(0, HEADS, one, 0)

    def take_chunk(j):
        c = chunk_at(j)
        arrived(f'dy_fwd{j}', dyb.at[c, at(diag_row, BLK)], mate)
        part = dot_nt(wo[:, at(c * CH, CH)], dyb[c, at(far, 2 * BLK), :])
        if j == 0:
            do_acc[...] = part
        elif j < NCH - 1:
            do_acc[...] += part
        else:
            do_t[:, at(far, 2 * BLK)] = (do_acc[...] + part).astype(BF16)
        if j < NCH // 2:
            dwo_send[j] = dot_nn(o_t[...], dyb[c]).astype(BF16)
            send(f'dwo{j}', dwo_send.at[j], dwo_recv.at[j], peer, 'dwo')

    forward_dy(1)
    take_chunk(0)
    forward_dy(2)
    take_chunk(1)
    take_chunk(2)
    forward_dy(3)

    for c in range(2):
        @pl.when(chip == c)
        def _(c=c):
            def step(h):
                for i in (2 * c, 2 * c + 1):
                    backward_block(h, i, False)
            with jax.named_scope('bwd_near'):
                over_heads(step)
    send('dq_near', dq.at[:, at(mate_row, BLK)], dq_mate.at[chip], mate, 'dq')
    forward_dy(4)
    take_chunk(3)
    forward_dy(5)
    take_chunk(4)
    take_chunk(5)
    with jax.named_scope('flip2'):
        flip_x(far)
    for j in range(6, NCH):
        forward_dy(j)
        take_chunk(j)

    for c in range(2):
        for first in range(2):
            @pl.when((chip == c) & (core == 1 - first))
            def _(c=c, first=first):
                with jax.named_scope('bwd_far0'):
                    for h in range(HEADS):
                        backward_block(h, 2 * (1 - c) + first, True)
    send('dq_far', dq.at[:, at(diag_row, BLK)], dq_mate.at[1 - chip], mate, 'dq')
    for c in range(2):
        for first in range(2):
            @pl.when((chip == c) & (core == 1 - first))
            def _(c=c, first=first):
                with jax.named_scope('bwd_far1'):
                    for h in range(HEADS):
                        backward_block(h, 2 * (1 - c) + 1 - first, True)
    arrived('wq_mate', wq4.at[pl.ds((1 - core) * HEADS, HEADS)], mate)
    arrived('dq_far', dq_mate.at[1 - chip], mate)

    def dx_cols(block, cols):
        rows = at((block * 2 + core) * BLK, BLK)
        acc = jnp.zeros((BLK, DXC), F32)
        for h in range(HEADS):
            acc += dot_nt(dq[h, rows, :], wq4[core * HEADS + h, cols, :])
            acc += dot_nt(dq_mate[block, h], wq4[(1 - core) * HEADS + h, cols, :])
        return acc

    def send_dx(j):
        dx_send[j] = dx_cols(1 - chip, slice(j * DXC, (j + 1) * DXC)).astype(BF16)
        send(f'dx{j}', dx_send.at[j], dx_recv.at[j], partner, 'dx')

    send_dx(0)
    send_dx(1)
    for c in range(2):
        @pl.when(chip == c)
        def _(c=c):
            def step(h):
                for i in (2 * (1 - c), 2 * (1 - c) + 1):
                    for j in range(i + 1):
                        rows = slice(j * BLK, (j + 1) * BLK)
                        add_dkv(h, i, j, p_t[h, rows, i * BLK:(i + 1) * BLK],
                                ds_t[h, rows, (i % 2) * BLK:(i % 2 + 1) * BLK])
            with jax.named_scope('dkv'):
                over_heads(step)
    send('dkv_mate', dkv.at[1 - core], dkv_mate, mate)

    def send_dwq(r):
        with jax.named_scope('dwq'):
            rows = at((1 - data) * HALF + r * 256, 256)
            for h in range(HEADS):
                dwq_send[r, h] = dot_nn(x_t[rows, :], dq[h]).astype(BF16)
            send(f'dwq{r}', dwq_send.at[r], dwq_recv.at[r], peer, 'dwq')
    send_dwq(0)
    arrived('dkv_mate', dkv_mate, mate)
    factor = jnp.where(core == 0, SCALE, 1.0).astype(F32)
    summed = (dkv[core] + dkv_mate[...]) * factor
    dkv_mate[...] = summed
    dkv_send[...] = summed.astype(BF16)
    send('dkv_far', dkv_send, dkv_part, partner)
    send_dx(2)
    send_dx(3)
    for r in range(1, 4):
        send_dwq(r)

    arrived('dq_near', dq_mate.at[chip], mate)
    for j in range(NDX):
        dx_own[:, j * DXC:(j + 1) * DXC] = dx_cols(chip, slice(j * DXC, (j + 1) * DXC))
    for j in range(NCH // 2):
        arrived(f'dwo{j}', dwo_recv.at[j], peer)
        cols = slice(j * CH, (j + 1) * CH)
        dwo_out[:, cols] = dot_nn(o_t[...], dyb[chunk_at(NCH // 2 + j)]) + dwo_recv[j].astype(F32)

    arrived('dkv_far', dkv_part, partner)
    dkv_full[core] = (dkv_mate[...] + dkv_part[...].astype(F32)).astype(BF16)
    send('dkv_full', dkv_full.at[core], dkv_full.at[core], mate)
    arrived('dkv_full', dkv_full.at[1 - core], mate)
    for n in range(2):
        peer_rows = at((model * 2 + 1 - data) * 256, 256)
        dwkv_send[n] = dot_nn(x_t[peer_rows, :], dkv_full[n]).astype(BF16)
    send('dwkv', dwkv_send, dwkv_recv, peer)
    kept_rows = at((model * 2 + data) * 256, 256)
    dwk_out[...] = dot_nn(x_t[kept_rows, :], dkv_full[0])
    dwv_out[...] = dot_nn(x_t[kept_rows, :], dkv_full[1])
    for j in range(NDX):
        cols = slice(j * DXC, (j + 1) * DXC)
        dx_own[:, cols] += (dot_nt(dkv_full[0, at(own_row, BLK), :], wkv[0, cols, :])
                            + dot_nt(dkv_full[1, at(own_row, BLK), :], wkv[1, cols, :]))

    def finish_dx(j):
        arrived(f'dx{j}', dx_recv.at[j], partner)
        cols = slice(j * DXC, (j + 1) * DXC)
        dx_out[:, cols] = (dx_own[:, cols] + dx_recv[j].astype(F32)).astype(BF16)

    finish_dx(0)
    finish_dx(1)
    for r in range(4):
        arrived(f'dwq{r}', dwq_recv.at[r], peer)
        with jax.named_scope('dwq_sum'):
            rows = at(data * HALF + r * 256, 256)
            for h in range(HEADS):
                value = dot_nn(x_t[rows, :], dq[h]) + dwq_recv[r, h].astype(F32)
                dwq_out[r * 256:(r + 1) * 256, h, :] = value
    finish_dx(2)
    arrived('dwkv', dwkv_recv, peer)
    dwk_out[...] += dwkv_recv[0].astype(F32)
    dwv_out[...] += dwkv_recv[1].astype(F32)
    finish_dx(3)
    with jax.named_scope('sends'):
        sent('x_far', x_ref)
        sent('x_mate', x_ref)
        sent('dy_far', dy_ref)
        sent('dy_mate', dy_ref)
        sent('wq_mate', wq4.at[pl.ds(core * HEADS, HEADS)])
        sent('x_fwd', xb.at[at(partner_row, BLK)])
        sent('dy_fwd', dyb.at[:, at(partner_row, BLK)])
        sent('dwo', dwo_send)
        sent('dq', dq_mate)
        sent('dx', dx_send)
        sent('dkv_mate', dkv_mate)
        sent('dkv_far', dkv_send)
        sent('dkv_full', dkv_send)
        sent('dwq', dwq_send)
        sent('dwkv', dwkv_send)
    assert len(groups) == sems.shape[0] and len(slots) == recvs.shape[0]


def fused_step(x, dy, wq, wk, wv, wo):
    any_spec = pl.BlockSpec(memory_space=pl.ANY)
    vmem_spec = pl.BlockSpec(memory_space=pltpu.VMEM)
    scratch = [
        pltpu.VMEM((SEQ, DIM), BF16),
        pltpu.VMEM((DIM, SEQ), BF16),
        pltpu.VMEM((NCH, SEQ, CH), BF16),
        pltpu.VMEM((DIM, HEADS, HD), BF16),
        pltpu.VMEM((2 * HEADS, DIM, HD), BF16),
        pltpu.VMEM((2, DIM, HD), BF16),
        pltpu.VMEM((HEADS * HD, DIM), BF16),
        pltpu.VMEM((SEQ, HEADS * HD), BF16),
        pltpu.VMEM((SEQ, HD), BF16),
        pltpu.VMEM((SEQ, HD), BF16),
        pltpu.VMEM((HD, SEQ), BF16),
        pltpu.VMEM((HD, SEQ), BF16),
        pltpu.VMEM((HEADS, SEQ, SEQ), F32),
        pltpu.VMEM((HEADS, SEQ, 2 * BLK), BF16),
        pltpu.VMEM((HEADS * HD, SEQ), BF16),
        pltpu.VMEM((HEADS * HD, 2 * BLK), F32),
        pltpu.VMEM((HEADS * HD, SEQ), BF16),
        pltpu.VMEM((2, SEQ, HD), F32),
        pltpu.VMEM((SEQ, HD), F32),
        pltpu.VMEM((SEQ, HD), BF16),
        pltpu.VMEM((SEQ, HD), BF16),
        pltpu.VMEM((2, SEQ, HD), BF16),
        pltpu.VMEM((HEADS, SEQ, HD), BF16),
        pltpu.VMEM((2, HEADS, BLK, HD), BF16),
        pltpu.VMEM((NCH // 2, HEADS * HD, CH), BF16),
        pltpu.VMEM((NCH // 2, HEADS * HD, CH), BF16),
        pltpu.VMEM((4, HEADS, HALF // 4, HD), BF16),
        pltpu.VMEM((4, HEADS, HALF // 4, HD), BF16),
        pltpu.VMEM((BLK, DIM), F32),
        pltpu.VMEM((NDX, BLK, DXC), BF16),
        pltpu.VMEM((NDX, BLK, DXC), BF16),
        pltpu.VMEM((2, 256, HD), BF16),
        pltpu.VMEM((2, 256, HD), BF16),
        pltpu.SemaphoreType.DMA((15,)),
        pltpu.SemaphoreType.DMA((43,)),
        pltpu.SemaphoreType.DMA((6,)),
    ]
    return pl.pallas_call(
        body,
        out_shape=(pltpu.VMEM((BLK, DIM), BF16),
                   pltpu.VMEM((HALF, HEADS, HD), F32),
                   pltpu.VMEM((256, HD), F32),
                   pltpu.VMEM((256, HD), F32),
                   pltpu.VMEM((HEADS * HD, HALF), F32)),
        in_specs=[any_spec] * 6,
        out_specs=(vmem_spec,) * 5,
        scratch_shapes=scratch,
        compiler_params=pltpu.CompilerParams(collective_id=0, has_side_effects=True,
                                             vmem_limit_bytes=58 * 2 ** 20),
        name='attention_backward',
    )(x, dy, wq, wk, wv, wo)


def flush_body(*refs):
    sources, results, sems = refs[:5], refs[5:10], refs[10]
    copies = [pltpu.make_async_copy(a, b, sems.at[n]) for n, (a, b) in enumerate(zip(sources, results))]
    for copy in copies:
        copy.start()
    for copy in copies:
        copy.wait()


def flush(*arrays):
    any_spec = pl.BlockSpec(memory_space=pl.ANY)
    return pl.pallas_call(
        flush_body,
        out_shape=tuple(jax.ShapeDtypeStruct(a.shape, a.dtype) for a in arrays),
        in_specs=[any_spec] * 5,
        out_specs=(any_spec,) * 5,
        scratch_shapes=[pltpu.SemaphoreType.DMA((5,))],
        compiler_params=pltpu.CompilerParams(vmem_limit_bytes=2 ** 20),
        name='write_results',
    )(*arrays)


def solution(mesh):
    tok_spec = P(('pod', 'data'), 'model', None)

    def device_step(x_loc, dy_loc, w_q, w_k, w_v, w_o):
        dx, dwq, dwk, dwv, dwo = flush(*fused_step(x_loc[0], dy_loc[0], w_q, w_k[0], w_v[0],
                                                   w_o.reshape(HEADS * HD, DIM)))
        return dx[None], dwq, dwk, dwv, dwo.reshape(HEADS, HD, HALF)

    kv_rows = P(('pod', 'model', 'data'), None)
    return jax.shard_map(device_step, mesh=mesh,
                         in_specs=(tok_spec, tok_spec, P(None, 'model', None), P(), P(), P('model', None, None)),
                         out_specs=(tok_spec, P(('pod', 'data'), 'model', None), kv_rows, kv_rows,
                                    P(('pod', 'model'), None, 'data')),
                         check_vma=False)
```

```python
import functools

import jax
import jax.numpy as jnp
from jax import lax
from jax.experimental import pallas as pl
from jax.experimental.pallas import tpu as pltpu
from jax.sharding import PartitionSpec as P

F32 = jnp.float32
BF16 = jnp.bfloat16
SEQ = 1024
BLK = 256
DIM = 2048
HD = 256
HEADS = 2
CH = 256
NCH = DIM // CH
DXC = 512
NDX = DIM // DXC
GRP = 128
PIECE = 64
NP = BLK // PIECE
HALF = DIM // 2
SCALE = HD ** -0.5
MESH = pl.DeviceIdType.MESH


def dot_nn(a, b):
    return lax.dot_general(a, b, (((1,), (0,)), ((), ())), preferred_element_type=F32)


def dot_nt(a, b):
    return lax.dot_general(a, b, (((1,), (1,)), ((), ())), preferred_element_type=F32)


def at(start, size, align=256):
    return pl.ds(pl.multiple_of(start, align), size)


def body(x_ref, dy_ref, wq_ref, wk_ref, wv_ref, wo_ref,
         dx_out, dwq_out, dwk_out, dwv_out, dwo_out,
         xb, x_t, dyb, wq_raw, wq4, wkv, wo, q, k, v, k_t, v_t, p_t, p_inv, ds_t, o_t, do_acc, do_t,
         dkv, dkv_mate, dkv_send, dkv_part, dkv_full, dq, dq_mate,
         dwo_send, dwo_recv, dwq_send, dwq_recv,
         dx_own, dx_send, dx_recv, dwkv_send, dwkv_recv,
         sems, recvs, locs):
    model = lax.axis_index('model')
    data = lax.axis_index('data')
    chip = model // 2
    core = model % 2
    mate = {'model': chip * 2 + 1 - core}
    partner = {'model': (1 - chip) * 2 + core}
    peer = {'data': 1 - data}
    own_row = model * BLK
    mate_row = (chip * 2 + 1 - core) * BLK
    partner_row = ((1 - chip) * 2 + core) * BLK
    diag_row = ((1 - chip) * 2 + 1 - core) * BLK
    near = chip * 2 * BLK
    far = (1 - chip) * 2 * BLK

    groups = {}
    slots = {}
    devices = {}

    def send(name, src, dst, device, group=None, part=None):
        group = group or name
        devices[group] = device
        copy = pltpu.make_async_remote_copy(
            src_ref=src, dst_ref=dst, send_sem=sems.at[groups.setdefault(group, len(groups))],
            recv_sem=recvs.at[slots.setdefault(part or name, len(slots))],
            device_id=device, device_id_type=MESH)
        copy.start()

    def arrived(name, dst, device):
        with jax.named_scope('w_' + name):
            pltpu.make_async_remote_copy(
                src_ref=dst, dst_ref=dst, send_sem=sems.at[0],
                recv_sem=recvs.at[slots.setdefault(name, len(slots))],
                device_id=device, device_id_type=MESH).wait_recv()

    def sent(group, src):
        pltpu.make_async_remote_copy(src_ref=src, dst_ref=src, send_sem=sems.at[groups[group]], recv_sem=recvs.at[0],
                                     device_id=devices[group], device_id_type=MESH).wait_send()

    def local(src, dst, n):
        copy = pltpu.make_async_copy(src, dst, locs.at[n])
        copy.start()
        return copy

    def chunk_at(j):
        return lax.rem((1 - data) * (NCH // 2) + j, NCH)

    def x_piece(row, p):
        return at(row + p * PIECE, PIECE, PIECE)

    late = pl.ds(data * (NCH // 2), NCH // 2)

    def group_row(row, g):
        return at(row + g * GRP, GRP, GRP)

    def send_dy():
        for j in range(NCH // 2):
            c = chunk_at(j)
            send(f'dy_far{j}', dy_ref.at[:, at(c * CH, CH)], dyb.at[c, at(own_row, BLK)], partner, 'dy_far')
        for g in range(2):
            for j in range(NCH // 2):
                c = data * (NCH // 2) + j
                send(f'dy_late{g}', dy_ref.at[g * GRP:(g + 1) * GRP, at(c * CH, CH)],
                     dyb.at[c, group_row(own_row, g)], partner, 'dy_far')

    barrier = pltpu.get_barrier_semaphore()
    for device in (mate, partner, peer):
        pl.semaphore_signal(barrier, inc=1, device_id=device, device_id_type=MESH)
    loads = [local(x_ref, xb.at[at(own_row, BLK)], 0), local(wq_ref, wq_raw, 1),
             local(wk_ref, wkv.at[0], 2), local(wv_ref, wkv.at[1], 3)]
    with jax.named_scope('barrier'):
        pl.semaphore_wait(barrier, 3)

    for p in range(NP):
        send(f'x_far{p}', x_ref.at[pl.ds(p * PIECE, PIECE)], xb.at[x_piece(own_row, p)], partner, 'x_far')
    send('x_mate', x_ref, xb.at[at(own_row, BLK)], mate)
    late_load = local(wo_ref, wo, 4)
    for c in range(NCH):
        own_chunk = dyb.at[c, at(own_row, BLK)]
        local(dy_ref.at[:, c * CH:(c + 1) * CH], own_chunk, 5)
        send('dy_mate', dy_ref.at[:, c * CH:(c + 1) * CH], own_chunk, mate)

    def project(xr, pieces):
        def put(dst, lo, value):
            for row, size, off in pieces:
                dst[row, lo:lo + HD] = value[off:off + size]
        for h in range(HEADS):
            put(q, h * HD, dot_nn(xr, wq4[core * HEADS + h]).astype(BF16))
        for n, (dst, dst_t) in enumerate(((k, k_t), (v, v_t))):
            value = dot_nn(xr, wkv[n]).astype(BF16)
            put(dst, 0, value)

    def flip_x(first_row):
        def step(t, carry):
            cols = at(t * 256, 256)
            for r in range(2):
                rows = at(first_row + r * BLK, BLK)
                x_t[cols, rows] = xb[rows, cols].T
            return carry
        lax.fori_loop(0, DIM // 256, step, 0)

    def flip_kv(first_row):
        for r in range(2):
            rows = at(first_row + r * BLK, BLK)
            k_t[:, rows] = k[rows, :].T
            v_t[:, rows] = v[rows, :].T

    with jax.named_scope('loads'):
        for copy in loads:
            copy.wait()

    with jax.named_scope('relay'):
        def relay(r, carry):
            rows = at(r * 128, 128, 128)
            for h in range(HEADS):
                wq4[core * HEADS + h, rows, :] = wq_raw[rows, h, :]
            return carry
        lax.fori_loop(0, DIM // 128, relay, 0)
    send('wq_mate', wq4.at[pl.ds(core * HEADS, HEADS)], wq4.at[pl.ds(core * HEADS, HEADS)], mate)

    arrived('x_mate', xb.at[at(mate_row, BLK)], mate)
    with jax.named_scope('proj1'):
        def project_near(r, carry):
            rows = at(near + r * BLK, BLK)
            project(xb[rows, :], [(rows, BLK, 0)])
            return carry
        lax.fori_loop(0, 2, project_near, 0)
        flip_kv(near)

    def forward_x(p):
        block = xb.at[x_piece(partner_row, p)]
        arrived(f'x_far{p}', block, partner)
        send(f'x_fwd{p}', block, block, mate, 'x_fwd', f'x_fwd{max(p, 1)}')

    def project_far(p):
        first, size = (0, 2 * PIECE) if p == 1 else (p * PIECE, PIECE)
        arrived(f'x_fwd{p}', xb.at[at(diag_row + first, size, PIECE)], mate)
        rows = [at(row + first, size, PIECE) for row in (partner_row, diag_row)]
        xr = jnp.concatenate([xb[r, :] for r in rows], axis=0)
        with jax.named_scope('proj2'):
            project(xr, [(rows[0], size, 0), (rows[1], size, size)])

    forward_x(0)
    with jax.named_scope('flip1'):
        flip_x(near)
    forward_x(1)
    project_far(1)
    late_load.wait()
    own_dy = dyb.at[:, at(own_row, BLK)]
    pltpu.make_async_copy(own_dy, own_dy, locs.at[5]).wait()
    arrived('dy_mate', dyb.at[:, at(mate_row, BLK)], mate)
    with jax.named_scope('do_near'):
        for half in range(HEADS):
            heads = slice(half * HD, (half + 1) * HD)
            acc = jnp.zeros((HD, 2 * BLK), F32)
            for c in range(NCH):
                acc += dot_nt(wo[heads, c * CH:(c + 1) * CH], dyb[c, at(near, 2 * BLK), :])
            do_t[heads, at(near, 2 * BLK)] = acc.astype(BF16)
        dkv[...] = jnp.zeros(dkv.shape, F32)
    forward_x(2)

    @pl.when(core == 0)
    def _():
        send_dy()
    project_far(2)
    forward_x(3)

    @pl.when(core == 1)
    def _():
        send_dy()
    project_far(3)
    flip_kv(far)

    def forward_dy(j):
        block = dyb.at[chunk_at(j), at(partner_row, BLK)]
        arrived(f'dy_far{j}', block, partner)
        send(f'dy_fwd{j}', block, block, mate, 'dy_fwd')

    mask = lax.broadcasted_iota(jnp.int32, (BLK, BLK), 0) <= lax.broadcasted_iota(jnp.int32, (BLK, BLK), 1)

    def forward_block(h, i):
        heads = slice(h * HD, (h + 1) * HD)
        cols = slice(i * BLK, (i + 1) * BLK)
        rows = (i + 1) * BLK
        qs = q[cols, heads] * jnp.asarray(SCALE, BF16)
        p_t[h, i * BLK:rows, cols] = jnp.where(mask, dot_nt(k[i * BLK:rows, :], qs), -jnp.inf)
        if i:
            p_t[h, :i * BLK, cols] = dot_nt(k[:i * BLK, :], qs)
        top = jnp.max(p_t[h, :rows, cols], axis=0, keepdims=True)
        e = jnp.exp(p_t[h, :rows, cols] - top)
        p_t[h, :rows, cols] = e
        inv = 1.0 / jnp.sum(e, axis=0, keepdims=True)
        p_inv[h, :, cols] = inv
        prob = (p_t[h, :rows, cols] * inv).astype(BF16)
        o_t[heads, cols] = dot_nn(v_t[:, :rows], prob).astype(BF16)
    with jax.named_scope('fwd'):
        for i in range(3):
            for h in range(HEADS):
                forward_block(h, i)
        forward_dy(0)
        for h in range(HEADS):
            forward_block(h, 3)

    def add_dkv(h, i, j, prob, ds):
        rows = slice(j * BLK, (j + 1) * BLK)
        cols = slice(i * BLK, (i + 1) * BLK)
        heads = at(h * HD, HD)
        dkv[0, rows, :] += dot_nn(ds, q[cols, heads])
        dkv[1, rows, :] += dot_nt(prob.astype(BF16), do_t[heads, cols])

    def backward_block(h, i, lo, size, keep):
        heads = slice(h * HD, (h + 1) * HD) if isinstance(h, int) else at(h * HD, HD)
        cols = slice(i * BLK + lo, i * BLK + lo + size)
        doi = do_t[heads, cols]
        delta = jnp.sum(doi.astype(F32) * o_t[heads, cols].astype(F32), axis=0, keepdims=True)
        inv = p_inv[h, :, cols]
        dqi = jnp.zeros((HD, size), F32)
        for j in range(i + 1):
            rows = slice(j * BLK, (j + 1) * BLK)
            prob = p_t[h, rows, cols] * inv
            ds = (prob * (dot_nn(v[rows, :], doi) - delta)).astype(BF16)
            dqi += dot_nn(k_t[:, rows], ds)
            if keep:
                ds_t[h, rows, (i % 2) * BLK + lo:(i % 2) * BLK + lo + size] = ds
            else:
                add_dkv(h, i, j, prob, ds)
        dq[h, cols, :] = (dqi * SCALE).astype(BF16).T

    def over_heads(step):
        def one(h, carry):
            step(h)
            return carry
        lax.fori_loop(0, HEADS, one, 0)

    def take_chunk(j):
        c = chunk_at(j)
        arrived(f'dy_fwd{j}', dyb.at[c, at(diag_row, BLK)], mate)
        part = dot_nt(wo[:, at(c * CH, CH)], dyb[c, at(far, 2 * BLK), :])
        if j == 0:
            do_acc[...] = part
        else:
            do_acc[...] += part
        dwo_send[j] = dot_nn(o_t[...], dyb[c]).astype(BF16)
        send('dwo', dwo_send.at[j], dwo_recv.at[j], peer)

    def forward_group(g):
        block = dyb.at[late, group_row(partner_row, g)]
        arrived(f'dy_late{g}', block, partner)
        send(f'dy_lfwd{g}', block, block, mate, 'dy_lfwd')

    def finish_do(row, g):
        with jax.named_scope('do_late'):
            cols = group_row(row, g)
            acc = do_acc[:, group_row(row - far, g)]
            for j in range(NCH // 2):
                c = data * (NCH // 2) + j
                acc += dot_nt(wo[:, at(c * CH, CH)], dyb[c, cols, :])
            do_t[:, cols] = acc.astype(BF16)

    def backward_far(g):
        def block_of(diag):
            for c in range(2):
                for n in range(2):
                    @pl.when((chip == c) & (core == n))
                    def _(c=c, n=n):
                        with jax.named_scope('bwd_far'):
                            for h in range(HEADS):
                                backward_block(h, 2 * (1 - c) + (1 - n if diag else n), g * GRP, GRP, True)
        finish_do(partner_row, g)
        arrived(f'dy_lfwd{g}', dyb.at[late, group_row(diag_row, g)], mate)
        finish_do(diag_row, g)
        block_of(True)
        send(f'dq_far{g}', dq.at[:, group_row(diag_row, g)], dq_mate.at[1 - chip, :, g * GRP:(g + 1) * GRP], mate, 'dq')
        block_of(False)
        arrived(f'dq_far{g}', dq_mate.at[1 - chip, :, g * GRP:(g + 1) * GRP], mate)

    def dx_cols(block, lo, size, cols):
        rows = at((block * 2 + core) * BLK + lo, size, GRP)
        acc = jnp.zeros((size, cols.stop - cols.start), F32)
        for h in range(HEADS):
            acc += dot_nt(dq[h, rows, :], wq4[core * HEADS + h, cols, :])
            acc += dot_nt(dq_mate[block, h, lo:lo + size], wq4[(1 - core) * HEADS + h, cols, :])
        return acc

    def send_dx(g):
        with jax.named_scope('dx'):
            for j in range(NDX):
                n = g * NDX + j
                dx_send[n] = dx_cols(1 - chip, g * GRP, GRP, slice(j * DXC, (j + 1) * DXC)).astype(BF16)
                send(f'dx{max(n, NDX)}' if g else 'dx', dx_send.at[n], dx_recv.at[n], partner, 'dx')

    take_chunk(0)
    forward_dy(1)
    forward_dy(2)
    take_chunk(1)
    take_chunk(2)
    forward_dy(3)

    for c in range(2):
        @pl.when(chip == c)
        def _(c=c):
            def step(h):
                for i in (2 * c, 2 * c + 1):
                    backward_block(h, i, 0, BLK, False)
            with jax.named_scope('bwd_near'):
                over_heads(step)
    send('dq_near', dq.at[:, at(mate_row, BLK)], dq_mate.at[chip], mate, 'dq')
    take_chunk(3)
    with jax.named_scope('flip2'):
        flip_x(far)
    arrived('wq_mate', wq4.at[pl.ds((1 - core) * HEADS, HEADS)], mate)
    forward_group(0)
    backward_far(0)
    send_dx(0)
    forward_group(1)
    backward_far(1)

    def send_dwq(r):
        with jax.named_scope('dwq'):
            rows = at((1 - data) * HALF + r * 256, 256)
            for h in range(HEADS):
                dwq_send[r, h] = dot_nn(x_t[rows, :], dq[h]).astype(BF16)
            send(f'dwq{r}', dwq_send.at[r], dwq_recv.at[r], peer, 'dwq')
    send_dwq(0)
    for c in range(2):
        @pl.when(chip == c)
        def _(c=c):
            def step(h):
                for i in (2 * (1 - c), 2 * (1 - c) + 1):
                    cols = slice(i * BLK, (i + 1) * BLK)
                    for j in range(i + 1):
                        rows = slice(j * BLK, (j + 1) * BLK)
                        add_dkv(h, i, j, p_t[h, rows, cols] * p_inv[h, :, cols],
                                ds_t[h, rows, (i % 2) * BLK:(i % 2 + 1) * BLK])
            with jax.named_scope('dkv'):
                over_heads(step)
    send('dkv_mate', dkv.at[1 - core], dkv_mate, mate)

    for r in range(1, 4):
        send_dwq(r)
    arrived('dkv_mate', dkv_mate, mate)
    factor = jnp.where(core == 0, SCALE, 1.0).astype(F32)
    summed = (dkv[core] + dkv_mate[...]) * factor
    dkv_mate[...] = summed
    dkv_send[...] = summed.astype(BF16)
    send('dkv_far', dkv_send, dkv_part, partner)
    send_dx(1)

    arrived('dq_near', dq_mate.at[chip], mate)
    for j in range(4):
        cols = slice(j * 512, (j + 1) * 512)
        dx_own[:, cols] = dx_cols(chip, 0, BLK, cols)
    arrived('dwo', dwo_recv, peer)
    for j in range(NCH // 2):
        cols = slice(j * CH, (j + 1) * CH)
        dwo_out[:, cols] = dot_nn(o_t[...], dyb[chunk_at(NCH // 2 + j)]) + dwo_recv[j].astype(F32)

    arrived('dkv_far', dkv_part, partner)
    dkv_full[core] = (dkv_mate[...] + dkv_part[...].astype(F32)).astype(BF16)
    send('dkv_full', dkv_full.at[core], dkv_full.at[core], mate)
    arrived('dkv_full', dkv_full.at[1 - core], mate)
    for n in range(2):
        peer_rows = at((model * 2 + 1 - data) * 256, 256)
        dwkv_send[n] = dot_nn(x_t[peer_rows, :], dkv_full[n]).astype(BF16)
    send('dwkv', dwkv_send, dwkv_recv, peer)
    kept_rows = at((model * 2 + data) * 256, 256)
    dwk_out[...] = dot_nn(x_t[kept_rows, :], dkv_full[0])
    dwv_out[...] = dot_nn(x_t[kept_rows, :], dkv_full[1])
    for j in range(4):
        cols = slice(j * 512, (j + 1) * 512)
        dx_own[:, cols] += (dot_nt(dkv_full[0, at(own_row, BLK), :], wkv[0, cols, :])
                            + dot_nt(dkv_full[1, at(own_row, BLK), :], wkv[1, cols, :]))

    def finish_dx(n):
        rows = slice(n // NDX * GRP, (n // NDX + 1) * GRP)
        cols = slice(n % NDX * DXC, (n % NDX + 1) * DXC)
        dx_out[rows, cols] = (dx_own[rows, cols] + dx_recv[n].astype(F32)).astype(BF16)

    arrived('dx', dx_recv.at[:NDX], partner)
    for n in range(NDX):
        finish_dx(n)
    for r in range(4):
        arrived(f'dwq{r}', dwq_recv.at[r], peer)
        with jax.named_scope('dwq_sum'):
            rows = at(data * HALF + r * 256, 256)
            for h in range(HEADS):
                value = dot_nn(x_t[rows, :], dq[h]) + dwq_recv[r, h].astype(F32)
                dwq_out[r * 256:(r + 1) * 256, h, :] = value
    for n in range(NDX, 2 * NDX):
        arrived(f'dx{n}', dx_recv.at[n], partner)
        finish_dx(n)
    arrived('dwkv', dwkv_recv, peer)
    dwk_out[...] += dwkv_recv[0].astype(F32)
    dwv_out[...] += dwkv_recv[1].astype(F32)
    with jax.named_scope('sends'):
        sent('x_far', x_ref)
        sent('x_mate', x_ref)
        sent('dy_far', dy_ref)
        sent('dy_mate', dy_ref)
        sent('wq_mate', wq4.at[pl.ds(core * HEADS, HEADS)])
        sent('x_fwd', xb.at[at(partner_row, BLK)])
        sent('dy_fwd', dyb.at[late, at(partner_row, BLK)])
        sent('dy_lfwd', dyb.at[late, at(partner_row, BLK)])
        sent('dwo', dwo_send)
        sent('dq', dq_mate)
        sent('dx', dx_send)
        sent('dkv_mate', dkv_mate)
        sent('dkv_far', dkv_send)
        sent('dkv_full', dkv_send)
        sent('dwq', dwq_send)
        sent('dwkv', dwkv_send)
    assert len(groups) == sems.shape[0] and len(slots) == recvs.shape[0]


def fused_step(x, dy, wq, wk, wv, wo):
    any_spec = pl.BlockSpec(memory_space=pl.ANY)
    vmem_spec = pl.BlockSpec(memory_space=pltpu.VMEM)
    scratch = [
        pltpu.VMEM((SEQ, DIM), BF16),
        pltpu.VMEM((DIM, SEQ), BF16),
        pltpu.VMEM((NCH, SEQ, CH), BF16),
        pltpu.VMEM((DIM, HEADS, HD), BF16),
        pltpu.VMEM((2 * HEADS, DIM, HD), BF16),
        pltpu.VMEM((2, DIM, HD), BF16),
        pltpu.VMEM((HEADS * HD, DIM), BF16),
        pltpu.VMEM((SEQ, HEADS * HD), BF16),
        pltpu.VMEM((SEQ, HD), BF16),
        pltpu.VMEM((SEQ, HD), BF16),
        pltpu.VMEM((HD, SEQ), BF16),
        pltpu.VMEM((HD, SEQ), BF16),
        pltpu.VMEM((HEADS, SEQ, SEQ), F32),
        pltpu.VMEM((HEADS, 1, SEQ), F32),
        pltpu.VMEM((HEADS, SEQ, 2 * BLK), BF16),
        pltpu.VMEM((HEADS * HD, SEQ), BF16),
        pltpu.VMEM((HEADS * HD, 2 * BLK), F32),
        pltpu.VMEM((HEADS * HD, SEQ), BF16),
        pltpu.VMEM((2, SEQ, HD), F32),
        pltpu.VMEM((SEQ, HD), F32),
        pltpu.VMEM((SEQ, HD), BF16),
        pltpu.VMEM((SEQ, HD), BF16),
        pltpu.VMEM((2, SEQ, HD), BF16),
        pltpu.VMEM((HEADS, SEQ, HD), BF16),
        pltpu.VMEM((2, HEADS, BLK, HD), BF16),
        pltpu.VMEM((NCH // 2, HEADS * HD, CH), BF16),
        pltpu.VMEM((NCH // 2, HEADS * HD, CH), BF16),
        pltpu.VMEM((4, HEADS, HALF // 4, HD), BF16),
        pltpu.VMEM((4, HEADS, HALF // 4, HD), BF16),
        pltpu.VMEM((BLK, DIM), F32),
        pltpu.VMEM((2 * NDX, GRP, DXC), BF16),
        pltpu.VMEM((2 * NDX, GRP, DXC), BF16),
        pltpu.VMEM((2, 256, HD), BF16),
        pltpu.VMEM((2, 256, HD), BF16),
        pltpu.SemaphoreType.DMA((16,)),
        pltpu.SemaphoreType.DMA((39,)),
        pltpu.SemaphoreType.DMA((6,)),
    ]
    return pl.pallas_call(
        body,
        out_shape=(pltpu.VMEM((BLK, DIM), BF16),
                   pltpu.VMEM((HALF, HEADS, HD), F32),
                   pltpu.VMEM((256, HD), F32),
                   pltpu.VMEM((256, HD), F32),
                   pltpu.VMEM((HEADS * HD, HALF), F32)),
        in_specs=[any_spec] * 6,
        out_specs=(vmem_spec,) * 5,
        scratch_shapes=scratch,
        compiler_params=pltpu.CompilerParams(collective_id=0, has_side_effects=True,
                                             vmem_limit_bytes=58 * 2 ** 20),
        name='attention_backward',
    )(x, dy, wq, wk, wv, wo)


def flush_body(*refs):
    sources, results, sems = refs[:5], refs[5:10], refs[10]
    copies = [pltpu.make_async_copy(a, b, sems.at[n]) for n, (a, b) in enumerate(zip(sources, results))]
    for copy in copies:
        copy.start()
    for copy in copies:
        copy.wait()


def flush(*arrays):
    any_spec = pl.BlockSpec(memory_space=pl.ANY)
    return pl.pallas_call(
        flush_body,
        out_shape=tuple(jax.ShapeDtypeStruct(a.shape, a.dtype) for a in arrays),
        in_specs=[any_spec] * 5,
        out_specs=(any_spec,) * 5,
        scratch_shapes=[pltpu.SemaphoreType.DMA((5,))],
        compiler_params=pltpu.CompilerParams(vmem_limit_bytes=2 ** 20),
        name='write_results',
    )(*arrays)


def solution(mesh):
    tok_spec = P(('pod', 'data'), 'model', None)

    def device_step(x_loc, dy_loc, w_q, w_k, w_v, w_o):
        dx, dwq, dwk, dwv, dwo = flush(*fused_step(x_loc[0], dy_loc[0], w_q, w_k[0], w_v[0],
                                                   w_o.reshape(HEADS * HD, DIM)))
        return dx[None], dwq, dwk, dwv, dwo.reshape(HEADS, HD, HALF)

    kv_rows = P(('pod', 'model', 'data'), None)
    return jax.shard_map(device_step, mesh=mesh,
                         in_specs=(tok_spec, tok_spec, P(None, 'model', None), P(), P(), P('model', None, None)),
                         out_specs=(tok_spec, P(('pod', 'data'), 'model', None), kv_rows, kv_rows,
                                    P(('pod', 'model'), None, 'data')),
                         check_vma=False)
```

```python
import functools

import jax
import jax.numpy as jnp
from jax import lax
from jax.experimental import pallas as pl
from jax.experimental.pallas import tpu as pltpu
from jax.sharding import PartitionSpec as P

F32 = jnp.float32
BF16 = jnp.bfloat16
SEQ = 1024
BLK = 256
DIM = 2048
HD = 256
HEADS = 2
CH = 256
NCH = DIM // CH
DXC = 512
NDX = DIM // DXC
GRP = 128
PIECE = 64
NP = BLK // PIECE
HALF = DIM // 2
SCALE = HD ** -0.5
MESH = pl.DeviceIdType.MESH


def dot_nn(a, b):
    return lax.dot_general(a, b, (((1,), (0,)), ((), ())), preferred_element_type=F32)


def dot_nt(a, b):
    return lax.dot_general(a, b, (((1,), (1,)), ((), ())), preferred_element_type=F32)


def at(start, size, align=256):
    return pl.ds(pl.multiple_of(start, align), size)


def body(x_ref, dy_ref, wq_ref, wk_ref, wv_ref, wo_ref,
         dx_out, dwq_out, dwk_out, dwv_out, dwo_out,
         xb, x_t, dyb, wq_raw, wq4, wkv, wo, q, k, v, k_t, v_t, p_t, p_inv, ds_t, o_t, do_acc, do_t,
         dkv, dkv_mate, dkv_send, dkv_part, dkv_full, dq, dq_mate,
         dwo_send, dwo_recv, dwq_send, dwq_recv,
         dx_own, dx_send, dx_recv, dwkv_send, dwkv_recv,
         sems, recvs, locs):
    model = lax.axis_index('model')
    data = lax.axis_index('data')
    chip = model // 2
    core = model % 2
    mate = {'model': chip * 2 + 1 - core}
    partner = {'model': (1 - chip) * 2 + core}
    peer = {'data': 1 - data}
    own_row = model * BLK
    mate_row = (chip * 2 + 1 - core) * BLK
    partner_row = ((1 - chip) * 2 + core) * BLK
    diag_row = ((1 - chip) * 2 + 1 - core) * BLK
    near = chip * 2 * BLK
    far = (1 - chip) * 2 * BLK

    groups = {}
    slots = {}
    devices = {}

    def send(name, src, dst, device, group=None, part=None):
        group = group or name
        devices[group] = device
        copy = pltpu.make_async_remote_copy(
            src_ref=src, dst_ref=dst, send_sem=sems.at[groups.setdefault(group, len(groups))],
            recv_sem=recvs.at[slots.setdefault(part or name, len(slots))],
            device_id=device, device_id_type=MESH)
        copy.start()

    def arrived(name, dst, device):
        with jax.named_scope('w_' + name):
            pltpu.make_async_remote_copy(
                src_ref=dst, dst_ref=dst, send_sem=sems.at[0],
                recv_sem=recvs.at[slots.setdefault(name, len(slots))],
                device_id=device, device_id_type=MESH).wait_recv()

    def sent(group, src):
        pltpu.make_async_remote_copy(src_ref=src, dst_ref=src, send_sem=sems.at[groups[group]], recv_sem=recvs.at[0],
                                     device_id=devices[group], device_id_type=MESH).wait_send()

    def local(src, dst, n):
        copy = pltpu.make_async_copy(src, dst, locs.at[n])
        copy.start()
        return copy

    def chunk_at(j):
        return lax.rem((1 - data) * (NCH // 2) + j, NCH)

    def x_piece(row, p):
        return at(row + p * PIECE, PIECE, PIECE)

    late = pl.ds(data * (NCH // 2), NCH // 2)

    def group_row(row, g):
        return at(row + g * GRP, GRP, GRP)

    def send_dy():
        for j in range(NCH // 2 - 1):
            c = chunk_at(j)
            send(f'dy_far{j}', dy_ref.at[:, at(c * CH, CH)], dyb.at[c, at(own_row, BLK)], partner, 'dy_far')
        for g in range(2):
            c = chunk_at(NCH // 2 - 1)
            send(f'dy_split{g}', dy_ref.at[g * GRP:(g + 1) * GRP, at(c * CH, CH)],
                 dyb.at[c, group_row(own_row, g)], partner, 'dy_far')
            for j in range(NCH // 2):
                c = data * (NCH // 2) + j
                send(f'dy_late{g}', dy_ref.at[g * GRP:(g + 1) * GRP, at(c * CH, CH)],
                     dyb.at[c, group_row(own_row, g)], partner, 'dy_far')

    barrier = pltpu.get_barrier_semaphore()
    for device in (mate, partner, peer):
        pl.semaphore_signal(barrier, inc=1, device_id=device, device_id_type=MESH)
    loads = [local(x_ref, xb.at[at(own_row, BLK)], 0), local(wq_ref, wq_raw, 1),
             local(wk_ref, wkv.at[0], 2), local(wv_ref, wkv.at[1], 3)]
    with jax.named_scope('barrier'):
        pl.semaphore_wait(barrier, 3)

    for p in range(NP):
        send(f'x_far{p}', x_ref.at[pl.ds(p * PIECE, PIECE)], xb.at[x_piece(own_row, p)], partner, 'x_far')
    send('x_mate', x_ref, xb.at[at(own_row, BLK)], mate)
    late_load = local(wo_ref, wo, 4)
    for c in range(NCH):
        own_chunk = dyb.at[c, at(own_row, BLK)]
        local(dy_ref.at[:, c * CH:(c + 1) * CH], own_chunk, 5)
        send('dy_mate', dy_ref.at[:, c * CH:(c + 1) * CH], own_chunk, mate)

    def project(xr, pieces):
        def put(dst, lo, value):
            for row, size, off in pieces:
                dst[row, lo:lo + HD] = value[off:off + size]
        for h in range(HEADS):
            put(q, h * HD, dot_nn(xr, wq4[core * HEADS + h]).astype(BF16))
        for n, (dst, dst_t) in enumerate(((k, k_t), (v, v_t))):
            value = dot_nn(xr, wkv[n]).astype(BF16)
            put(dst, 0, value)

    def flip_x(first_row):
        def step(t, carry):
            cols = at(t * 256, 256)
            for r in range(2):
                rows = at(first_row + r * BLK, BLK)
                x_t[cols, rows] = xb[rows, cols].T
            return carry
        lax.fori_loop(0, DIM // 256, step, 0)

    def flip_kv(first_row):
        for r in range(2):
            rows = at(first_row + r * BLK, BLK)
            k_t[:, rows] = k[rows, :].T
            v_t[:, rows] = v[rows, :].T

    with jax.named_scope('loads'):
        for copy in loads:
            copy.wait()

    with jax.named_scope('relay'):
        def relay(r, carry):
            rows = at(r * 128, 128, 128)
            for h in range(HEADS):
                wq4[core * HEADS + h, rows, :] = wq_raw[rows, h, :]
            return carry
        lax.fori_loop(0, DIM // 128, relay, 0)
    send('wq_mate', wq4.at[pl.ds(core * HEADS, HEADS)], wq4.at[pl.ds(core * HEADS, HEADS)], mate)

    arrived('x_mate', xb.at[at(mate_row, BLK)], mate)
    with jax.named_scope('proj1'):
        def project_near(r, carry):
            rows = at(near + r * BLK, BLK)
            project(xb[rows, :], [(rows, BLK, 0)])
            return carry
        lax.fori_loop(0, 2, project_near, 0)
        flip_kv(near)

    def forward_x(p):
        block = xb.at[x_piece(partner_row, p)]
        arrived(f'x_far{p}', block, partner)
        send(f'x_fwd{p}', block, block, mate, 'x_fwd', f'x_fwd{max(p, 1)}')

    def project_far(p):
        first, size = (0, 2 * PIECE) if p == 1 else (p * PIECE, PIECE)
        arrived(f'x_fwd{p}', xb.at[at(diag_row + first, size, PIECE)], mate)
        rows = [at(row + first, size, PIECE) for row in (partner_row, diag_row)]
        xr = jnp.concatenate([xb[r, :] for r in rows], axis=0)
        with jax.named_scope('proj2'):
            project(xr, [(rows[0], size, 0), (rows[1], size, size)])

    forward_x(0)
    with jax.named_scope('flip1'):
        flip_x(near)
    forward_x(1)
    project_far(1)
    late_load.wait()
    own_dy = dyb.at[:, at(own_row, BLK)]
    pltpu.make_async_copy(own_dy, own_dy, locs.at[5]).wait()
    arrived('dy_mate', dyb.at[:, at(mate_row, BLK)], mate)
    with jax.named_scope('do_near'):
        for half in range(HEADS):
            heads = slice(half * HD, (half + 1) * HD)
            acc = jnp.zeros((HD, 2 * BLK), F32)
            for c in range(NCH):
                acc += dot_nt(wo[heads, c * CH:(c + 1) * CH], dyb[c, at(near, 2 * BLK), :])
            do_t[heads, at(near, 2 * BLK)] = acc.astype(BF16)
        dkv[...] = jnp.zeros(dkv.shape, F32)
    forward_x(2)

    @pl.when(core == 0)
    def _():
        send_dy()
    project_far(2)
    forward_x(3)

    @pl.when(core == 1)
    def _():
        send_dy()
    project_far(3)
    flip_kv(far)

    def forward_dy(j):
        block = dyb.at[chunk_at(j), at(partner_row, BLK)]
        arrived(f'dy_far{j}', block, partner)
        send(f'dy_fwd{j}', block, block, mate, 'dy_fwd')

    mask = lax.broadcasted_iota(jnp.int32, (BLK, BLK), 0) <= lax.broadcasted_iota(jnp.int32, (BLK, BLK), 1)

    def scores(h, i):
        heads = slice(h * HD, (h + 1) * HD)
        cols = slice(i * BLK, (i + 1) * BLK)
        rows = (i + 1) * BLK
        qs = q[cols, heads] * jnp.asarray(SCALE, BF16)
        p_t[h, i * BLK:rows, cols] = jnp.where(mask, dot_nt(k[i * BLK:rows, :], qs), -jnp.inf)
        if i:
            p_t[h, :i * BLK, cols] = dot_nt(k[:i * BLK, :], qs)
        top = jnp.max(p_t[h, :rows, cols], axis=0, keepdims=True)
        e = jnp.exp(p_t[h, :rows, cols] - top)
        p_t[h, :rows, cols] = e
        p_inv[h, :, cols] = 1.0 / jnp.sum(e, axis=0, keepdims=True)

    def values(h, i):
        cols = slice(i * BLK, (i + 1) * BLK)
        rows = (i + 1) * BLK
        prob = (p_t[h, :rows, cols] * p_inv[h, :, cols]).astype(BF16)
        o_t[h * HD:(h + 1) * HD, cols] = dot_nn(v_t[:, :rows], prob).astype(BF16)

    def on_core(n, step):
        @pl.when(core == n)
        def _():
            step()

    with jax.named_scope('fwd'):
        for i in range(2):
            for h in range(HEADS):
                scores(h, i)
        on_core(1, lambda: forward_dy(0))
        for i in range(2, 4):
            for h in range(HEADS):
                scores(h, i)
        on_core(0, lambda: forward_dy(0))
        for i in range(4):
            for h in range(HEADS):
                values(h, i)

    def add_dkv(h, i, j, prob, ds):
        rows = slice(j * BLK, (j + 1) * BLK)
        cols = slice(i * BLK, (i + 1) * BLK)
        heads = at(h * HD, HD)
        dkv[0, rows, :] += dot_nn(ds, q[cols, heads])
        dkv[1, rows, :] += dot_nt(prob.astype(BF16), do_t[heads, cols])

    def backward_block(h, i, lo, size, keep):
        heads = slice(h * HD, (h + 1) * HD) if isinstance(h, int) else at(h * HD, HD)
        cols = slice(i * BLK + lo, i * BLK + lo + size)
        doi = do_t[heads, cols]
        delta = jnp.sum(doi.astype(F32) * o_t[heads, cols].astype(F32), axis=0, keepdims=True)
        inv = p_inv[h, :, cols]
        dqi = jnp.zeros((HD, size), F32)
        for j in range(i + 1):
            rows = slice(j * BLK, (j + 1) * BLK)
            prob = p_t[h, rows, cols] * inv
            ds = (prob * (dot_nn(v[rows, :], doi) - delta)).astype(BF16)
            dqi += dot_nn(k_t[:, rows], ds)
            if keep:
                ds_t[h, rows, (i % 2) * BLK + lo:(i % 2) * BLK + lo + size] = ds
            else:
                add_dkv(h, i, j, prob, ds)
        dq[h, cols, :] = (dqi * SCALE).astype(BF16).T

    def over_heads(step):
        def one(h, carry):
            step(h)
            return carry
        lax.fori_loop(0, HEADS, one, 0)

    def take_chunk(j):
        c = chunk_at(j)
        arrived(f'dy_fwd{j}', dyb.at[c, at(diag_row, BLK)], mate)
        dwo_send[j] = dot_nn(o_t[...], dyb[c]).astype(BF16)
        send('dwo', dwo_send.at[j], dwo_recv.at[j], peer)
        part = dot_nt(wo[:, at(c * CH, CH)], dyb[c, at(far, 2 * BLK), :])
        if j == 0:
            do_acc[...] = part
        else:
            do_acc[...] += part

    split = chunk_at(NCH // 2 - 1)

    def forward_split(g):
        block = dyb.at[split, group_row(partner_row, g)]
        arrived(f'dy_split{g}', block, partner)
        send(f'dy_sfwd{g}', block, block, mate, 'dy_fwd')

    def take_split():
        arrived('dy_sfwd1', dyb.at[split, group_row(diag_row, 1)], mate)
        with jax.named_scope('dwo3'):
            dwo_send[NCH // 2 - 1] = dot_nn(o_t[...], dyb[split]).astype(BF16)
            send('dwo', dwo_send.at[NCH // 2 - 1], dwo_recv.at[NCH // 2 - 1], peer)

    def forward_group(g):
        block = dyb.at[late, group_row(partner_row, g)]
        arrived(f'dy_late{g}', block, partner)
        send(f'dy_lfwd{g}', block, block, mate, 'dy_lfwd')

    def finish_do(rows, g):
        with jax.named_scope('do_late'):
            cols = [group_row(row, g) for row in rows]
            accs = [do_acc[:, group_row(row - far, g)] for row in rows]
            for c in [split] + [data * (NCH // 2) + j for j in range(NCH // 2)]:
                part = dot_nt(wo[:, at(c * CH, CH)], jnp.concatenate([dyb[c, n, :] for n in cols], axis=0))
                accs = [acc + part[:, n * GRP:(n + 1) * GRP] for n, acc in enumerate(accs)]
            for n, acc in zip(cols, accs):
                do_t[:, n] = acc.astype(BF16)

    def backward_far(g):
        def block_of(diag):
            for c in range(2):
                for n in range(2):
                    @pl.when((chip == c) & (core == n))
                    def _(c=c, n=n):
                        with jax.named_scope('bwd_far'):
                            for h in range(HEADS):
                                backward_block(h, 2 * (1 - c) + (1 - n if diag else n), g * GRP, GRP, True)
        if g == 0:
            finish_do([partner_row], g)
            forward_split(1)
            arrived('dy_sfwd0', dyb.at[split, group_row(diag_row, 0)], mate)
        arrived(f'dy_lfwd{g}', dyb.at[late, group_row(diag_row, g)], mate)
        finish_do([diag_row] if g == 0 else [partner_row, diag_row], g)
        block_of(True)
        send(f'dq_far{g}', dq.at[:, group_row(diag_row, g)], dq_mate.at[1 - chip, :, g * GRP:(g + 1) * GRP], mate, 'dq')
        if g == 0:
            take_split()
        block_of(False)
        arrived(f'dq_far{g}', dq_mate.at[1 - chip, :, g * GRP:(g + 1) * GRP], mate)

    def dx_cols(block, lo, size, cols):
        rows = at((block * 2 + core) * BLK + lo, size, GRP)
        acc = jnp.zeros((size, cols.stop - cols.start), F32)
        for h in range(HEADS):
            acc += dot_nt(dq[h, rows, :], wq4[core * HEADS + h, cols, :])
            acc += dot_nt(dq_mate[block, h, lo:lo + size], wq4[(1 - core) * HEADS + h, cols, :])
        return acc

    def send_dx(g, pieces):
        with jax.named_scope('dx'):
            for j in pieces:
                n = g * NDX + j
                dx_send[n] = dx_cols(1 - chip, g * GRP, GRP, slice(j * DXC, (j + 1) * DXC)).astype(BF16)
                send(f'dx{max(n, NDX)}' if g else 'dx', dx_send.at[n], dx_recv.at[n], partner, 'dx')

    take_chunk(0)
    forward_dy(1)
    forward_dy(2)
    take_chunk(1)
    take_chunk(2)

    for c in range(2):
        @pl.when(chip == c)
        def _(c=c):
            def step(h):
                for i in (2 * c, 2 * c + 1):
                    backward_block(h, i, 0, BLK, False)
            with jax.named_scope('bwd_near'):
                over_heads(step)
    send('dq_near', dq.at[:, at(mate_row, BLK)], dq_mate.at[chip], mate, 'dq')
    with jax.named_scope('flip2'):
        flip_x(far)
    arrived('wq_mate', wq4.at[pl.ds((1 - core) * HEADS, HEADS)], mate)
    forward_split(0)
    forward_group(0)
    backward_far(0)
    send_dx(0, (0, 1))
    forward_group(1)
    send_dx(0, (2, 3))
    backward_far(1)

    def send_dwq(r):
        with jax.named_scope('dwq'):
            rows = at((1 - data) * HALF + r * 256, 256)
            for h in range(HEADS):
                dwq_send[r, h] = dot_nn(x_t[rows, :], dq[h]).astype(BF16)
            send(f'dwq{r}', dwq_send.at[r], dwq_recv.at[r], peer, 'dwq')
    send_dwq(0)
    for c in range(2):
        @pl.when(chip == c)
        def _(c=c):
            def step(h):
                for i in (2 * (1 - c), 2 * (1 - c) + 1):
                    cols = slice(i * BLK, (i + 1) * BLK)
                    for j in range(i + 1):
                        rows = slice(j * BLK, (j + 1) * BLK)
                        add_dkv(h, i, j, p_t[h, rows, cols] * p_inv[h, :, cols],
                                ds_t[h, rows, (i % 2) * BLK:(i % 2 + 1) * BLK])
            with jax.named_scope('dkv'):
                over_heads(step)
    send('dkv_mate', dkv.at[1 - core], dkv_mate, mate)

    for r in range(1, 4):
        send_dwq(r)
    arrived('dkv_mate', dkv_mate, mate)
    factor = jnp.where(core == 0, SCALE, 1.0).astype(F32)
    summed = (dkv[core] + dkv_mate[...]) * factor
    dkv_mate[...] = summed
    dkv_send[...] = summed.astype(BF16)
    send('dkv_far', dkv_send, dkv_part, partner)
    send_dx(1, range(NDX))

    arrived('dq_near', dq_mate.at[chip], mate)
    for j in range(4):
        cols = slice(j * 512, (j + 1) * 512)
        dx_own[:, cols] = dx_cols(chip, 0, BLK, cols)
    arrived('dwo', dwo_recv, peer)
    for j in range(NCH // 2):
        cols = slice(j * CH, (j + 1) * CH)
        dwo_out[:, cols] = dot_nn(o_t[...], dyb[chunk_at(NCH // 2 + j)]) + dwo_recv[j].astype(F32)

    arrived('dkv_far', dkv_part, partner)
    dkv_full[core] = (dkv_mate[...] + dkv_part[...].astype(F32)).astype(BF16)
    send('dkv_full', dkv_full.at[core], dkv_full.at[core], mate)
    arrived('dkv_full', dkv_full.at[1 - core], mate)
    for n in range(2):
        peer_rows = at((model * 2 + 1 - data) * 256, 256)
        dwkv_send[n] = dot_nn(x_t[peer_rows, :], dkv_full[n]).astype(BF16)
    send('dwkv', dwkv_send, dwkv_recv, peer)
    kept_rows = at((model * 2 + data) * 256, 256)
    dwk_out[...] = dot_nn(x_t[kept_rows, :], dkv_full[0])
    dwv_out[...] = dot_nn(x_t[kept_rows, :], dkv_full[1])
    for j in range(4):
        cols = slice(j * 512, (j + 1) * 512)
        dx_own[:, cols] += (dot_nt(dkv_full[0, at(own_row, BLK), :], wkv[0, cols, :])
                            + dot_nt(dkv_full[1, at(own_row, BLK), :], wkv[1, cols, :]))

    def finish_dx(n):
        rows = slice(n // NDX * GRP, (n // NDX + 1) * GRP)
        cols = slice(n % NDX * DXC, (n % NDX + 1) * DXC)
        dx_out[rows, cols] = (dx_own[rows, cols] + dx_recv[n].astype(F32)).astype(BF16)

    arrived('dx', dx_recv.at[:NDX], partner)
    for n in range(NDX):
        finish_dx(n)
    for r in range(4):
        arrived(f'dwq{r}', dwq_recv.at[r], peer)
        with jax.named_scope('dwq_sum'):
            rows = at(data * HALF + r * 256, 256)
            for h in range(HEADS):
                value = dot_nn(x_t[rows, :], dq[h]) + dwq_recv[r, h].astype(F32)
                dwq_out[r * 256:(r + 1) * 256, h, :] = value
    for n in range(NDX, 2 * NDX):
        arrived(f'dx{n}', dx_recv.at[n], partner)
        finish_dx(n)
    arrived('dwkv', dwkv_recv, peer)
    dwk_out[...] += dwkv_recv[0].astype(F32)
    dwv_out[...] += dwkv_recv[1].astype(F32)
    with jax.named_scope('sends'):
        sent('x_far', x_ref)
        sent('x_mate', x_ref)
        sent('dy_far', dy_ref)
        sent('dy_mate', dy_ref)
        sent('wq_mate', wq4.at[pl.ds(core * HEADS, HEADS)])
        sent('x_fwd', xb.at[at(partner_row, BLK)])
        sent('dy_fwd', dyb.at[late, at(partner_row, BLK)])
        sent('dy_lfwd', dyb.at[late, at(partner_row, BLK)])
        sent('dwo', dwo_send)
        sent('dq', dq_mate)
        sent('dx', dx_send)
        sent('dkv_mate', dkv_mate)
        sent('dkv_far', dkv_send)
        sent('dkv_full', dkv_send)
        sent('dwq', dwq_send)
        sent('dwkv', dwkv_send)
    assert len(groups) == sems.shape[0] and len(slots) == recvs.shape[0]


def fused_step(x, dy, wq, wk, wv, wo):
    any_spec = pl.BlockSpec(memory_space=pl.ANY)
    vmem_spec = pl.BlockSpec(memory_space=pltpu.VMEM)
    scratch = [
        pltpu.VMEM((SEQ, DIM), BF16),
        pltpu.VMEM((DIM, SEQ), BF16),
        pltpu.VMEM((NCH, SEQ, CH), BF16),
        pltpu.VMEM((DIM, HEADS, HD), BF16),
        pltpu.VMEM((2 * HEADS, DIM, HD), BF16),
        pltpu.VMEM((2, DIM, HD), BF16),
        pltpu.VMEM((HEADS * HD, DIM), BF16),
        pltpu.VMEM((SEQ, HEADS * HD), BF16),
        pltpu.VMEM((SEQ, HD), BF16),
        pltpu.VMEM((SEQ, HD), BF16),
        pltpu.VMEM((HD, SEQ), BF16),
        pltpu.VMEM((HD, SEQ), BF16),
        pltpu.VMEM((HEADS, SEQ, SEQ), F32),
        pltpu.VMEM((HEADS, 1, SEQ), F32),
        pltpu.VMEM((HEADS, SEQ, 2 * BLK), BF16),
        pltpu.VMEM((HEADS * HD, SEQ), BF16),
        pltpu.VMEM((HEADS * HD, 2 * BLK), F32),
        pltpu.VMEM((HEADS * HD, SEQ), BF16),
        pltpu.VMEM((2, SEQ, HD), F32),
        pltpu.VMEM((SEQ, HD), F32),
        pltpu.VMEM((SEQ, HD), BF16),
        pltpu.VMEM((SEQ, HD), BF16),
        pltpu.VMEM((2, SEQ, HD), BF16),
        pltpu.VMEM((HEADS, SEQ, HD), BF16),
        pltpu.VMEM((2, HEADS, BLK, HD), BF16),
        pltpu.VMEM((NCH // 2, HEADS * HD, CH), BF16),
        pltpu.VMEM((NCH // 2, HEADS * HD, CH), BF16),
        pltpu.VMEM((4, HEADS, HALF // 4, HD), BF16),
        pltpu.VMEM((4, HEADS, HALF // 4, HD), BF16),
        pltpu.VMEM((BLK, DIM), F32),
        pltpu.VMEM((2 * NDX, GRP, DXC), BF16),
        pltpu.VMEM((2 * NDX, GRP, DXC), BF16),
        pltpu.VMEM((2, 256, HD), BF16),
        pltpu.VMEM((2, 256, HD), BF16),
        pltpu.SemaphoreType.DMA((16,)),
        pltpu.SemaphoreType.DMA((41,)),
        pltpu.SemaphoreType.DMA((6,)),
    ]
    return pl.pallas_call(
        body,
        out_shape=(pltpu.VMEM((BLK, DIM), BF16),
                   pltpu.VMEM((HALF, HEADS, HD), F32),
                   pltpu.VMEM((256, HD), F32),
                   pltpu.VMEM((256, HD), F32),
                   pltpu.VMEM((HEADS * HD, HALF), F32)),
        in_specs=[any_spec] * 6,
        out_specs=(vmem_spec,) * 5,
        scratch_shapes=scratch,
        compiler_params=pltpu.CompilerParams(collective_id=0, has_side_effects=True,
                                             vmem_limit_bytes=58 * 2 ** 20),
        name='attention_backward',
    )(x, dy, wq, wk, wv, wo)


def flush_body(*refs):
    sources, results, sems = refs[:5], refs[5:10], refs[10]
    copies = [pltpu.make_async_copy(a, b, sems.at[n]) for n, (a, b) in enumerate(zip(sources, results))]
    for copy in copies:
        copy.start()
    for copy in copies:
        copy.wait()


def flush(*arrays):
    any_spec = pl.BlockSpec(memory_space=pl.ANY)
    return pl.pallas_call(
        flush_body,
        out_shape=tuple(jax.ShapeDtypeStruct(a.shape, a.dtype) for a in arrays),
        in_specs=[any_spec] * 5,
        out_specs=(any_spec,) * 5,
        scratch_shapes=[pltpu.SemaphoreType.DMA((5,))],
        compiler_params=pltpu.CompilerParams(vmem_limit_bytes=2 ** 20),
        name='write_results',
    )(*arrays)


def solution(mesh):
    tok_spec = P(('pod', 'data'), 'model', None)

    def device_step(x_loc, dy_loc, w_q, w_k, w_v, w_o):
        dx, dwq, dwk, dwv, dwo = flush(*fused_step(x_loc[0], dy_loc[0], w_q, w_k[0], w_v[0],
                                                   w_o.reshape(HEADS * HD, DIM)))
        return dx[None], dwq, dwk, dwv, dwo.reshape(HEADS, HD, HALF)

    kv_rows = P(('pod', 'model', 'data'), None)
    return jax.shard_map(device_step, mesh=mesh,
                         in_specs=(tok_spec, tok_spec, P(None, 'model', None), P(), P(), P('model', None, None)),
                         out_specs=(tok_spec, P(('pod', 'data'), 'model', None), kv_rows, kv_rows,
                                    P(('pod', 'model'), None, 'data')),
                         check_vma=False)
```

```python
import functools

import jax
import jax.numpy as jnp
from jax import lax
from jax.experimental import pallas as pl
from jax.experimental.pallas import tpu as pltpu
from jax.sharding import PartitionSpec as P

F32 = jnp.float32
BF16 = jnp.bfloat16
SEQ = 1024
BLK = 256
DIM = 2048
HD = 256
HEADS = 2
CH = 256
NCH = DIM // CH
DXC = 512
NDX = DIM // DXC
GRP = 128
PIECE = 64
NP = BLK // PIECE
HALF = DIM // 2
SCALE = HD ** -0.5
MESH = pl.DeviceIdType.MESH


def dot_nn(a, b):
    return lax.dot_general(a, b, (((1,), (0,)), ((), ())), preferred_element_type=F32)


def dot_nt(a, b):
    return lax.dot_general(a, b, (((1,), (1,)), ((), ())), preferred_element_type=F32)


def at(start, size, align=256):
    return pl.ds(pl.multiple_of(start, align), size)


def body(x_ref, dy_ref, wq_ref, wk_ref, wv_ref, wo_ref,
         dx_out, dwq_out, dwk_out, dwv_out, dwo_out,
         xb, x_t, dyb, wq_raw, wq4, wkv, wo, q, k, v, k_t, v_t, p_t, p_inv, ds_t, o_t, do_acc, do_t,
         dkv, dkv_mate, dkv_send, dkv_part, dkv_full, dq, dq_mate,
         dwo_send, dwo_recv, dwq_send, dwq_recv,
         dx_own, dx_send, dx_recv, dwkv_send, dwkv_recv,
         sems, recvs, locs):
    model = lax.axis_index('model')
    data = lax.axis_index('data')
    chip = model // 2
    core = model % 2
    mate = {'model': chip * 2 + 1 - core}
    partner = {'model': (1 - chip) * 2 + core}
    peer = {'data': 1 - data}
    own_row = model * BLK
    mate_row = (chip * 2 + 1 - core) * BLK
    partner_row = ((1 - chip) * 2 + core) * BLK
    diag_row = ((1 - chip) * 2 + 1 - core) * BLK
    near = chip * 2 * BLK
    far = (1 - chip) * 2 * BLK

    groups = {}
    slots = {}
    devices = {}

    def send(name, src, dst, device, group=None, part=None):
        group = group or name
        devices[group] = device
        copy = pltpu.make_async_remote_copy(
            src_ref=src, dst_ref=dst, send_sem=sems.at[groups.setdefault(group, len(groups))],
            recv_sem=recvs.at[slots.setdefault(part or name, len(slots))],
            device_id=device, device_id_type=MESH)
        copy.start()

    def arrived(name, dst, device):
        with jax.named_scope('w_' + name):
            pltpu.make_async_remote_copy(
                src_ref=dst, dst_ref=dst, send_sem=sems.at[0],
                recv_sem=recvs.at[slots.setdefault(name, len(slots))],
                device_id=device, device_id_type=MESH).wait_recv()

    def sent(group, src):
        pltpu.make_async_remote_copy(src_ref=src, dst_ref=src, send_sem=sems.at[groups[group]], recv_sem=recvs.at[0],
                                     device_id=devices[group], device_id_type=MESH).wait_send()

    def local(src, dst, n):
        copy = pltpu.make_async_copy(src, dst, locs.at[n])
        copy.start()
        return copy

    def chunk_at(j):
        return lax.rem((1 - data) * (NCH // 2) + j, NCH)

    def x_piece(row, p):
        return at(row + p * PIECE, PIECE, PIECE)

    late = pl.ds(data * (NCH // 2), NCH // 2)

    def group_row(row, g):
        return at(row + g * GRP, GRP, GRP)

    def send_dy():
        for j in range(NCH // 2 - 1):
            c = chunk_at(j)
            send(f'dy_far{j}', dy_ref.at[:, at(c * CH, CH)], dyb.at[c, at(own_row, BLK)], partner, 'dy_far')
        for g in range(2):
            c = chunk_at(NCH // 2 - 1)
            send(f'dy_split{g}', dy_ref.at[g * GRP:(g + 1) * GRP, at(c * CH, CH)],
                 dyb.at[c, group_row(own_row, g)], partner, 'dy_far')
            for j in range(NCH // 2):
                c = data * (NCH // 2) + j
                send(f'dy_late{g}', dy_ref.at[g * GRP:(g + 1) * GRP, at(c * CH, CH)],
                     dyb.at[c, group_row(own_row, g)], partner, 'dy_far')

    barrier = pltpu.get_barrier_semaphore()
    for device in (mate, partner, peer):
        pl.semaphore_signal(barrier, inc=1, device_id=device, device_id_type=MESH)
    loads = [local(x_ref, xb.at[at(own_row, BLK)], 0), local(wq_ref, wq_raw, 1),
             local(wk_ref, wkv.at[0], 2), local(wv_ref, wkv.at[1], 3)]
    with jax.named_scope('barrier'):
        pl.semaphore_wait(barrier, 3)

    for p in range(NP):
        send(f'x_far{p}', x_ref.at[pl.ds(p * PIECE, PIECE)], xb.at[x_piece(own_row, p)], partner, 'x_far')
    send('x_mate', x_ref, xb.at[at(own_row, BLK)], mate)
    late_load = local(wo_ref, wo, 4)
    for c in range(NCH):
        own_chunk = dyb.at[c, at(own_row, BLK)]
        local(dy_ref.at[:, c * CH:(c + 1) * CH], own_chunk, 5)
        send('dy_mate', dy_ref.at[:, c * CH:(c + 1) * CH], own_chunk, mate)

    def project(xr, pieces):
        def put(dst, lo, value):
            for row, size, off in pieces:
                dst[row, lo:lo + HD] = value[off:off + size]
        for h in range(HEADS):
            put(q, h * HD, dot_nn(xr, wq4[core * HEADS + h]).astype(BF16))
        for n, (dst, dst_t) in enumerate(((k, k_t), (v, v_t))):
            value = dot_nn(xr, wkv[n]).astype(BF16)
            put(dst, 0, value)

    def flip_x(first_row):
        def step(t, carry):
            cols = at(t * 256, 256)
            for r in range(2):
                rows = at(first_row + r * BLK, BLK)
                x_t[cols, rows] = xb[rows, cols].T
            return carry
        lax.fori_loop(0, DIM // 256, step, 0)

    def flip_kv(first_row):
        for r in range(2):
            rows = at(first_row + r * BLK, BLK)
            k_t[:, rows] = k[rows, :].T
            v_t[:, rows] = v[rows, :].T

    with jax.named_scope('loads'):
        for copy in loads:
            copy.wait()

    with jax.named_scope('relay'):
        def relay(r, carry):
            rows = at(r * 128, 128, 128)
            for h in range(HEADS):
                wq4[core * HEADS + h, rows, :] = wq_raw[rows, h, :]
            return carry
        lax.fori_loop(0, DIM // 128, relay, 0)
    send('wq_mate', wq4.at[pl.ds(core * HEADS, HEADS)], wq4.at[pl.ds(core * HEADS, HEADS)], mate)

    arrived('x_mate', xb.at[at(mate_row, BLK)], mate)
    with jax.named_scope('proj1'):
        def project_near(r, carry):
            rows = at(near + r * BLK, BLK)
            project(xb[rows, :], [(rows, BLK, 0)])
            return carry
        lax.fori_loop(0, 2, project_near, 0)
        flip_kv(near)

    def forward_x(p):
        block = xb.at[x_piece(partner_row, p)]
        arrived(f'x_far{p}', block, partner)
        send(f'x_fwd{p}', block, block, mate, 'x_fwd', f'x_fwd{max(p, 1)}')

    def project_far(p):
        first, size = (0, 2 * PIECE) if p == 1 else (p * PIECE, PIECE)
        arrived(f'x_fwd{p}', xb.at[at(diag_row + first, size, PIECE)], mate)
        rows = [at(row + first, size, PIECE) for row in (partner_row, diag_row)]
        xr = jnp.concatenate([xb[r, :] for r in rows], axis=0)
        with jax.named_scope('proj2'):
            project(xr, [(rows[0], size, 0), (rows[1], size, size)])

    forward_x(0)
    with jax.named_scope('flip1'):
        flip_x(near)
    forward_x(1)
    project_far(1)
    late_load.wait()
    own_dy = dyb.at[:, at(own_row, BLK)]
    pltpu.make_async_copy(own_dy, own_dy, locs.at[5]).wait()
    arrived('dy_mate', dyb.at[:, at(mate_row, BLK)], mate)
    with jax.named_scope('do_near'):
        for half in range(HEADS):
            heads = slice(half * HD, (half + 1) * HD)
            acc = jnp.zeros((HD, 2 * BLK), F32)
            for c in range(NCH):
                acc += dot_nt(wo[heads, c * CH:(c + 1) * CH], dyb[c, at(near, 2 * BLK), :])
            do_t[heads, at(near, 2 * BLK)] = acc.astype(BF16)
        dkv[...] = jnp.zeros(dkv.shape, F32)
    forward_x(2)

    @pl.when(core == 0)
    def _():
        send_dy()
    project_far(2)
    forward_x(3)

    @pl.when(core == 1)
    def _():
        send_dy()
    project_far(3)
    flip_kv(far)

    def forward_dy(j):
        block = dyb.at[chunk_at(j), at(partner_row, BLK)]
        arrived(f'dy_far{j}', block, partner)
        send(f'dy_fwd{j}', block, block, mate, 'dy_fwd')

    mask = lax.broadcasted_iota(jnp.int32, (BLK, BLK), 0) <= lax.broadcasted_iota(jnp.int32, (BLK, BLK), 1)

    def scores(h, i):
        heads = slice(h * HD, (h + 1) * HD)
        cols = slice(i * BLK, (i + 1) * BLK)
        rows = (i + 1) * BLK
        qs = q[cols, heads] * jnp.asarray(SCALE, BF16)
        p_t[h, i * BLK:rows, cols] = jnp.where(mask, dot_nt(k[i * BLK:rows, :], qs), -jnp.inf)
        if i:
            p_t[h, :i * BLK, cols] = dot_nt(k[:i * BLK, :], qs)
        top = jnp.max(p_t[h, :rows, cols], axis=0, keepdims=True)
        e = jnp.exp(p_t[h, :rows, cols] - top)
        p_t[h, :rows, cols] = e
        p_inv[h, :, cols] = 1.0 / jnp.sum(e, axis=0, keepdims=True)

    def values(h, i):
        cols = slice(i * BLK, (i + 1) * BLK)
        rows = (i + 1) * BLK
        prob = (p_t[h, :rows, cols] * p_inv[h, :, cols]).astype(BF16)
        o_t[h * HD:(h + 1) * HD, cols] = dot_nn(v_t[:, :rows], prob).astype(BF16)

    def on_core(n, step):
        @pl.when(core == n)
        def _():
            step()

    with jax.named_scope('fwd'):
        for i in range(2):
            for h in range(HEADS):
                scores(h, i)
        on_core(1, lambda: forward_dy(0))
        for i in range(2, 4):
            for h in range(HEADS):
                scores(h, i)
        on_core(0, lambda: forward_dy(0))
        for i in range(4):
            for h in range(HEADS):
                values(h, i)

    def add_dkv(h, i, j, prob, ds):
        rows = slice(j * BLK, (j + 1) * BLK)
        cols = slice(i * BLK, (i + 1) * BLK)
        heads = at(h * HD, HD)
        dkv[0, rows, :] += dot_nn(ds, q[cols, heads])
        dkv[1, rows, :] += dot_nt(prob.astype(BF16), do_t[heads, cols])

    def backward_block(h, i, lo, size, keep):
        heads = slice(h * HD, (h + 1) * HD) if isinstance(h, int) else at(h * HD, HD)
        cols = slice(i * BLK + lo, i * BLK + lo + size)
        doi = do_t[heads, cols]
        delta = jnp.sum(doi.astype(F32) * o_t[heads, cols].astype(F32), axis=0, keepdims=True)
        inv = p_inv[h, :, cols]
        dqi = jnp.zeros((HD, size), F32)
        for j in range(i + 1):
            rows = slice(j * BLK, (j + 1) * BLK)
            prob = p_t[h, rows, cols] * inv
            ds = (prob * (dot_nn(v[rows, :], doi) - delta)).astype(BF16)
            dqi += dot_nn(k_t[:, rows], ds)
            if keep:
                ds_t[h, rows, (i % 2) * BLK + lo:(i % 2) * BLK + lo + size] = ds
            else:
                add_dkv(h, i, j, prob, ds)
        dq[h, cols, :] = (dqi * SCALE).astype(BF16).T

    def over_heads(step):
        def one(h, carry):
            step(h)
            return carry
        lax.fori_loop(0, HEADS, one, 0)

    def take_chunk(j):
        c = chunk_at(j)
        arrived(f'dy_fwd{j}', dyb.at[c, at(diag_row, BLK)], mate)
        dwo_send[j] = dot_nn(o_t[...], dyb[c]).astype(BF16)
        send('dwo', dwo_send.at[j], dwo_recv.at[j], peer)
        part = dot_nt(wo[:, at(c * CH, CH)], dyb[c, at(far, 2 * BLK), :])
        if j == 0:
            do_acc[...] = part
        else:
            do_acc[...] += part

    split = chunk_at(NCH // 2 - 1)

    def forward_split(g):
        block = dyb.at[split, group_row(partner_row, g)]
        arrived(f'dy_split{g}', block, partner)
        send(f'dy_sfwd{g}', block, block, mate, 'dy_fwd')

    def take_split():
        arrived('dy_sfwd1', dyb.at[split, group_row(diag_row, 1)], mate)
        with jax.named_scope('dwo3'):
            dwo_send[NCH // 2 - 1] = dot_nn(o_t[...], dyb[split]).astype(BF16)
            send('dwo', dwo_send.at[NCH // 2 - 1], dwo_recv.at[NCH // 2 - 1], peer)

    def forward_group(g):
        block = dyb.at[late, group_row(partner_row, g)]
        arrived(f'dy_late{g}', block, partner)
        send(f'dy_lfwd{g}', block, block, mate, 'dy_lfwd')

    def finish_do(rows, g):
        with jax.named_scope('do_late'):
            cols = [group_row(row, g) for row in rows]
            accs = [do_acc[:, group_row(row - far, g)] for row in rows]
            for c in [split] + [data * (NCH // 2) + j for j in range(NCH // 2)]:
                part = dot_nt(wo[:, at(c * CH, CH)], jnp.concatenate([dyb[c, n, :] for n in cols], axis=0))
                accs = [acc + part[:, n * GRP:(n + 1) * GRP] for n, acc in enumerate(accs)]
            for n, acc in zip(cols, accs):
                do_t[:, n] = acc.astype(BF16)

    def far_blocks(g, heads, blocks_of):
        for c in range(2):
            for n in range(2):
                @pl.when((chip == c) & (core == n))
                def _(c=c, n=n):
                    with jax.named_scope('bwd_far'):
                        for h in heads:
                            for b in blocks_of(n):
                                backward_block(h, 2 * (1 - c) + b, g * GRP, GRP, True)

    def exchange_dq(g):
        send(f'dq_far{g}', dq.at[:, group_row(diag_row, g)], dq_mate.at[1 - chip, :, g * GRP:(g + 1) * GRP], mate, 'dq')

    def arrived_dq(g):
        arrived(f'dq_far{g}', dq_mate.at[1 - chip, :, g * GRP:(g + 1) * GRP], mate)

    def dx_cols(block, lo, size, cols):
        rows = at((block * 2 + core) * BLK + lo, size, GRP)
        acc = jnp.zeros((size, cols.stop - cols.start), F32)
        for h in range(HEADS):
            acc += dot_nt(dq[h, rows, :], wq4[core * HEADS + h, cols, :])
            acc += dot_nt(dq_mate[block, h, lo:lo + size], wq4[(1 - core) * HEADS + h, cols, :])
        return acc

    def send_dx(g, pieces):
        with jax.named_scope('dx'):
            for j in pieces:
                n = g * NDX + j
                dx_send[n] = dx_cols(1 - chip, g * GRP, GRP, slice(j * DXC, (j + 1) * DXC)).astype(BF16)
                send(f'dx{max(n, NDX)}' if g else 'dx', dx_send.at[n], dx_recv.at[n], partner, 'dx')

    take_chunk(0)
    forward_dy(1)
    forward_dy(2)
    take_chunk(1)
    take_chunk(2)

    for c in range(2):
        @pl.when(chip == c)
        def _(c=c):
            def step(h):
                for i in (2 * c, 2 * c + 1):
                    backward_block(h, i, 0, BLK, False)
            with jax.named_scope('bwd_near'):
                over_heads(step)
    send('dq_near', dq.at[:, at(mate_row, BLK)], dq_mate.at[chip], mate, 'dq')
    with jax.named_scope('flip2'):
        flip_x(far)
    arrived('wq_mate', wq4.at[pl.ds((1 - core) * HEADS, HEADS)], mate)
    def send_dwq(r, heads):
        with jax.named_scope('dwq'):
            rows = at((1 - data) * HALF + r * 256, 256)
            for h in heads:
                dwq_send[r, h] = dot_nn(x_t[rows, :], dq[h]).astype(BF16)
                send(f'dwq{r}', dwq_send.at[r, h], dwq_recv.at[r, h], peer, 'dwq')

    forward_split(0)
    forward_group(0)
    finish_do([partner_row], 0)
    far_blocks(0, range(HEADS), lambda n: (n,))
    forward_split(1)
    arrived('dy_sfwd0', dyb.at[split, group_row(diag_row, 0)], mate)
    arrived('dy_lfwd0', dyb.at[late, group_row(diag_row, 0)], mate)
    finish_do([diag_row], 0)
    far_blocks(0, range(HEADS), lambda n: (1 - n,))
    exchange_dq(0)
    take_split()
    arrived_dq(0)
    send_dx(0, (0, 1))
    forward_group(1)
    send_dx(0, (2, 3))
    arrived('dy_lfwd1', dyb.at[late, group_row(diag_row, 1)], mate)
    finish_do([partner_row, diag_row], 1)
    for h in range(HEADS):
        for c in range(2):
            @pl.when(chip == c)
            def _(c=c):
                with jax.named_scope('bwd_far'):
                    for b in range(2):
                        backward_block(h, 2 * (1 - c) + b, GRP, GRP, True)
        for r in range(2):
            send_dwq(r, [h])
    exchange_dq(1)
    for c in range(2):
        @pl.when(chip == c)
        def _(c=c):
            def step(h):
                for i in (2 * (1 - c), 2 * (1 - c) + 1):
                    cols = slice(i * BLK, (i + 1) * BLK)
                    for j in range(i + 1):
                        rows = slice(j * BLK, (j + 1) * BLK)
                        add_dkv(h, i, j, p_t[h, rows, cols] * p_inv[h, :, cols],
                                ds_t[h, rows, (i % 2) * BLK:(i % 2 + 1) * BLK])
            with jax.named_scope('dkv'):
                over_heads(step)
    send('dkv_mate', dkv.at[1 - core], dkv_mate, mate)

    for r in range(2, 4):
        send_dwq(r, range(HEADS))
    arrived_dq(1)
    arrived('dkv_mate', dkv_mate, mate)
    factor = jnp.where(core == 0, SCALE, 1.0).astype(F32)
    summed = (dkv[core] + dkv_mate[...]) * factor
    dkv_mate[...] = summed
    dkv_send[...] = summed.astype(BF16)
    send('dkv_far', dkv_send, dkv_part, partner)
    send_dx(1, range(NDX))

    arrived('dq_near', dq_mate.at[chip], mate)
    for j in range(4):
        cols = slice(j * 512, (j + 1) * 512)
        dx_own[:, cols] = dx_cols(chip, 0, BLK, cols)
    arrived('dwo', dwo_recv, peer)
    for j in range(NCH // 2):
        cols = slice(j * CH, (j + 1) * CH)
        dwo_out[:, cols] = dot_nn(o_t[...], dyb[chunk_at(NCH // 2 + j)]) + dwo_recv[j].astype(F32)

    arrived('dkv_far', dkv_part, partner)
    dkv_full[core] = (dkv_mate[...] + dkv_part[...].astype(F32)).astype(BF16)
    send('dkv_full', dkv_full.at[core], dkv_full.at[core], mate)
    arrived('dkv_full', dkv_full.at[1 - core], mate)
    for n in range(2):
        peer_rows = at((model * 2 + 1 - data) * 256, 256)
        dwkv_send[n] = dot_nn(x_t[peer_rows, :], dkv_full[n]).astype(BF16)
    send('dwkv', dwkv_send, dwkv_recv, peer)
    kept_rows = at((model * 2 + data) * 256, 256)
    dwk_out[...] = dot_nn(x_t[kept_rows, :], dkv_full[0])
    dwv_out[...] = dot_nn(x_t[kept_rows, :], dkv_full[1])
    for j in range(4):
        cols = slice(j * 512, (j + 1) * 512)
        dx_own[:, cols] += (dot_nt(dkv_full[0, at(own_row, BLK), :], wkv[0, cols, :])
                            + dot_nt(dkv_full[1, at(own_row, BLK), :], wkv[1, cols, :]))

    def finish_dx(n):
        rows = slice(n // NDX * GRP, (n // NDX + 1) * GRP)
        cols = slice(n % NDX * DXC, (n % NDX + 1) * DXC)
        dx_out[rows, cols] = (dx_own[rows, cols] + dx_recv[n].astype(F32)).astype(BF16)

    arrived('dx', dx_recv.at[:NDX], partner)
    for n in range(NDX):
        finish_dx(n)
    for r in range(4):
        arrived(f'dwq{r}', dwq_recv.at[r], peer)
        with jax.named_scope('dwq_sum'):
            rows = at(data * HALF + r * 256, 256)
            for h in range(HEADS):
                value = dot_nn(x_t[rows, :], dq[h]) + dwq_recv[r, h].astype(F32)
                dwq_out[r * 256:(r + 1) * 256, h, :] = value
    for n in range(NDX, 2 * NDX):
        arrived(f'dx{n}', dx_recv.at[n], partner)
        finish_dx(n)
    arrived('dwkv', dwkv_recv, peer)
    dwk_out[...] += dwkv_recv[0].astype(F32)
    dwv_out[...] += dwkv_recv[1].astype(F32)
    with jax.named_scope('sends'):
        sent('x_far', x_ref)
        sent('x_mate', x_ref)
        sent('dy_far', dy_ref)
        sent('dy_mate', dy_ref)
        sent('wq_mate', wq4.at[pl.ds(core * HEADS, HEADS)])
        sent('x_fwd', xb.at[at(partner_row, BLK)])
        sent('dy_fwd', dyb.at[late, at(partner_row, BLK)])
        sent('dy_lfwd', dyb.at[late, at(partner_row, BLK)])
        sent('dwo', dwo_send)
        sent('dq', dq_mate)
        sent('dx', dx_send)
        sent('dkv_mate', dkv_mate)
        sent('dkv_far', dkv_send)
        sent('dkv_full', dkv_send)
        sent('dwq', dwq_send)
        sent('dwkv', dwkv_send)
    assert len(groups) == sems.shape[0] and len(slots) == recvs.shape[0]


def fused_step(x, dy, wq, wk, wv, wo):
    any_spec = pl.BlockSpec(memory_space=pl.ANY)
    vmem_spec = pl.BlockSpec(memory_space=pltpu.VMEM)
    scratch = [
        pltpu.VMEM((SEQ, DIM), BF16),
        pltpu.VMEM((DIM, SEQ), BF16),
        pltpu.VMEM((NCH, SEQ, CH), BF16),
        pltpu.VMEM((DIM, HEADS, HD), BF16),
        pltpu.VMEM((2 * HEADS, DIM, HD), BF16),
        pltpu.VMEM((2, DIM, HD), BF16),
        pltpu.VMEM((HEADS * HD, DIM), BF16),
        pltpu.VMEM((SEQ, HEADS * HD), BF16),
        pltpu.VMEM((SEQ, HD), BF16),
        pltpu.VMEM((SEQ, HD), BF16),
        pltpu.VMEM((HD, SEQ), BF16),
        pltpu.VMEM((HD, SEQ), BF16),
        pltpu.VMEM((HEADS, SEQ, SEQ), F32),
        pltpu.VMEM((HEADS, 1, SEQ), F32),
        pltpu.VMEM((HEADS, SEQ, 2 * BLK), BF16),
        pltpu.VMEM((HEADS * HD, SEQ), BF16),
        pltpu.VMEM((HEADS * HD, 2 * BLK), F32),
        pltpu.VMEM((HEADS * HD, SEQ), BF16),
        pltpu.VMEM((2, SEQ, HD), F32),
        pltpu.VMEM((SEQ, HD), F32),
        pltpu.VMEM((SEQ, HD), BF16),
        pltpu.VMEM((SEQ, HD), BF16),
        pltpu.VMEM((2, SEQ, HD), BF16),
        pltpu.VMEM((HEADS, SEQ, HD), BF16),
        pltpu.VMEM((2, HEADS, BLK, HD), BF16),
        pltpu.VMEM((NCH // 2, HEADS * HD, CH), BF16),
        pltpu.VMEM((NCH // 2, HEADS * HD, CH), BF16),
        pltpu.VMEM((4, HEADS, HALF // 4, HD), BF16),
        pltpu.VMEM((4, HEADS, HALF // 4, HD), BF16),
        pltpu.VMEM((BLK, DIM), F32),
        pltpu.VMEM((2 * NDX, GRP, DXC), BF16),
        pltpu.VMEM((2 * NDX, GRP, DXC), BF16),
        pltpu.VMEM((2, 256, HD), BF16),
        pltpu.VMEM((2, 256, HD), BF16),
        pltpu.SemaphoreType.DMA((16,)),
        pltpu.SemaphoreType.DMA((41,)),
        pltpu.SemaphoreType.DMA((6,)),
    ]
    return pl.pallas_call(
        body,
        out_shape=(pltpu.VMEM((BLK, DIM), BF16),
                   pltpu.VMEM((HALF, HEADS, HD), F32),
                   pltpu.VMEM((256, HD), F32),
                   pltpu.VMEM((256, HD), F32),
                   pltpu.VMEM((HEADS * HD, HALF), F32)),
        in_specs=[any_spec] * 6,
        out_specs=(vmem_spec,) * 5,
        scratch_shapes=scratch,
        compiler_params=pltpu.CompilerParams(collective_id=0, has_side_effects=True,
                                             vmem_limit_bytes=58 * 2 ** 20),
        name='attention_backward',
    )(x, dy, wq, wk, wv, wo)


def flush_body(*refs):
    sources, results, sems = refs[:5], refs[5:10], refs[10]
    copies = [pltpu.make_async_copy(a, b, sems.at[n]) for n, (a, b) in enumerate(zip(sources, results))]
    for copy in copies:
        copy.start()
    for copy in copies:
        copy.wait()


def flush(*arrays):
    any_spec = pl.BlockSpec(memory_space=pl.ANY)
    return pl.pallas_call(
        flush_body,
        out_shape=tuple(jax.ShapeDtypeStruct(a.shape, a.dtype) for a in arrays),
        in_specs=[any_spec] * 5,
        out_specs=(any_spec,) * 5,
        scratch_shapes=[pltpu.SemaphoreType.DMA((5,))],
        compiler_params=pltpu.CompilerParams(vmem_limit_bytes=2 ** 20),
        name='write_results',
    )(*arrays)


def solution(mesh):
    tok_spec = P(('pod', 'data'), 'model', None)

    def device_step(x_loc, dy_loc, w_q, w_k, w_v, w_o):
        dx, dwq, dwk, dwv, dwo = flush(*fused_step(x_loc[0], dy_loc[0], w_q, w_k[0], w_v[0],
                                                   w_o.reshape(HEADS * HD, DIM)))
        return dx[None], dwq, dwk, dwv, dwo.reshape(HEADS, HD, HALF)

    kv_rows = P(('pod', 'model', 'data'), None)
    return jax.shard_map(device_step, mesh=mesh,
                         in_specs=(tok_spec, tok_spec, P(None, 'model', None), P(), P(), P('model', None, None)),
                         out_specs=(tok_spec, P(('pod', 'data'), 'model', None), kv_rows, kv_rows,
                                    P(('pod', 'model'), None, 'data')),
                         check_vma=False)
```

```python
import functools

import jax
import jax.numpy as jnp
from jax import lax
from jax.experimental import pallas as pl
from jax.experimental.pallas import tpu as pltpu
from jax.sharding import PartitionSpec as P

F32 = jnp.float32
BF16 = jnp.bfloat16
SEQ = 1024
BLK = 256
DIM = 2048
HD = 256
HEADS = 2
CH = 256
NCH = DIM // CH
DXC = 512
NDX = DIM // DXC
GRP = 128
SHARED = {**dict.fromkeys(('x_far', 'x_mate', 'dy_far', 'dy_mate'), 'inputs'),
          **dict.fromkeys(('x_fwd', 'dwo', 'dwq', 'dx'), 'mib'),
          **dict.fromkeys(('wq_mate', 'dy_fwd', 'dy_lfwd', 'dkv_mate'), 'pair'),
          **dict.fromkeys(('dkv_far', 'dkv_full'), 'dkv'), 'dq': 'dq', 'dwkv': 'dwkv'}
PIECE = 64
NP = BLK // PIECE
HALF = DIM // 2
SCALE = HD ** -0.5
MESH = pl.DeviceIdType.MESH


def dot_nn(a, b):
    return lax.dot_general(a, b, (((1,), (0,)), ((), ())), preferred_element_type=F32)


def dot_nt(a, b):
    return lax.dot_general(a, b, (((1,), (1,)), ((), ())), preferred_element_type=F32)


def at(start, size, align=256):
    return pl.ds(pl.multiple_of(start, align), size)


def body(x_ref, dy_ref, wq_ref, wk_ref, wv_ref, wo_ref,
         dx_out, dwq_out, dwk_out, dwv_out, dwo_out,
         xb, x_t, dyb, wq_raw, wq4, wkv, wo, q, k, v, k_t, v_t, p_t, p_inv, ds_t, o_t, do_acc, do_t,
         dkv, dkv_mate, dkv_send, dkv_part, dkv_full, dq, dq_mate,
         dwo_send, dwo_recv, dwq_send, dwq_recv,
         dx_own, dx_send, dx_recv, dwkv_send, dwkv_recv,
         sems, recvs, locs):
    model = lax.axis_index('model')
    data = lax.axis_index('data')
    chip = model // 2
    core = model % 2
    mate = {'model': chip * 2 + 1 - core}
    partner = {'model': (1 - chip) * 2 + core}
    peer = {'data': 1 - data}
    own_row = model * BLK
    mate_row = (chip * 2 + 1 - core) * BLK
    partner_row = ((1 - chip) * 2 + core) * BLK
    diag_row = ((1 - chip) * 2 + 1 - core) * BLK
    near = chip * 2 * BLK
    far = (1 - chip) * 2 * BLK

    groups = {}
    slots = {}
    devices = {}

    def send(name, src, dst, device, group=None, part=None):
        group = SHARED[group or name]
        devices[group] = device
        copy = pltpu.make_async_remote_copy(
            src_ref=src, dst_ref=dst, send_sem=sems.at[groups.setdefault(group, len(groups))],
            recv_sem=recvs.at[slots.setdefault(part or name, len(slots))],
            device_id=device, device_id_type=MESH)
        copy.start()

    def arrived(name, dst, device):
        with jax.named_scope('w_' + name):
            pltpu.make_async_remote_copy(
                src_ref=dst, dst_ref=dst, send_sem=sems.at[0],
                recv_sem=recvs.at[slots.setdefault(name, len(slots))],
                device_id=device, device_id_type=MESH).wait_recv()

    def sent(group, src):
        pltpu.make_async_remote_copy(src_ref=src, dst_ref=src, send_sem=sems.at[groups[group]], recv_sem=recvs.at[0],
                                     device_id=devices[group], device_id_type=MESH).wait_send()

    def local(src, dst, n):
        copy = pltpu.make_async_copy(src, dst, locs.at[n])
        copy.start()
        return copy

    def chunk_at(j):
        return lax.rem((1 - data) * (NCH // 2) + j, NCH)

    def x_piece(row, p):
        return at(row + p * PIECE, PIECE, PIECE)

    late = pl.ds(data * (NCH // 2), NCH // 2)

    def group_row(row, g):
        return at(row + g * GRP, GRP, GRP)

    def send_dy():
        for j in range(NCH // 2 - 1):
            c = chunk_at(j)
            send(f'dy_far{j}', dy_ref.at[:, at(c * CH, CH)], dyb.at[c, at(own_row, BLK)], partner, 'dy_far')
        for g in range(2):
            c = chunk_at(NCH // 2 - 1)
            send(f'dy_split{g}', dy_ref.at[g * GRP:(g + 1) * GRP, at(c * CH, CH)],
                 dyb.at[c, group_row(own_row, g)], partner, 'dy_far')
            for j in range(NCH // 2):
                c = data * (NCH // 2) + j
                send(f'dy_late{g}', dy_ref.at[g * GRP:(g + 1) * GRP, at(c * CH, CH)],
                     dyb.at[c, group_row(own_row, g)], partner, 'dy_far')

    barrier = pltpu.get_barrier_semaphore()
    for device in (mate, partner, peer):
        pl.semaphore_signal(barrier, inc=1, device_id=device, device_id_type=MESH)
    loads = [local(x_ref, xb.at[at(own_row, BLK)], 0), local(wq_ref, wq_raw, 1),
             local(wk_ref, wkv.at[0], 2), local(wv_ref, wkv.at[1], 3)]
    with jax.named_scope('barrier'):
        pl.semaphore_wait(barrier, 3)

    for p in range(NP):
        send(f'x_far{p}', x_ref.at[pl.ds(p * PIECE, PIECE)], xb.at[x_piece(own_row, p)], partner, 'x_far')
    send('x_mate', x_ref, xb.at[at(own_row, BLK)], mate)
    late_load = local(wo_ref, wo, 4)
    for c in range(NCH):
        own_chunk = dyb.at[c, at(own_row, BLK)]
        local(dy_ref.at[:, c * CH:(c + 1) * CH], own_chunk, 5)
        send('dy_mate', dy_ref.at[:, c * CH:(c + 1) * CH], own_chunk, mate)

    def project(xr, pieces):
        def put(dst, lo, value):
            for row, size, off in pieces:
                dst[row, lo:lo + HD] = value[off:off + size]
        for h in range(HEADS):
            put(q, h * HD, dot_nn(xr, wq4[core * HEADS + h]).astype(BF16))
        for n, (dst, dst_t) in enumerate(((k, k_t), (v, v_t))):
            value = dot_nn(xr, wkv[n]).astype(BF16)
            put(dst, 0, value)

    def flip_x(first_row):
        def step(t, carry):
            cols = at(t * 256, 256)
            for r in range(2):
                rows = at(first_row + r * BLK, BLK)
                x_t[cols, rows] = xb[rows, cols].T
            return carry
        lax.fori_loop(0, DIM // 256, step, 0)

    def flip_kv(first_row):
        for r in range(2):
            rows = at(first_row + r * BLK, BLK)
            k_t[:, rows] = k[rows, :].T
            v_t[:, rows] = v[rows, :].T

    with jax.named_scope('loads'):
        for copy in loads:
            copy.wait()

    with jax.named_scope('relay'):
        def relay(r, carry):
            rows = at(r * 128, 128, 128)
            for h in range(HEADS):
                wq4[core * HEADS + h, rows, :] = wq_raw[rows, h, :]
            return carry
        lax.fori_loop(0, DIM // 128, relay, 0)
    send('wq_mate', wq4.at[pl.ds(core * HEADS, HEADS)], wq4.at[pl.ds(core * HEADS, HEADS)], mate)

    arrived('x_mate', xb.at[at(mate_row, BLK)], mate)
    with jax.named_scope('proj1'):
        def project_near(r, carry):
            rows = at(near + r * BLK, BLK)
            project(xb[rows, :], [(rows, BLK, 0)])
            return carry
        lax.fori_loop(0, 2, project_near, 0)
        flip_kv(near)

    def forward_x(p):
        block = xb.at[x_piece(partner_row, p)]
        arrived(f'x_far{p}', block, partner)
        send(f'x_fwd{p}', block, block, mate, 'x_fwd', f'x_fwd{max(p, 1)}')

    def project_far(p):
        first, size = (0, 2 * PIECE) if p == 1 else (p * PIECE, PIECE)
        arrived(f'x_fwd{p}', xb.at[at(diag_row + first, size, PIECE)], mate)
        rows = [at(row + first, size, PIECE) for row in (partner_row, diag_row)]
        xr = jnp.concatenate([xb[r, :] for r in rows], axis=0)
        with jax.named_scope('proj2'):
            project(xr, [(rows[0], size, 0), (rows[1], size, size)])

    forward_x(0)
    with jax.named_scope('flip1'):
        flip_x(near)
    forward_x(1)
    project_far(1)
    late_load.wait()
    own_dy = dyb.at[:, at(own_row, BLK)]
    pltpu.make_async_copy(own_dy, own_dy, locs.at[5]).wait()
    arrived('dy_mate', dyb.at[:, at(mate_row, BLK)], mate)
    with jax.named_scope('do_near'):
        for half in range(HEADS):
            heads = slice(half * HD, (half + 1) * HD)
            acc = jnp.zeros((HD, 2 * BLK), F32)
            for c in range(NCH):
                acc += dot_nt(wo[heads, c * CH:(c + 1) * CH], dyb[c, at(near, 2 * BLK), :])
            do_t[heads, at(near, 2 * BLK)] = acc.astype(BF16)
        dkv[...] = jnp.zeros(dkv.shape, F32)
    forward_x(2)

    @pl.when(core == 0)
    def _():
        send_dy()
    project_far(2)
    forward_x(3)

    @pl.when(core == 1)
    def _():
        send_dy()
    project_far(3)
    flip_kv(far)

    def forward_dy(j):
        block = dyb.at[chunk_at(j), at(partner_row, BLK)]
        arrived(f'dy_far{j}', block, partner)
        send(f'dy_fwd{j}', block, block, mate, 'dy_fwd')

    mask = lax.broadcasted_iota(jnp.int32, (BLK, BLK), 0) <= lax.broadcasted_iota(jnp.int32, (BLK, BLK), 1)

    def scores(h, i):
        heads = slice(h * HD, (h + 1) * HD)
        cols = slice(i * BLK, (i + 1) * BLK)
        rows = (i + 1) * BLK
        qs = q[cols, heads] * jnp.asarray(SCALE, BF16)
        p_t[h, i * BLK:rows, cols] = jnp.where(mask, dot_nt(k[i * BLK:rows, :], qs), -jnp.inf)
        if i:
            p_t[h, :i * BLK, cols] = dot_nt(k[:i * BLK, :], qs)
        top = jnp.max(p_t[h, :rows, cols], axis=0, keepdims=True)
        e = jnp.exp(p_t[h, :rows, cols] - top)
        p_t[h, :rows, cols] = e
        p_inv[h, :, cols] = 1.0 / jnp.sum(e, axis=0, keepdims=True)

    def values(h, i):
        cols = slice(i * BLK, (i + 1) * BLK)
        rows = (i + 1) * BLK
        prob = (p_t[h, :rows, cols] * p_inv[h, :, cols]).astype(BF16)
        o_t[h * HD:(h + 1) * HD, cols] = dot_nn(v_t[:, :rows], prob).astype(BF16)

    def on_core(n, step):
        @pl.when(core == n)
        def _():
            step()

    with jax.named_scope('fwd'):
        for i in range(2):
            for h in range(HEADS):
                scores(h, i)
        on_core(1, lambda: forward_dy(0))
        for i in range(2, 4):
            for h in range(HEADS):
                scores(h, i)
        on_core(0, lambda: forward_dy(0))
        for i in range(4):
            for h in range(HEADS):
                values(h, i)

    def add_dkv(h, i, j, prob, ds):
        rows = slice(j * BLK, (j + 1) * BLK)
        cols = slice(i * BLK, (i + 1) * BLK)
        heads = at(h * HD, HD)
        dkv[0, rows, :] += dot_nn(ds, q[cols, heads])
        dkv[1, rows, :] += dot_nt(prob.astype(BF16), do_t[heads, cols])

    def backward_block(h, i, lo, size, keep):
        heads = slice(h * HD, (h + 1) * HD) if isinstance(h, int) else at(h * HD, HD)
        cols = slice(i * BLK + lo, i * BLK + lo + size)
        doi = do_t[heads, cols]
        delta = jnp.sum(doi.astype(F32) * o_t[heads, cols].astype(F32), axis=0, keepdims=True)
        inv = p_inv[h, :, cols]
        dqi = jnp.zeros((HD, size), F32)
        for j in range(i + 1):
            rows = slice(j * BLK, (j + 1) * BLK)
            prob = p_t[h, rows, cols] * inv
            ds = (prob * (dot_nn(v[rows, :], doi) - delta)).astype(BF16)
            dqi += dot_nn(k_t[:, rows], ds)
            if keep:
                ds_t[h, rows, (i % 2) * BLK + lo:(i % 2) * BLK + lo + size] = ds
            else:
                add_dkv(h, i, j, prob, ds)
        dq[h, cols, :] = (dqi * SCALE).astype(BF16).T

    def over_heads(step):
        def one(h, carry):
            step(h)
            return carry
        lax.fori_loop(0, HEADS, one, 0)

    def take_chunk(j):
        c = chunk_at(j)
        arrived(f'dy_fwd{j}', dyb.at[c, at(diag_row, BLK)], mate)
        for h in range(HEADS):
            heads = slice(h * HD, (h + 1) * HD)
            dwo_send[j, heads, :] = dot_nn(o_t[heads, :], dyb[c]).astype(BF16)
            send('dwo', dwo_send.at[j, heads], dwo_recv.at[j, heads], peer)
        part = dot_nt(wo[:, at(c * CH, CH)], dyb[c, at(far, 2 * BLK), :])
        if j == 0:
            do_acc[...] = part
        else:
            do_acc[...] += part

    split = chunk_at(NCH // 2 - 1)

    def forward_split(g):
        block = dyb.at[split, group_row(partner_row, g)]
        arrived(f'dy_split{g}', block, partner)
        send(f'dy_sfwd{g}', block, block, mate, 'dy_fwd')

    def take_split():
        arrived('dy_sfwd1', dyb.at[split, group_row(diag_row, 1)], mate)
        with jax.named_scope('dwo3'):
            dwo_send[NCH // 2 - 1] = dot_nn(o_t[...], dyb[split]).astype(BF16)
            send('dwo', dwo_send.at[NCH // 2 - 1], dwo_recv.at[NCH // 2 - 1], peer)

    def forward_group(g):
        block = dyb.at[late, group_row(partner_row, g)]
        arrived(f'dy_late{g}', block, partner)
        send(f'dy_lfwd{g}', block, block, mate, 'dy_lfwd')

    def finish_do(rows, g):
        with jax.named_scope('do_late'):
            cols = [group_row(row, g) for row in rows]
            accs = [do_acc[:, group_row(row - far, g)] for row in rows]
            for c in [split] + [data * (NCH // 2) + j for j in range(NCH // 2)]:
                part = dot_nt(wo[:, at(c * CH, CH)], jnp.concatenate([dyb[c, n, :] for n in cols], axis=0))
                accs = [acc + part[:, n * GRP:(n + 1) * GRP] for n, acc in enumerate(accs)]
            for n, acc in zip(cols, accs):
                do_t[:, n] = acc.astype(BF16)

    def far_blocks(g, heads, blocks_of):
        for c in range(2):
            for n in range(2):
                @pl.when((chip == c) & (core == n))
                def _(c=c, n=n):
                    with jax.named_scope('bwd_far'):
                        for h in heads:
                            for b in blocks_of(n):
                                backward_block(h, 2 * (1 - c) + b, g * GRP, GRP, True)

    def exchange_dq(g):
        send(f'dq_far{g}', dq.at[:, group_row(diag_row, g)], dq_mate.at[1 - chip, :, g * GRP:(g + 1) * GRP], mate, 'dq')

    def arrived_dq(g):
        arrived(f'dq_far{g}', dq_mate.at[1 - chip, :, g * GRP:(g + 1) * GRP], mate)

    def dx_cols(block, lo, size, cols):
        rows = at((block * 2 + core) * BLK + lo, size, GRP)
        acc = jnp.zeros((size, cols.stop - cols.start), F32)
        for h in range(HEADS):
            acc += dot_nt(dq[h, rows, :], wq4[core * HEADS + h, cols, :])
            acc += dot_nt(dq_mate[block, h, lo:lo + size], wq4[(1 - core) * HEADS + h, cols, :])
        return acc

    def send_dx(g, pieces):
        with jax.named_scope('dx'):
            for j in pieces:
                n = g * NDX + j
                dx_send[n] = dx_cols(1 - chip, g * GRP, GRP, slice(j * DXC, (j + 1) * DXC)).astype(BF16)
                send(f'dx{max(n, NDX + 1)}' if g else 'dx', dx_send.at[n], dx_recv.at[n], partner, 'dx')

    take_chunk(0)
    forward_dy(1)
    forward_dy(2)
    take_chunk(1)
    take_chunk(2)

    for c in range(2):
        @pl.when(chip == c)
        def _(c=c):
            def step(h):
                for i in (2 * c, 2 * c + 1):
                    backward_block(h, i, 0, BLK, False)
            with jax.named_scope('bwd_near'):
                over_heads(step)
    send('dq_near', dq.at[:, at(mate_row, BLK)], dq_mate.at[chip], mate, 'dq')
    with jax.named_scope('flip2'):
        flip_x(far)
    arrived('wq_mate', wq4.at[pl.ds((1 - core) * HEADS, HEADS)], mate)
    def send_dwq(r, heads):
        with jax.named_scope('dwq'):
            rows = at((1 - data) * HALF + r * 256, 256)
            for h in heads:
                dwq_send[r, h] = dot_nn(x_t[rows, :], dq[h]).astype(BF16)
                send('dwq' if r < 3 else 'dwq3', dwq_send.at[r, h], dwq_recv.at[r, h], peer, 'dwq')

    forward_split(0)
    forward_group(0)
    finish_do([partner_row], 0)
    far_blocks(0, range(HEADS), lambda n: (n,))
    forward_split(1)
    arrived('dy_sfwd0', dyb.at[split, group_row(diag_row, 0)], mate)
    arrived('dy_lfwd0', dyb.at[late, group_row(diag_row, 0)], mate)
    finish_do([diag_row], 0)
    far_blocks(0, range(HEADS), lambda n: (1 - n,))
    exchange_dq(0)
    take_split()
    arrived_dq(0)
    send_dx(0, (0, 1))
    forward_group(1)
    send_dx(0, (2, 3))
    arrived('dy_lfwd1', dyb.at[late, group_row(diag_row, 1)], mate)
    finish_do([partner_row, diag_row], 1)
    for h in range(HEADS):
        for c in range(2):
            @pl.when(chip == c)
            def _(c=c):
                with jax.named_scope('bwd_far'):
                    for b in range(2):
                        backward_block(h, 2 * (1 - c) + b, GRP, GRP, True)
        for r in range(2):
            send_dwq(r, [h])
    exchange_dq(1)
    for c in range(2):
        @pl.when(chip == c)
        def _(c=c):
            def step(h):
                for i in (2 * (1 - c), 2 * (1 - c) + 1):
                    cols = slice(i * BLK, (i + 1) * BLK)
                    for j in range(i + 1):
                        rows = slice(j * BLK, (j + 1) * BLK)
                        add_dkv(h, i, j, p_t[h, rows, cols] * p_inv[h, :, cols],
                                ds_t[h, rows, (i % 2) * BLK:(i % 2 + 1) * BLK])
            with jax.named_scope('dkv'):
                over_heads(step)
    send('dkv_mate', dkv.at[1 - core], dkv_mate, mate)

    for r in range(2, 4):
        send_dwq(r, range(HEADS))
    arrived_dq(1)
    arrived('dkv_mate', dkv_mate, mate)
    factor = jnp.where(core == 0, SCALE, 1.0).astype(F32)
    summed = (dkv[core] + dkv_mate[...]) * factor
    dkv_mate[...] = summed
    dkv_send[...] = summed.astype(BF16)
    send('dkv_far', dkv_send, dkv_part, partner)
    send_dx(1, range(NDX))

    arrived('dq_near', dq_mate.at[chip], mate)
    for j in range(4):
        cols = slice(j * 512, (j + 1) * 512)
        dx_own[:, cols] = dx_cols(chip, 0, BLK, cols)
    arrived('dwo', dwo_recv, peer)
    for j in range(NCH // 2):
        cols = slice(j * CH, (j + 1) * CH)
        dwo_out[:, cols] = dot_nn(o_t[...], dyb[chunk_at(NCH // 2 + j)]) + dwo_recv[j].astype(F32)

    arrived('dkv_far', dkv_part, partner)
    dkv_full[core] = (dkv_mate[...] + dkv_part[...].astype(F32)).astype(BF16)
    send('dkv_full', dkv_full.at[core], dkv_full.at[core], mate)
    arrived('dkv_full', dkv_full.at[1 - core], mate)
    for n in range(2):
        peer_rows = at((model * 2 + 1 - data) * 256, 256)
        dwkv_send[n] = dot_nn(x_t[peer_rows, :], dkv_full[n]).astype(BF16)
    send('dwkv', dwkv_send, dwkv_recv, peer)
    kept_rows = at((model * 2 + data) * 256, 256)
    dwk_out[...] = dot_nn(x_t[kept_rows, :], dkv_full[0])
    dwv_out[...] = dot_nn(x_t[kept_rows, :], dkv_full[1])
    for j in range(4):
        cols = slice(j * 512, (j + 1) * 512)
        dx_own[:, cols] += (dot_nt(dkv_full[0, at(own_row, BLK), :], wkv[0, cols, :])
                            + dot_nt(dkv_full[1, at(own_row, BLK), :], wkv[1, cols, :]))

    def finish_dx(n):
        rows = slice(n // NDX * GRP, (n // NDX + 1) * GRP)
        cols = slice(n % NDX * DXC, (n % NDX + 1) * DXC)
        dx_out[rows, cols] = (dx_own[rows, cols] + dx_recv[n].astype(F32)).astype(BF16)

    arrived('dx', dx_recv.at[:NDX], partner)
    for n in range(NDX):
        finish_dx(n)
    arrived('dwq', dwq_recv.at[:3], peer)
    for r in range(4):
        if r == 3:
            arrived('dwq3', dwq_recv.at[3], peer)
        with jax.named_scope('dwq_sum'):
            rows = at(data * HALF + r * 256, 256)
            for h in range(HEADS):
                value = dot_nn(x_t[rows, :], dq[h]) + dwq_recv[r, h].astype(F32)
                dwq_out[r * 256:(r + 1) * 256, h, :] = value
    arrived(f'dx{NDX + 1}', dx_recv.at[NDX:NDX + 2], partner)
    for n in range(NDX, 2 * NDX):
        if n > NDX + 1:
            arrived(f'dx{n}', dx_recv.at[n], partner)
        finish_dx(n)
    arrived('dwkv', dwkv_recv, peer)
    dwk_out[...] += dwkv_recv[0].astype(F32)
    dwv_out[...] += dwkv_recv[1].astype(F32)
    with jax.named_scope('sends'):
        for group in ('inputs', 'mib', 'pair'):
            sent(group, xb)
        sent('dkv', dkv_full)
        sent('dq', dq_mate)
        sent('dwkv', dwkv_send)
    assert len(groups) == sems.shape[0] and len(slots) == recvs.shape[0]


def fused_step(x, dy, wq, wk, wv, wo):
    any_spec = pl.BlockSpec(memory_space=pl.ANY)
    vmem_spec = pl.BlockSpec(memory_space=pltpu.VMEM)
    scratch = [
        pltpu.VMEM((SEQ, DIM), BF16),
        pltpu.VMEM((DIM, SEQ), BF16),
        pltpu.VMEM((NCH, SEQ, CH), BF16),
        pltpu.VMEM((DIM, HEADS, HD), BF16),
        pltpu.VMEM((2 * HEADS, DIM, HD), BF16),
        pltpu.VMEM((2, DIM, HD), BF16),
        pltpu.VMEM((HEADS * HD, DIM), BF16),
        pltpu.VMEM((SEQ, HEADS * HD), BF16),
        pltpu.VMEM((SEQ, HD), BF16),
        pltpu.VMEM((SEQ, HD), BF16),
        pltpu.VMEM((HD, SEQ), BF16),
        pltpu.VMEM((HD, SEQ), BF16),
        pltpu.VMEM((HEADS, SEQ, SEQ), F32),
        pltpu.VMEM((HEADS, 1, SEQ), F32),
        pltpu.VMEM((HEADS, SEQ, 2 * BLK), BF16),
        pltpu.VMEM((HEADS * HD, SEQ), BF16),
        pltpu.VMEM((HEADS * HD, 2 * BLK), F32),
        pltpu.VMEM((HEADS * HD, SEQ), BF16),
        pltpu.VMEM((2, SEQ, HD), F32),
        pltpu.VMEM((SEQ, HD), F32),
        pltpu.VMEM((SEQ, HD), BF16),
        pltpu.VMEM((SEQ, HD), BF16),
        pltpu.VMEM((2, SEQ, HD), BF16),
        pltpu.VMEM((HEADS, SEQ, HD), BF16),
        pltpu.VMEM((2, HEADS, BLK, HD), BF16),
        pltpu.VMEM((NCH // 2, HEADS * HD, CH), BF16),
        pltpu.VMEM((NCH // 2, HEADS * HD, CH), BF16),
        pltpu.VMEM((4, HEADS, HALF // 4, HD), BF16),
        pltpu.VMEM((4, HEADS, HALF // 4, HD), BF16),
        pltpu.VMEM((BLK, DIM), F32),
        pltpu.VMEM((2 * NDX, GRP, DXC), BF16),
        pltpu.VMEM((2 * NDX, GRP, DXC), BF16),
        pltpu.VMEM((2, 256, HD), BF16),
        pltpu.VMEM((2, 256, HD), BF16),
        pltpu.SemaphoreType.DMA((6,)),
        pltpu.SemaphoreType.DMA((38,)),
        pltpu.SemaphoreType.DMA((6,)),
    ]
    return pl.pallas_call(
        body,
        out_shape=(pltpu.VMEM((BLK, DIM), BF16),
                   pltpu.VMEM((HALF, HEADS, HD), F32),
                   pltpu.VMEM((256, HD), F32),
                   pltpu.VMEM((256, HD), F32),
                   pltpu.VMEM((HEADS * HD, HALF), F32)),
        in_specs=[any_spec] * 6,
        out_specs=(vmem_spec,) * 5,
        scratch_shapes=scratch,
        compiler_params=pltpu.CompilerParams(collective_id=0, has_side_effects=True,
                                             vmem_limit_bytes=58 * 2 ** 20),
        name='attention_backward',
    )(x, dy, wq, wk, wv, wo)


def flush_body(*refs):
    sources, results, sems = refs[:5], refs[5:10], refs[10]
    copies = [pltpu.make_async_copy(a, b, sems.at[n]) for n, (a, b) in enumerate(zip(sources, results))]
    for copy in copies:
        copy.start()
    for copy in copies:
        copy.wait()


def flush(*arrays):
    any_spec = pl.BlockSpec(memory_space=pl.ANY)
    return pl.pallas_call(
        flush_body,
        out_shape=tuple(jax.ShapeDtypeStruct(a.shape, a.dtype) for a in arrays),
        in_specs=[any_spec] * 5,
        out_specs=(any_spec,) * 5,
        scratch_shapes=[pltpu.SemaphoreType.DMA((5,))],
        compiler_params=pltpu.CompilerParams(vmem_limit_bytes=2 ** 20),
        name='write_results',
    )(*arrays)


def solution(mesh):
    tok_spec = P(('pod', 'data'), 'model', None)

    def device_step(x_loc, dy_loc, w_q, w_k, w_v, w_o):
        dx, dwq, dwk, dwv, dwo = flush(*fused_step(x_loc[0], dy_loc[0], w_q, w_k[0], w_v[0],
                                                   w_o.reshape(HEADS * HD, DIM)))
        return dx[None], dwq, dwk, dwv, dwo.reshape(HEADS, HD, HALF)

    kv_rows = P(('pod', 'model', 'data'), None)
    return jax.shard_map(device_step, mesh=mesh,
                         in_specs=(tok_spec, tok_spec, P(None, 'model', None), P(), P(), P('model', None, None)),
                         out_specs=(tok_spec, P(('pod', 'data'), 'model', None), kv_rows, kv_rows,
                                    P(('pod', 'model'), None, 'data')),
                         check_vma=False)
```

```python
import functools

import jax
import jax.numpy as jnp
from jax import lax
from jax.experimental import pallas as pl
from jax.experimental.pallas import tpu as pltpu
from jax.sharding import PartitionSpec as P

F32 = jnp.float32
BF16 = jnp.bfloat16
SEQ = 1024
BLK = 256
DIM = 2048
HD = 256
HEADS = 2
CH = 256
NCH = DIM // CH
DXC = 512
NDX = DIM // DXC
GRP = 128
SHARED = {**dict.fromkeys(('x_far', 'x_mate', 'dy_far', 'dy_mate'), 'inputs'),
          **dict.fromkeys(('x_fwd', 'dwo', 'dwq', 'dx'), 'mib'),
          **dict.fromkeys(('wq_mate', 'dy_fwd', 'dy_lfwd', 'dkv_mate'), 'pair'),
          **dict.fromkeys(('dkv_far', 'dkv_full'), 'dkv'), 'dq': 'dq', 'dwkv': 'dwkv'}
PIECE = 64
NP = BLK // PIECE
HALF = DIM // 2
SCALE = HD ** -0.5
MESH = pl.DeviceIdType.MESH


def dot_nn(a, b):
    return lax.dot_general(a, b, (((1,), (0,)), ((), ())), preferred_element_type=F32)


def dot_nt(a, b):
    return lax.dot_general(a, b, (((1,), (1,)), ((), ())), preferred_element_type=F32)


def at(start, size, align=256):
    return pl.ds(pl.multiple_of(start, align), size)


def body(x_ref, dy_ref, wq_ref, wk_ref, wv_ref, wo_ref,
         dx_out, dwq_out, dwk_out, dwv_out, dwo_out,
         xb, x_t, dyb, wq_raw, wq4, wkv, wo, q, k, v, k_t, v_t, p_t, p_inv, ds_t, o_t, do_acc, do_t,
         dkv, dkv_mate, dkv_send, dkv_part, dkv_full, dq, dq_mate,
         dwo_send, dwo_recv, dwq_send, dwq_recv,
         dx_own, dx_send, dx_recv, dwkv_send, dwkv_recv,
         sems, recvs, locs):
    model = lax.axis_index('model')
    data = lax.axis_index('data')
    chip = model // 2
    core = model % 2
    mate = {'model': chip * 2 + 1 - core}
    partner = {'model': (1 - chip) * 2 + core}
    peer = {'data': 1 - data}
    own_row = model * BLK
    mate_row = (chip * 2 + 1 - core) * BLK
    partner_row = ((1 - chip) * 2 + core) * BLK
    diag_row = ((1 - chip) * 2 + 1 - core) * BLK
    near = chip * 2 * BLK
    far = (1 - chip) * 2 * BLK

    groups = {}
    slots = {}
    devices = {}

    def send(name, src, dst, device, group=None, part=None):
        group = SHARED[group or name]
        devices[group] = device
        copy = pltpu.make_async_remote_copy(
            src_ref=src, dst_ref=dst, send_sem=sems.at[groups.setdefault(group, len(groups))],
            recv_sem=recvs.at[slots.setdefault(part or name, len(slots))],
            device_id=device, device_id_type=MESH)
        copy.start()

    def arrived(name, dst, device):
        with jax.named_scope('w_' + name):
            pltpu.make_async_remote_copy(
                src_ref=dst, dst_ref=dst, send_sem=sems.at[0],
                recv_sem=recvs.at[slots.setdefault(name, len(slots))],
                device_id=device, device_id_type=MESH).wait_recv()

    def sent(group, src):
        pltpu.make_async_remote_copy(src_ref=src, dst_ref=src, send_sem=sems.at[groups[group]], recv_sem=recvs.at[0],
                                     device_id=devices[group], device_id_type=MESH).wait_send()

    def local(src, dst, n):
        copy = pltpu.make_async_copy(src, dst, locs.at[n])
        copy.start()
        return copy

    def chunk_at(j):
        return lax.rem((1 - data) * (NCH // 2) + j, NCH)

    def x_piece(row, p):
        return at(row + p * PIECE, PIECE, PIECE)

    late = pl.ds(data * (NCH // 2), NCH // 2)

    def group_row(row, g):
        return at(row + g * GRP, GRP, GRP)

    def send_dy():
        for j in range(NCH // 2 - 1):
            c = chunk_at(j)
            send(f'dy_far{j}', dy_ref.at[:, at(c * CH, CH)], dyb.at[c, at(own_row, BLK)], partner, 'dy_far')
        for g in range(2):
            c = chunk_at(NCH // 2 - 1)
            send(f'dy_split{g}', dy_ref.at[g * GRP:(g + 1) * GRP, at(c * CH, CH)],
                 dyb.at[c, group_row(own_row, g)], partner, 'dy_far')
            for j in range(NCH // 2):
                c = data * (NCH // 2) + j
                send(f'dy_late{g}', dy_ref.at[g * GRP:(g + 1) * GRP, at(c * CH, CH)],
                     dyb.at[c, group_row(own_row, g)], partner, 'dy_far')

    barrier = pltpu.get_barrier_semaphore()
    for device in (mate, partner, peer):
        pl.semaphore_signal(barrier, inc=1, device_id=device, device_id_type=MESH)
    loads = [local(x_ref, xb.at[at(own_row, BLK)], 0), local(wq_ref, wq_raw, 1),
             local(wk_ref, wkv.at[0], 2), local(wv_ref, wkv.at[1], 3)]
    with jax.named_scope('barrier'):
        pl.semaphore_wait(barrier, 3)

    for p in range(NP):
        send(f'x_far{p}', x_ref.at[pl.ds(p * PIECE, PIECE)], xb.at[x_piece(own_row, p)], partner, 'x_far')
    send('x_mate', x_ref, xb.at[at(own_row, BLK)], mate)
    late_load = local(wo_ref, wo, 4)
    for c in range(NCH):
        own_chunk = dyb.at[c, at(own_row, BLK)]
        local(dy_ref.at[:, c * CH:(c + 1) * CH], own_chunk, 5)
        send('dy_mate', dy_ref.at[:, c * CH:(c + 1) * CH], own_chunk, mate)

    def project(xr, pieces):
        def put(dst, lo, value):
            for row, size, off in pieces:
                dst[row, lo:lo + HD] = value[off:off + size]
        for h in range(HEADS):
            put(q, h * HD, dot_nn(xr, wq4[core * HEADS + h]).astype(BF16))
        for n, (dst, dst_t) in enumerate(((k, k_t), (v, v_t))):
            value = dot_nn(xr, wkv[n]).astype(BF16)
            put(dst, 0, value)

    def flip_x(first_row):
        def step(t, carry):
            cols = at(t * 256, 256)
            for r in range(2):
                rows = at(first_row + r * BLK, BLK)
                x_t[cols, rows] = xb[rows, cols].T
            return carry
        lax.fori_loop(0, DIM // 256, step, 0)

    def flip_kv(first_row, pairs):
        for r in range(2):
            rows = at(first_row + r * BLK, BLK)
            for src, dst in pairs:
                dst[:, rows] = src[rows, :].T

    with jax.named_scope('loads'):
        for copy in loads:
            copy.wait()

    with jax.named_scope('relay'):
        def relay(r, carry):
            rows = at(r * 128, 128, 128)
            for h in range(HEADS):
                wq4[core * HEADS + h, rows, :] = wq_raw[rows, h, :]
            return carry
        lax.fori_loop(0, DIM // 128, relay, 0)
    send('wq_mate', wq4.at[pl.ds(core * HEADS, HEADS)], wq4.at[pl.ds(core * HEADS, HEADS)], mate)

    arrived('x_mate', xb.at[at(mate_row, BLK)], mate)
    with jax.named_scope('proj1'):
        def project_near(r, carry):
            rows = at(near + r * BLK, BLK)
            project(xb[rows, :], [(rows, BLK, 0)])
            return carry
        lax.fori_loop(0, 2, project_near, 0)
        flip_kv(near, ((k, k_t), (v, v_t)))

    def forward_x(p):
        block = xb.at[x_piece(partner_row, p)]
        arrived(f'x_far{p}', block, partner)
        send(f'x_fwd{p}', block, block, mate, 'x_fwd', f'x_fwd{max(p, 1)}')

    def project_far(p):
        first, size = (0, 2 * PIECE) if p == 1 else (p * PIECE, PIECE)
        arrived(f'x_fwd{p}', xb.at[at(diag_row + first, size, PIECE)], mate)
        rows = [at(row + first, size, PIECE) for row in (partner_row, diag_row)]
        xr = jnp.concatenate([xb[r, :] for r in rows], axis=0)
        with jax.named_scope('proj2'):
            project(xr, [(rows[0], size, 0), (rows[1], size, size)])

    forward_x(0)
    with jax.named_scope('flip1'):
        flip_x(near)
    forward_x(1)
    project_far(1)
    late_load.wait()
    own_dy = dyb.at[:, at(own_row, BLK)]
    pltpu.make_async_copy(own_dy, own_dy, locs.at[5]).wait()
    arrived('dy_mate', dyb.at[:, at(mate_row, BLK)], mate)
    with jax.named_scope('do_near'):
        for half in range(HEADS):
            heads = slice(half * HD, (half + 1) * HD)
            acc = jnp.zeros((HD, 2 * BLK), F32)
            for c in range(NCH):
                acc += dot_nt(wo[heads, c * CH:(c + 1) * CH], dyb[c, at(near, 2 * BLK), :])
            do_t[heads, at(near, 2 * BLK)] = acc.astype(BF16)
        dkv[...] = jnp.zeros(dkv.shape, F32)
    forward_x(2)

    @pl.when(core == 0)
    def _():
        send_dy()
    project_far(2)
    forward_x(3)

    @pl.when(core == 1)
    def _():
        send_dy()
    project_far(3)
    flip_kv(far, ((v, v_t),))

    def forward_dy(j):
        block = dyb.at[chunk_at(j), at(partner_row, BLK)]
        arrived(f'dy_far{j}', block, partner)
        send(f'dy_fwd{j}', block, block, mate, 'dy_fwd')

    mask = lax.broadcasted_iota(jnp.int32, (BLK, BLK), 0) <= lax.broadcasted_iota(jnp.int32, (BLK, BLK), 1)

    def scores(h, i):
        heads = slice(h * HD, (h + 1) * HD)
        cols = slice(i * BLK, (i + 1) * BLK)
        rows = (i + 1) * BLK
        qs = q[cols, heads] * jnp.asarray(SCALE, BF16)
        p_t[h, i * BLK:rows, cols] = jnp.where(mask, dot_nt(k[i * BLK:rows, :], qs), -jnp.inf)
        if i:
            p_t[h, :i * BLK, cols] = dot_nt(k[:i * BLK, :], qs)
        top = jnp.max(p_t[h, :rows, cols], axis=0, keepdims=True)
        e = jnp.exp(p_t[h, :rows, cols] - top)
        p_t[h, :rows, cols] = e
        p_inv[h, :, cols] = 1.0 / jnp.sum(e, axis=0, keepdims=True)

    def values(h, i):
        cols = slice(i * BLK, (i + 1) * BLK)
        rows = (i + 1) * BLK
        prob = (p_t[h, :rows, cols] * p_inv[h, :, cols]).astype(BF16)
        o_t[h * HD:(h + 1) * HD, cols] = dot_nn(v_t[:, :rows], prob).astype(BF16)

    def on_core(n, step):
        @pl.when(core == n)
        def _():
            step()

    with jax.named_scope('fwd'):
        for i in range(2):
            for h in range(HEADS):
                scores(h, i)
        on_core(1, lambda: forward_dy(0))
        for i in range(2, 4):
            for h in range(HEADS):
                scores(h, i)
        on_core(0, lambda: forward_dy(0))
        for i in range(4):
            for h in range(HEADS):
                values(h, i)

    def add_dkv(h, i, j, prob, ds):
        rows = slice(j * BLK, (j + 1) * BLK)
        cols = slice(i * BLK, (i + 1) * BLK)
        heads = at(h * HD, HD)
        dkv[0, rows, :] += dot_nn(ds, q[cols, heads])
        dkv[1, rows, :] += dot_nt(prob.astype(BF16), do_t[heads, cols])

    def backward_block(h, i, lo, size, keep):
        heads = slice(h * HD, (h + 1) * HD) if isinstance(h, int) else at(h * HD, HD)
        cols = slice(i * BLK + lo, i * BLK + lo + size)
        doi = do_t[heads, cols]
        delta = jnp.sum(doi.astype(F32) * o_t[heads, cols].astype(F32), axis=0, keepdims=True)
        inv = p_inv[h, :, cols]
        dqi = jnp.zeros((HD, size), F32)
        for j in range(i + 1):
            rows = slice(j * BLK, (j + 1) * BLK)
            prob = p_t[h, rows, cols] * inv
            ds = (prob * (dot_nn(v[rows, :], doi) - delta)).astype(BF16)
            dqi += dot_nn(k_t[:, rows], ds)
            if keep:
                ds_t[h, rows, (i % 2) * BLK + lo:(i % 2) * BLK + lo + size] = ds
            else:
                add_dkv(h, i, j, prob, ds)
        dq[h, cols, :] = (dqi * SCALE).astype(BF16).T

    def over_heads(step):
        def one(h, carry):
            step(h)
            return carry
        lax.fori_loop(0, HEADS, one, 0)

    def take_chunk(j):
        c = chunk_at(j)
        arrived(f'dy_fwd{j}', dyb.at[c, at(diag_row, BLK)], mate)
        for h in range(HEADS):
            heads = slice(h * HD, (h + 1) * HD)
            dwo_send[j, heads, :] = dot_nn(o_t[heads, :], dyb[c]).astype(BF16)
            send('dwo', dwo_send.at[j, heads], dwo_recv.at[j, heads], peer)
        part = dot_nt(wo[:, at(c * CH, CH)], dyb[c, at(far, 2 * BLK), :])
        if j == 0:
            do_acc[...] = part
        else:
            do_acc[...] += part

    split = chunk_at(NCH // 2 - 1)

    def forward_split(g):
        block = dyb.at[split, group_row(partner_row, g)]
        arrived(f'dy_split{g}', block, partner)
        send(f'dy_sfwd{g}', block, block, mate, 'dy_fwd')

    def take_split():
        arrived('dy_sfwd1', dyb.at[split, group_row(diag_row, 1)], mate)
        with jax.named_scope('dwo3'):
            dwo_send[NCH // 2 - 1] = dot_nn(o_t[...], dyb[split]).astype(BF16)
            send('dwo', dwo_send.at[NCH // 2 - 1], dwo_recv.at[NCH // 2 - 1], peer)

    def forward_group(g):
        block = dyb.at[late, group_row(partner_row, g)]
        arrived(f'dy_late{g}', block, partner)
        send(f'dy_lfwd{g}', block, block, mate, 'dy_lfwd')

    def finish_do(rows, g):
        with jax.named_scope('do_late'):
            cols = [group_row(row, g) for row in rows]
            accs = [do_acc[:, group_row(row - far, g)] for row in rows]
            for c in [split] + [data * (NCH // 2) + j for j in range(NCH // 2)]:
                part = dot_nt(wo[:, at(c * CH, CH)], jnp.concatenate([dyb[c, n, :] for n in cols], axis=0))
                accs = [acc + part[:, n * GRP:(n + 1) * GRP] for n, acc in enumerate(accs)]
            for n, acc in zip(cols, accs):
                do_t[:, n] = acc.astype(BF16)

    def far_blocks(g, heads, blocks_of):
        for c in range(2):
            for n in range(2):
                @pl.when((chip == c) & (core == n))
                def _(c=c, n=n):
                    with jax.named_scope('bwd_far'):
                        for h in heads:
                            for b in blocks_of(n):
                                backward_block(h, 2 * (1 - c) + b, g * GRP, GRP, True)

    def exchange_dq(g):
        send(f'dq_far{g}', dq.at[:, group_row(diag_row, g)], dq_mate.at[1 - chip, :, g * GRP:(g + 1) * GRP], mate, 'dq')

    def arrived_dq(g):
        arrived(f'dq_far{g}', dq_mate.at[1 - chip, :, g * GRP:(g + 1) * GRP], mate)

    def dx_cols(block, lo, size, cols):
        rows = at((block * 2 + core) * BLK + lo, size, GRP)
        acc = jnp.zeros((size, cols.stop - cols.start), F32)
        for h in range(HEADS):
            acc += dot_nt(dq[h, rows, :], wq4[core * HEADS + h, cols, :])
            acc += dot_nt(dq_mate[block, h, lo:lo + size], wq4[(1 - core) * HEADS + h, cols, :])
        return acc

    def send_dx(g, pieces):
        with jax.named_scope('dx'):
            for j in pieces:
                n = g * NDX + j
                dx_send[n] = dx_cols(1 - chip, g * GRP, GRP, slice(j * DXC, (j + 1) * DXC)).astype(BF16)
                send(f'dx{max(n, NDX + 1)}' if g else 'dx', dx_send.at[n], dx_recv.at[n], partner, 'dx')

    take_chunk(0)
    forward_dy(1)
    forward_dy(2)
    take_chunk(1)
    take_chunk(2)
    flip_kv(far, ((k, k_t),))

    for c in range(2):
        @pl.when(chip == c)
        def _(c=c):
            def step(h):
                for i in (2 * c, 2 * c + 1):
                    backward_block(h, i, 0, BLK, False)
            with jax.named_scope('bwd_near'):
                over_heads(step)
    send('dq_near', dq.at[:, at(mate_row, BLK)], dq_mate.at[chip], mate, 'dq')
    with jax.named_scope('flip2'):
        flip_x(far)
    arrived('wq_mate', wq4.at[pl.ds((1 - core) * HEADS, HEADS)], mate)
    def send_dwq(r, heads):
        with jax.named_scope('dwq'):
            rows = at((1 - data) * HALF + r * 256, 256)
            for h in heads:
                dwq_send[r, h] = dot_nn(x_t[rows, :], dq[h]).astype(BF16)
                send('dwq' if r < 3 else 'dwq3', dwq_send.at[r, h], dwq_recv.at[r, h], peer, 'dwq')

    forward_split(0)
    forward_group(0)
    finish_do([partner_row], 0)
    far_blocks(0, range(HEADS), lambda n: (n,))
    forward_split(1)
    arrived('dy_sfwd0', dyb.at[split, group_row(diag_row, 0)], mate)
    arrived('dy_lfwd0', dyb.at[late, group_row(diag_row, 0)], mate)
    finish_do([diag_row], 0)
    far_blocks(0, range(HEADS), lambda n: (1 - n,))
    exchange_dq(0)
    take_split()
    arrived_dq(0)
    send_dx(0, (0, 1))
    forward_group(1)
    send_dx(0, (2, 3))
    arrived('dy_lfwd1', dyb.at[late, group_row(diag_row, 1)], mate)
    finish_do([partner_row, diag_row], 1)
    for h in range(HEADS):
        for c in range(2):
            @pl.when(chip == c)
            def _(c=c):
                with jax.named_scope('bwd_far'):
                    for b in range(2):
                        backward_block(h, 2 * (1 - c) + b, GRP, GRP, True)
        for r in range(2):
            send_dwq(r, [h])
    exchange_dq(1)
    for c in range(2):
        @pl.when(chip == c)
        def _(c=c):
            def step(h):
                for i in (2 * (1 - c), 2 * (1 - c) + 1):
                    cols = slice(i * BLK, (i + 1) * BLK)
                    for j in range(i + 1):
                        rows = slice(j * BLK, (j + 1) * BLK)
                        add_dkv(h, i, j, p_t[h, rows, cols] * p_inv[h, :, cols],
                                ds_t[h, rows, (i % 2) * BLK:(i % 2 + 1) * BLK])
            with jax.named_scope('dkv'):
                over_heads(step)
    send('dkv_mate', dkv.at[1 - core], dkv_mate, mate)

    for r in range(2, 4):
        send_dwq(r, range(HEADS))
    arrived_dq(1)
    arrived('dkv_mate', dkv_mate, mate)
    factor = jnp.where(core == 0, SCALE, 1.0).astype(F32)
    summed = (dkv[core] + dkv_mate[...]) * factor
    dkv_mate[...] = summed
    dkv_send[...] = summed.astype(BF16)
    send('dkv_far', dkv_send, dkv_part, partner)
    send_dx(1, range(NDX))

    arrived('dq_near', dq_mate.at[chip], mate)
    for j in range(4):
        cols = slice(j * 512, (j + 1) * 512)
        dx_own[:, cols] = dx_cols(chip, 0, BLK, cols)
    arrived('dwo', dwo_recv, peer)
    for j in range(NCH // 2):
        cols = slice(j * CH, (j + 1) * CH)
        dwo_out[:, cols] = dot_nn(o_t[...], dyb[chunk_at(NCH // 2 + j)]) + dwo_recv[j].astype(F32)

    arrived('dkv_far', dkv_part, partner)
    dkv_full[core] = (dkv_mate[...] + dkv_part[...].astype(F32)).astype(BF16)
    send('dkv_full', dkv_full.at[core], dkv_full.at[core], mate)
    arrived('dkv_full', dkv_full.at[1 - core], mate)
    for n in range(2):
        peer_rows = at((model * 2 + 1 - data) * 256, 256)
        dwkv_send[n] = dot_nn(x_t[peer_rows, :], dkv_full[n]).astype(BF16)
    send('dwkv', dwkv_send, dwkv_recv, peer)
    kept_rows = at((model * 2 + data) * 256, 256)
    dwk_out[...] = dot_nn(x_t[kept_rows, :], dkv_full[0])
    dwv_out[...] = dot_nn(x_t[kept_rows, :], dkv_full[1])
    for j in range(4):
        cols = slice(j * 512, (j + 1) * 512)
        dx_own[:, cols] += (dot_nt(dkv_full[0, at(own_row, BLK), :], wkv[0, cols, :])
                            + dot_nt(dkv_full[1, at(own_row, BLK), :], wkv[1, cols, :]))

    def finish_dx(n):
        rows = slice(n // NDX * GRP, (n // NDX + 1) * GRP)
        cols = slice(n % NDX * DXC, (n % NDX + 1) * DXC)
        dx_out[rows, cols] = (dx_own[rows, cols] + dx_recv[n].astype(F32)).astype(BF16)

    arrived('dx', dx_recv.at[:NDX], partner)
    for n in range(NDX):
        finish_dx(n)
    arrived('dwq', dwq_recv.at[:3], peer)
    for r in range(4):
        if r == 3:
            arrived('dwq3', dwq_recv.at[3], peer)
        with jax.named_scope('dwq_sum'):
            rows = at(data * HALF + r * 256, 256)
            for h in range(HEADS):
                value = dot_nn(x_t[rows, :], dq[h]) + dwq_recv[r, h].astype(F32)
                dwq_out[r * 256:(r + 1) * 256, h, :] = value
    arrived(f'dx{NDX + 1}', dx_recv.at[NDX:NDX + 2], partner)
    for n in range(NDX, 2 * NDX):
        if n > NDX + 1:
            arrived(f'dx{n}', dx_recv.at[n], partner)
        finish_dx(n)
    arrived('dwkv', dwkv_recv, peer)
    dwk_out[...] += dwkv_recv[0].astype(F32)
    dwv_out[...] += dwkv_recv[1].astype(F32)
    with jax.named_scope('sends'):
        for group in ('inputs', 'mib', 'pair'):
            sent(group, xb)
        sent('dkv', dkv_full)
        sent('dq', dq_mate)
        sent('dwkv', dwkv_send)
    assert len(groups) == sems.shape[0] and len(slots) == recvs.shape[0]


def fused_step(x, dy, wq, wk, wv, wo):
    any_spec = pl.BlockSpec(memory_space=pl.ANY)
    vmem_spec = pl.BlockSpec(memory_space=pltpu.VMEM)
    scratch = [
        pltpu.VMEM((SEQ, DIM), BF16),
        pltpu.VMEM((DIM, SEQ), BF16),
        pltpu.VMEM((NCH, SEQ, CH), BF16),
        pltpu.VMEM((DIM, HEADS, HD), BF16),
        pltpu.VMEM((2 * HEADS, DIM, HD), BF16),
        pltpu.VMEM((2, DIM, HD), BF16),
        pltpu.VMEM((HEADS * HD, DIM), BF16),
        pltpu.VMEM((SEQ, HEADS * HD), BF16),
        pltpu.VMEM((SEQ, HD), BF16),
        pltpu.VMEM((SEQ, HD), BF16),
        pltpu.VMEM((HD, SEQ), BF16),
        pltpu.VMEM((HD, SEQ), BF16),
        pltpu.VMEM((HEADS, SEQ, SEQ), F32),
        pltpu.VMEM((HEADS, 1, SEQ), F32),
        pltpu.VMEM((HEADS, SEQ, 2 * BLK), BF16),
        pltpu.VMEM((HEADS * HD, SEQ), BF16),
        pltpu.VMEM((HEADS * HD, 2 * BLK), F32),
        pltpu.VMEM((HEADS * HD, SEQ), BF16),
        pltpu.VMEM((2, SEQ, HD), F32),
        pltpu.VMEM((SEQ, HD), F32),
        pltpu.VMEM((SEQ, HD), BF16),
        pltpu.VMEM((SEQ, HD), BF16),
        pltpu.VMEM((2, SEQ, HD), BF16),
        pltpu.VMEM((HEADS, SEQ, HD), BF16),
        pltpu.VMEM((2, HEADS, BLK, HD), BF16),
        pltpu.VMEM((NCH // 2, HEADS * HD, CH), BF16),
        pltpu.VMEM((NCH // 2, HEADS * HD, CH), BF16),
        pltpu.VMEM((4, HEADS, HALF // 4, HD), BF16),
        pltpu.VMEM((4, HEADS, HALF // 4, HD), BF16),
        pltpu.VMEM((BLK, DIM), F32),
        pltpu.VMEM((2 * NDX, GRP, DXC), BF16),
        pltpu.VMEM((2 * NDX, GRP, DXC), BF16),
        pltpu.VMEM((2, 256, HD), BF16),
        pltpu.VMEM((2, 256, HD), BF16),
        pltpu.SemaphoreType.DMA((6,)),
        pltpu.SemaphoreType.DMA((38,)),
        pltpu.SemaphoreType.DMA((6,)),
    ]
    return pl.pallas_call(
        body,
        out_shape=(pltpu.VMEM((BLK, DIM), BF16),
                   pltpu.VMEM((HALF, HEADS, HD), F32),
                   pltpu.VMEM((256, HD), F32),
                   pltpu.VMEM((256, HD), F32),
                   pltpu.VMEM((HEADS * HD, HALF), F32)),
        in_specs=[any_spec] * 6,
        out_specs=(vmem_spec,) * 5,
        scratch_shapes=scratch,
        compiler_params=pltpu.CompilerParams(collective_id=0, has_side_effects=True,
                                             vmem_limit_bytes=58 * 2 ** 20),
        name='attention_backward',
    )(x, dy, wq, wk, wv, wo)


def flush_body(*refs):
    sources, results, sems = refs[:5], refs[5:10], refs[10]
    copies = [pltpu.make_async_copy(a, b, sems.at[n]) for n, (a, b) in enumerate(zip(sources, results))]
    for copy in copies:
        copy.start()
    for copy in copies:
        copy.wait()


def flush(*arrays):
    any_spec = pl.BlockSpec(memory_space=pl.ANY)
    return pl.pallas_call(
        flush_body,
        out_shape=tuple(jax.ShapeDtypeStruct(a.shape, a.dtype) for a in arrays),
        in_specs=[any_spec] * 5,
        out_specs=(any_spec,) * 5,
        scratch_shapes=[pltpu.SemaphoreType.DMA((5,))],
        compiler_params=pltpu.CompilerParams(vmem_limit_bytes=2 ** 20),
        name='write_results',
    )(*arrays)


def solution(mesh):
    tok_spec = P(('pod', 'data'), 'model', None)

    def device_step(x_loc, dy_loc, w_q, w_k, w_v, w_o):
        dx, dwq, dwk, dwv, dwo = flush(*fused_step(x_loc[0], dy_loc[0], w_q, w_k[0], w_v[0],
                                                   w_o.reshape(HEADS * HD, DIM)))
        return dx[None], dwq, dwk, dwv, dwo.reshape(HEADS, HD, HALF)

    kv_rows = P(('pod', 'model', 'data'), None)
    return jax.shard_map(device_step, mesh=mesh,
                         in_specs=(tok_spec, tok_spec, P(None, 'model', None), P(), P(), P('model', None, None)),
                         out_specs=(tok_spec, P(('pod', 'data'), 'model', None), kv_rows, kv_rows,
                                    P(('pod', 'model'), None, 'data')),
                         check_vma=False)
```
